768 devices in a mesh: sfc: 96 (over x, z, core), grp: 8 (over y).
Axes of the slice: x: 4, y: 8, z: 12, core: 2. Of those that a mesh axis runs over, the one named last changes fastest.
Arguments:
- source: float32 [384, 16, 2048], P('sfc', None, 'grp'), may hold values from -8 to 8
- layer_counts: int32 [96], P('sfc'), may hold values from 1 to 4, 256 in all
Outputs:
- solution: float32 [384, 16, 2048], P('sfc', None, 'grp')
- residual: float32 [384, 16, 2048], P('sfc', None, 'grp')
- direction: float32 [384, 16, 2048], P('sfc', None, 'grp')
The draws below stay inside these ranges and needn't reach their ends.
Inputs may be any that keep to these rules, and one draw needn't show every extreme that they name: `layer_counts`: each entry counts the live leading slots of that index of sfc; they sum to 256, and at least one entry equals 4.
All inputs are finite; a program needn't handle non-finite values. No bound on the sum of `layer_counts` on one device may be relied on, other than what follows from the above.
Results may differ from the reference program's by a relative error of at most 0.00011.
Values sent between devices are 32-bit elements; how exact they have to be, the bound alone decides.
A program may use at most 32 MiB of HBM per device.

```python
import math
import jax
import jax.numpy as jnp
import numpy as np

E = 16
H = 8
BCAP = 4
PRE_SWEEPS = 2
POST_SWEEPS = 2
COARSE_SWEEPS = 4
SLOTS = 384
LIVE = 256
N_SFC = 96
N_GRP = 8


def draw_source(key, part):
    shape = (BCAP * N_SFC, E, N_GRP * E * E)
    slot = jnp.arange(BCAP * N_SFC, dtype=jnp.float32)
    device = jnp.floor(slot / BCAP)
    rise = (1.0 + 2.0 * device / max(N_SFC - 1, 1))[:, None, None]
    values = jax.random.normal(key, shape, jnp.float32) * rise
    return jnp.clip(values, -8.0, 8.0)


def profile(amount, total, reach, lean):
    portions = [(1 << 20) // math.isqrt(grade ** lean) + 1 for grade in range(2, amount + 1)]
    rest, given = total - reach - (amount - 1), [1] * (amount - 1)
    while rest > 0:
        free = [i for i in range(amount - 1) if given[i] < reach]
        whole, remaining = sum([portions[i] for i in free]), rest
        for i in free:
            extra = min(reach - given[i], max(1, remaining * portions[i] // whole), rest)
            given[i] = given[i] + extra
            rest = rest - extra
    return np.array([reach] + given)


def uneven_parts(own_key, amount, total, reach, slope):
    if amount == 2:
        one = jax.random.randint(own_key, (), max(1, total - reach), min(reach, total - 1) + 1)
        return jnp.stack([one, total - one])
    tallies = jnp.asarray(profile(amount, total, reach, slope), jnp.int32)
    twos = (amount - 1) // 2
    giver, sink = tallies[1:1 + 2 * twos:2], tallies[2:2 + 2 * twos:2]
    slack = jnp.minimum(giver - 1, reach - sink)
    shifted = jax.random.randint(jax.random.fold_in(own_key, 1), (twos,), 0, 1 << 20) % (slack + 1)
    tallies = tallies.at[1:1 + 2 * twos:2].set(giver - shifted).at[2:2 + 2 * twos:2].set(sink + shifted)
    return tallies[jax.random.permutation(jax.random.fold_in(own_key, 2), amount)]


def setup_inputs(seed: int = 0) -> dict:
    keys = jax.random.split(jax.random.key(seed), 3)
    return {
        "source": draw_source(jax.random.fold_in(keys[2], 71), 0),
        "layer_counts": uneven_parts(keys[1], N_SFC, LIVE, BCAP, 2).astype(jnp.int32),
    }


OMEGA = 2.0 / 3.0


def laplace(field, counts, edge):
    n_dev, planes, width = field.shape
    zero_plane = jnp.zeros((1, 1, width), jnp.float32)
    last_index = (counts * edge - 1).astype(jnp.int32)
    last = jnp.take_along_axis(field, last_index[:, None, None], axis=1)
    first = field[:, :1]
    prev_last = jnp.concatenate([zero_plane, last[:-1]], axis=0)
    next_first = jnp.concatenate([first[1:], zero_plane], axis=0)
    below = jnp.concatenate([prev_last, field[:, :-1]], axis=1)
    above = jnp.concatenate([field[:, 1:], jnp.zeros((n_dev, 1, width), jnp.float32)], axis=1)
    plane = jnp.arange(planes, dtype=jnp.int32)
    at_last = (plane[None, :] == last_index[:, None])[:, :, None]
    above = above + jnp.where(at_last, next_first, 0.0)
    pad_rows = jnp.zeros((n_dev, planes, edge), jnp.float32)
    north = jnp.concatenate([field[:, :, edge:], pad_rows], axis=2)
    south = jnp.concatenate([pad_rows, field[:, :, :-edge]], axis=2)
    column = (jnp.arange(width, dtype=jnp.int32) % edge)[None, None, :]
    pad_col = jnp.zeros((n_dev, planes, 1), jnp.float32)
    up_z = jnp.where(column != edge - 1, jnp.concatenate([field[:, :, 1:], pad_col], axis=2), 0.0)
    down_z = jnp.where(column != 0, jnp.concatenate([pad_col, field[:, :, :-1]], axis=2), 0.0)
    total = 6.0 * field - below - above - north - south - up_z - down_z
    live = (plane[None, :] < (counts * edge)[:, None])[:, :, None]
    return jnp.where(live, total, 0.0)


def restrict(field):
    n_dev, planes, width = field.shape
    across = width // (E * E) * E
    blocks = field.reshape(n_dev, planes // 2, 2, across // 2, 2, H, 2)
    return 0.125 * jnp.sum(blocks, axis=(2, 4, 6)).reshape(n_dev, planes // 2, (across // 2) * H)


def prolong(coarse):
    n_dev, planes, width = coarse.shape
    across = width // H
    blocks = coarse.reshape(n_dev, planes, 1, across, 1, H, 1)
    blocks = jnp.broadcast_to(blocks, (n_dev, planes, 2, across, 2, H, 2))
    return blocks.reshape(n_dev, planes * 2, across * 2 * H * 2)


def vcycle(rhs, counts):
    step = OMEGA / 6.0
    smooth = step * rhs
    for sweep in range(PRE_SWEEPS - 1):
        smooth = smooth + step * (rhs - laplace(smooth, counts, E))
    defect = rhs - laplace(smooth, counts, E)
    coarse_rhs = restrict(defect)
    coarse_step = OMEGA / 1.5
    correction = coarse_step * coarse_rhs
    for sweep in range(COARSE_SWEEPS - 1):
        correction = correction + coarse_step * (coarse_rhs - 0.25 * laplace(correction, counts, H))
    smooth = smooth + prolong(correction)
    for sweep in range(POST_SWEEPS):
        smooth = smooth + step * (rhs - laplace(smooth, counts, E))
    return smooth


def reference(source, layer_counts):
    width = source.shape[2]
    field = source.reshape(N_SFC, BCAP * E, width)
    plane = jnp.arange(BCAP * E, dtype=jnp.int32)
    live = (plane[None, :] < (layer_counts * E)[:, None])[:, :, None]
    first_rhs = jnp.where(live, field, 0.0)
    first_z = vcycle(first_rhs, layer_counts)
    image = laplace(first_z, layer_counts, E)
    rz_value = jnp.sum(first_rhs * first_z)
    curv = jnp.sum(first_z * image)
    alpha = rz_value / curv
    solution = alpha * first_z
    residual = first_rhs - alpha * image
    next_z = vcycle(residual, layer_counts)
    cross = jnp.sum(next_z * image)
    direction = next_z - (cross / curv) * first_z
    shape = (SLOTS, E, width)
    return solution.reshape(shape), residual.reshape(shape), direction.reshape(shape)
```

```python
import functools

import jax
import jax.numpy as jnp
from jax import lax
from jax.experimental import pallas as pl
from jax.experimental.pallas import tpu as pltpu
from jax.sharding import PartitionSpec as P

E = 16
OMEGA = 2.0 / 3.0
STEP = OMEGA / 6.0
KEEP = 1.0 - OMEGA
TAU = OMEGA / 1.5
SHAPES = {96: (4, 12, 2), 8: (2, 2, 2)}
MESH = pl.DeviceIdType.MESH
F32 = jnp.float32
ROWS = 48 * E
COARSE = 24 * 8


def others(*axes):
    found = [()]
    for count in axes:
        found = [f + (i,) for f in found for i in range(count)]
    return [f for f in found if any(f)]


def kernel(dims, src_hbm, cnt_ref, z_out, v_out, w_out, tot_out, *scratch):
    nx, nz, nc, ny = dims
    (own, last, ysl, ynl, below, above, r, g, q, t, c1, c2, e, cd, cu, buf_a, buf_b, row,
     load_sem, s1, r1, s2, r2, sa, ra, sb, rb) = scratch
    s = lax.axis_index("sfc")
    y = lax.axis_index("grp")
    ns = nx * nz * nc
    px = s // (nz * nc)
    pz = lax.rem(s // nc, nz)
    pc = lax.rem(s, nc)

    def near(ds, dy):
        return (lax.rem(s + ds + ns, ns), lax.rem(y + dy + ny, ny))

    def line(dz, dc):
        return ((px * nz + lax.rem(pz + dz, nz)) * nc + lax.rem(pc + dc, nc), y)

    def plane(dx, dy):
        return ((lax.rem(px + dx, nx) * nz + pz) * nc + pc, lax.rem(y + dy, ny))

    load = pltpu.make_async_copy(src_hbm, own, load_sem)
    load.start()
    line_set, plane_set = others(nz, nc), others(nx, ny)
    around = [(-1, -1), (-1, 0), (-1, 1), (0, -1), (0, 1), (1, -1), (1, 0), (1, 1)]
    barrier = pltpu.get_barrier_semaphore()
    targets = [near(*o) for o in around] + [line(*o) for o in line_set] + [plane(*o) for o in plane_set]
    for target in targets:
        pl.semaphore_signal(barrier, inc=1, device_id=target, device_id_type=MESH)
    load.wait()
    count = cnt_ref[0]
    last[...] = own[lax.rem(count + 3, 4)]
    pl.semaphore_wait(barrier, len(targets))

    copies = []

    def send(src, dst, k, target, ss, rs):
        copy = pltpu.make_async_remote_copy(
            src_ref=src, dst_ref=dst, send_sem=ss.at[k], recv_sem=rs.at[k],
            device_id=target, device_id_type=MESH)
        copy.start()
        copies.append(copy)

    for j, dy in enumerate((1, 0, -1)):
        send(last, below.at[j], j, near(1, dy), s1, r1)
        send(own.at[0], above.at[j], 3 + j, near(-1, dy), s1, r1)
    send(own, ysl, 6, near(0, 1), s1, r1)
    send(own, ynl, 7, near(0, -1), s1, r1)
    for copy in copies:
        copy.wait_recv()

    zero = jnp.zeros((E, 16 * E), F32)
    pieces = (ysl, own, ynl)
    row_ok = (y > 0, None, y < ny - 1)
    for b in range(3):
        ok = row_ok[b]

        def live(cond, value):
            if ok is not None:
                cond = jnp.logical_and(cond, ok)
            return jnp.where(cond, value, 0.0)

        slots = [live(s > 0, below[b])]
        up = live(s < ns - 1, above[b])
        for k in range(4):
            mine = live(k < count, pieces[b][k])
            slots.append(jnp.where(k == count, up, mine) if k else mine)
        slots.append(jnp.where(count == 4, up, 0.0))
        stack = jnp.concatenate(slots + [zero, zero], axis=0)
        for half in range(2):
            r[pl.ds(b * 256 + half * 128, 128), :] = stack[:, half * 128:half * 128 + 128].T

    lane = lax.broadcasted_iota(jnp.int32, (1, 128), 1)
    end = 16 + 16 * count
    mask = jnp.where((lane < 16) & (s > 0) | (lane >= 16) & (lane < end)
                     | (lane >= end) & (lane < end + 16) & (s < ns - 1), 1.0, 0.0).astype(F32)
    masks = [jnp.where(y > 0, mask, 0.0), mask, jnp.where(y < ny - 1, mask, 0.0)]
    fine_masks = [jnp.broadcast_to(m * STEP, (16, 128)) for m in masks]
    coarse_masks = [jnp.broadcast_to(m * (TAU / 4.0), (8, 128)) for m in masks]
    sub16 = lax.broadcasted_iota(jnp.int32, (16, 128), 0)
    sub8 = lax.broadcasted_iota(jnp.int32, (8, 128), 0)
    even = lax.rem(lax.broadcasted_iota(jnp.int32, (8, 128), 1), 2) == 0

    def total(ref, yy):
        i = 16 * yy
        mid = ref[pl.ds(i, 16), :]
        south, north = ref[pl.ds(i - 16, 16), :], ref[pl.ds(i + 16, 16), :]
        down = jnp.where(sub16 == 0, 0.0, pltpu.roll(mid, 1, 0))
        up = jnp.where(sub16 == 15, 0.0, pltpu.roll(mid, 15, 0))
        left, right = pltpu.roll(mid, 1, 1), pltpu.roll(mid, 127, 1)
        return mid, (south + north) + (down + up) + (left + right)

    def smooth(src, dst, lo, hi, add=None):
        for yy in range(lo, hi):
            mid, six = total(src, yy)
            value = KEEP * mid + fine_masks[yy // 16] * six
            if add is not None:
                value = value + STEP * add[pl.ds(16 * yy, 16), :]
            dst[pl.ds(16 * yy, 16), :] = value

    def restrict(src, c, lo, hi):
        for yc in range(lo, hi):
            i = 32 * yc
            u = (src[pl.ds(i, 8, stride=2), :] + src[pl.ds(i + 1, 8, stride=2), :]
                 + src[pl.ds(i + 16, 8, stride=2), :] + src[pl.ds(i + 17, 8, stride=2), :])
            pair = jnp.where(even, pltpu.roll(u, 127, 1), pltpu.roll(u, 1, 1))
            c[pl.ds(8 * yc, 8), :] = 0.125 * (u + pair)

    def coarse_sweep(c, src, dst, lo, hi):
        for yc in range(lo, hi):
            mid = src[pl.ds(8 * yc, 8), :]
            south, north = src[pl.ds(8 * yc - 8, 8), :], src[pl.ds(8 * yc + 8, 8), :]
            down = jnp.where(sub8 == 0, 0.0, pltpu.roll(mid, 1, 0))
            up = jnp.where(sub8 == 7, 0.0, pltpu.roll(mid, 7, 0))
            left, right = pltpu.roll(mid, 2, 1), pltpu.roll(mid, 126, 1)
            six = (south + north) + (down + up) + (left + right)
            dst[pl.ds(8 * yc, 8), :] = (
                KEEP * mid + TAU * c[pl.ds(8 * yc, 8), :] + coarse_masks[yc // 8] * six)

    def coarse_solve(c, lo, hi):
        e[0, pl.ds(8 * lo, 8 * (hi - lo)), :] = TAU * c[pl.ds(8 * lo, 8 * (hi - lo)), :]
        coarse_sweep(c, e.at[0], e.at[1], lo + 1, hi - 1)
        coarse_sweep(c, e.at[1], e.at[0], lo + 2, hi - 2)
        coarse_sweep(c, e.at[0], e.at[1], lo + 3, hi - 3)

    def corrected(rhs, first, dst, lo, hi):
        for yc in range(lo, hi):
            add = e[1, pl.ds(8 * yc, 8), :]
            for k in range(4):
                at = pl.ds(32 * yc + (k // 2) * 16 + k % 2, 8, stride=2)
                dst[at, :] = STEP * (rhs[at, :] + first[at, :]) + add

    smooth(r, g, 1, 47)
    smooth(g, q, 2, 46)
    restrict(q, c1, 1, 23)
    coarse_solve(c1, 1, 23)
    corrected(r, g, q, 4, 20)
    smooth(q, g, 10, 38, r)
    smooth(g, t, 11, 37, r)
    for yy in range(12, 36):
        mid, six = total(t, yy)
        q[pl.ds(16 * yy, 16), :] = 6.0 * mid - (1.0 / STEP) * fine_masks[yy // 16] * six
    alive = (lane >= 16) & (lane < end)
    v = q
    zv = jnp.zeros((16, 128), F32)
    rz, curv = zv, zv
    for yy in range(16, 32):
        at = pl.ds(16 * yy, 16)
        rz = rz + r[at, :] * t[at, :]
        curv = curv + t[at, :] * v[at, :]

    smooth(v, g, 13, 35)
    smooth(g, r, 14, 34)
    restrict(r, c1, 8, 16)

    mine = c1[pl.ds(64, 64), :]
    moved = pltpu.roll(mine, 112, 1)
    for k in range(2, 5):
        moved = jnp.where(count == k, pltpu.roll(mine, 128 - 16 * k, 1), moved)
    cd[0] = moved
    cu[0] = mine
    copies2 = []

    def send2(src, dst, k, target):
        copy = pltpu.make_async_remote_copy(
            src_ref=src, dst_ref=dst, send_sem=s2.at[k], recv_sem=r2.at[k],
            device_id=target, device_id_type=MESH)
        copy.start()
        copies2.append(copy)

    send2(cd.at[0], cd.at[1], 0, near(1, 0))
    send2(cu.at[0], cu.at[1], 1, near(-1, 0))
    for copy in copies2:
        copy.wait_recv()
    ahead = cu[1]
    moved = pltpu.roll(ahead, 16, 1)
    for k in range(2, 5):
        moved = jnp.where(count == k, pltpu.roll(ahead, 16 * k, 1), moved)
    lo_lane = (lane < 16) & (s > 0)
    hi_lane = (lane >= end) & (lane < end + 16) & (s < ns - 1)
    full = jnp.where(alive, mine, jnp.where(lo_lane, cd[1], jnp.where(hi_lane, moved, 0.0)))
    c2[pl.ds(64, 64), :] = full
    send2(c2.at[pl.ds(64, 32)], c2.at[pl.ds(128, 32)], 2, near(0, -1))
    send2(c2.at[pl.ds(96, 32)], c2.at[pl.ds(32, 32)], 3, near(0, 1))
    for copy in copies2[2:]:
        copy.wait_recv()

    @pl.when(y == 0)
    def _():
        c2[pl.ds(32, 32), :] = jnp.zeros((32, 128), F32)

    @pl.when(y == ny - 1)
    def _():
        c2[pl.ds(128, 32), :] = jnp.zeros((32, 128), F32)

    coarse_solve(c2, 4, 20)
    corrected(v, g, r, 7, 17)
    smooth(r, g, 15, 33, v)
    smooth(g, r, 16, 32, v)
    wv = zv
    for yy in range(16, 32):
        at = pl.ds(16 * yy, 16)
        wv = wv + r[at, :] * v[at, :]

    def dot(acc):
        return jnp.sum(jnp.where(alive, acc, 0.0))

    sums = jnp.where(lane == 0, dot(rz), jnp.where(lane == 1, dot(curv), dot(wv)))

    def all_to_all(value, buf, where, group, ss, rs):
        n = len(group)
        buf[n] = value
        out = []
        for k, o in enumerate(group):
            copy = pltpu.make_async_remote_copy(
                src_ref=buf.at[n], dst_ref=buf.at[k], send_sem=ss.at[k], recv_sem=rs.at[k],
                device_id=where(*o), device_id_type=MESH)
            copy.start()
            out.append(copy)
        return out

    first = all_to_all(sums, buf_a, line, line_set, sa, ra)

    for src, dst in ((t, z_out), (v, v_out), (r, w_out)):
        halves = []
        for half in range(2):
            x = src[pl.ds(256 + half * 128, 128), :]
            halves.append(jnp.where(alive, x, 0.0).T)
        for k in range(4):
            for half in range(2):
                dst[k, :, pl.ds(half * 128, 128)] = halves[half][16 + 16 * k:32 + 16 * k, :]

    for copy in first:
        copy.wait_recv()
    second = all_to_all(jnp.sum(buf_a[...], axis=0), buf_b, plane, plane_set, sb, rb)
    for copy in second:
        copy.wait_recv()
    tot_out[...] = jnp.sum(buf_b[...], axis=0)
    for copy in copies + copies2 + first + second:
        copy.wait_send()


def solution(mesh):
    ns, ny = mesh.shape["sfc"], mesh.shape["grp"]
    nx, nz, nc = SHAPES[ns]
    n_line, n_plane = nz * nc - 1, nx * ny - 1
    dma = pltpu.SemaphoreType.DMA

    def shards(source, layer_counts):
        block = jax.ShapeDtypeStruct((4, E, 16 * E), F32)
        vmem = pl.BlockSpec(memory_space=pltpu.VMEM)
        z0, image, w, total = pl.pallas_call(
            functools.partial(kernel, (nx, nz, nc, ny)),
            out_shape=(block, block, block, jax.ShapeDtypeStruct((1, 128), F32)),
            in_specs=[pl.BlockSpec(memory_space=pl.ANY), pl.BlockSpec(memory_space=pltpu.SMEM)],
            out_specs=(vmem, vmem, vmem, vmem),
            scratch_shapes=[
                pltpu.VMEM((4, E, 256), F32), pltpu.VMEM((E, 256), F32),
                pltpu.VMEM((4, E, 256), F32), pltpu.VMEM((4, E, 256), F32),
                pltpu.VMEM((3, E, 256), F32), pltpu.VMEM((3, E, 256), F32),
                pltpu.VMEM((ROWS, 128), F32), pltpu.VMEM((ROWS, 128), F32),
                pltpu.VMEM((ROWS, 128), F32), pltpu.VMEM((ROWS, 128), F32),
                pltpu.VMEM((COARSE, 128), F32), pltpu.VMEM((COARSE, 128), F32), pltpu.VMEM((2, COARSE, 128), F32),
                pltpu.VMEM((2, 64, 128), F32), pltpu.VMEM((2, 64, 128), F32),
                pltpu.VMEM((n_line + 1, 1, 128), F32), pltpu.VMEM((n_plane + 1, 1, 128), F32),
                pltpu.VMEM((1, 128), F32),
                dma, dma((8,)), dma((8,)), dma((4,)), dma((4,)),
                dma((n_line,)), dma((n_line,)), dma((n_plane,)), dma((n_plane,)),
            ],
            compiler_params=pltpu.CompilerParams(collective_id=0, has_side_effects=True),
        )(source, layer_counts)
        rz, curv, wv = total[0, 0], total[0, 1], total[0, 2]
        alpha = rz / curv
        k = lax.broadcasted_iota(jnp.int32, (4, 1, 1), 0)
        rhs = jnp.where(k < layer_counts[0], source, 0.0)
        return alpha * z0, rhs - alpha * image, alpha * ((wv / curv) * z0 - w)

    spec = P("sfc", None, "grp")
    return jax.shard_map(
        shards, mesh=mesh, in_specs=(spec, P("sfc")), out_specs=(spec, spec, spec), check_vma=False)
```

```python
import functools

import jax
import jax.numpy as jnp
from jax import lax
from jax.experimental import pallas as pl
from jax.experimental.pallas import tpu as pltpu
from jax.sharding import PartitionSpec as P

E = 16
OMEGA = 2.0 / 3.0
STEP = OMEGA / 6.0
KEEP = 1.0 - OMEGA
TAU = OMEGA / 1.5
QUARTER = TAU / 4.0
SHAPES = {96: (4, 12, 2), 8: (2, 2, 2)}
MESH = pl.DeviceIdType.MESH
F32 = jnp.float32
ROWS = 48 * E
COARSE = 24 * 8
NEED = dict(g=(1, 47), q=(2, 46), c=(1, 23), e1=(2, 22), e2=(3, 21), e3=(4, 20), zp=(8, 40),
            z1=(10, 38), z0=(11, 37), v=(12, 36), g2=(13, 35), q2=(14, 34), c2=(7, 17))


def others(*axes):
    found = [()]
    for count in axes:
        found = [f + (i,) for f in found for i in range(count)]
    return [f for f in found if any(f)]


def kernel(dims, src_hbm, cnt_hbm, sol_ref, res_ref, dir_ref, *scratch):
    nx, nz, nc, ny = dims
    (own, cnt, last, ysl, ynl, below, above, r, g, q, zp, z1, z0, v, g2, q2, w1, w,
     c, e1, e2, e3, c2, kap, cw, cd, cu, zt, vt, wt,
     msg, face, faces, hb, hs, hx, hall, hrow, tot,
     load_sem, s1, r1, s2, r2, sm, rb, rs, rx, sh, rh, st, rt) = scratch
    s = lax.axis_index("sfc")
    y = lax.axis_index("grp")
    ns, size = nx * nz * nc, nz * nc
    px, place = s // size, lax.rem(s, size)
    is_head = place == 1
    plane_set = others(nx, ny)

    load = pltpu.make_async_copy(src_hbm, own, load_sem.at[0])
    load.start()
    load_count = pltpu.make_async_copy(cnt_hbm, cnt, load_sem.at[1])
    load_count.start()

    around = [(1, 1), (1, -1), (-1, 1), (-1, -1), (1, 0), (-1, 0), (0, 1), (0, -1)]
    d_ok = {1: s < ns - 1, -1: s > 0, 0: None}
    y_ok = {1: y < ny - 1, -1: y > 0, 0: None}

    def there(ds, dy):
        conds = [k for k in (d_ok[ds], y_ok[dy]) if k is not None]
        return functools.reduce(jnp.logical_and, conds)

    def near(ds, dy):
        return (s + ds, y + dy)

    def head_of(x, yy):
        return (x * size + 1, yy)

    def plane(dx, dy):
        return (lax.rem(px + dx, nx) * size + 1, lax.rem(y + dy, ny))

    barrier = pltpu.get_barrier_semaphore()

    def greet(target):
        pl.semaphore_signal(barrier, inc=1, device_id=target, device_id_type=MESH)

    for o in around:
        pl.when(there(*o))(functools.partial(greet, near(*o)))

    @pl.when(is_head)
    def _():
        for o in plane_set:
            greet(plane(*o))
        for k in range(size):
            if k != 1:
                greet((px * size + k, y))

        @pl.when(y < ny - 1)
        def _():
            for k in range(size):
                greet((px * size + k, y + 1))

        @pl.when(px < nx - 1)
        def _():
            greet(((px + 1) * size, y))

    one = lambda cond: jnp.where(cond, 1, 0)
    beside = (1 + one(s > 0) + one(s < ns - 1)) * (1 + one(y > 0) + one(y < ny - 1)) - 1
    heads = one(y > 0) + one((place == 0) & (px > 0)) + jnp.where(is_head, len(plane_set), 1)

    load.wait()
    load_count.wait()
    count = cnt[0]
    last[...] = own[lax.rem(count + 3, 4)]
    pl.semaphore_wait(barrier, beside + heads)

    def copy_to(src, dst, ss, rs_, target):
        return pltpu.make_async_remote_copy(
            src_ref=src, dst_ref=dst, send_sem=ss, recv_sem=rs_, device_id=target, device_id_type=MESH)

    halo = {}
    for k, (ds, dy) in enumerate(around):
        if ds == 0:
            continue
        src, box = (last, below) if ds == 1 else (own.at[0], above)
        halo[ds, dy] = [copy_to(src, box.at[1 - dy], s1.at[k], r1.at[k], near(ds, dy))]
    for k, (dy, box) in enumerate(((1, ysl), (-1, ynl))):
        halo[0, dy] = []
        for part in range(2):
            half = pl.ds(128 * (1 - part if dy == 1 else part), 128)
            i = 6 + 2 * k + part
            halo[0, dy].append(copy_to(own.at[:, :, half], box.at[:, :, half], s1.at[i], r1.at[i], near(0, dy)))
    for part in range(2):
        for o in around:
            if part < len(halo[o]):
                pl.when(there(*o))(halo[o][part].start)

    def arrived(ds, dy, part=0):
        pl.when(there(-ds, -dy))(halo[ds, dy][part].wait_recv)

    pieces = (ysl, own, ynl)
    row_ok = (y > 0, None, y < ny - 1)

    def assemble(b, half):
        at = pl.ds(128 * half, 128)
        ok = row_ok[b]

        def live(cond, value):
            if ok is not None:
                cond = jnp.logical_and(cond, ok)
            return jnp.where(cond, value, 0.0)

        slots = [live(s > 0, below[b, :, at])]
        up = live(s < ns - 1, above[b, :, at])
        for k in range(4):
            mine = live(k < count, pieces[b][k, :, at])
            slots.append(jnp.where(k == count, up, mine) if k else mine)
        slots.append(jnp.where(count == 4, up, 0.0))
        zero = jnp.zeros((2 * E, 128), F32)
        r[pl.ds(b * 256 + half * 128, 128), :] = jnp.concatenate(slots + [zero], axis=0).T

    lane = lax.broadcasted_iota(jnp.int32, (1, 128), 1)
    end = 16 + 16 * count
    mask = jnp.where((lane < 16) & (s > 0) | (lane >= 16) & (lane < end)
                     | (lane >= end) & (lane < end + 16) & (s < ns - 1), 1.0, 0.0).astype(F32)
    masks = [jnp.where(y > 0, mask, 0.0), mask, jnp.where(y < ny - 1, mask, 0.0)]
    fine_masks = [jnp.broadcast_to(m * STEP, (16, 128)) for m in masks]
    coarse_masks = [jnp.broadcast_to(m * QUARTER, (8, 128)) for m in masks]
    sub16 = lax.broadcasted_iota(jnp.int32, (16, 128), 0)
    sub8 = lax.broadcasted_iota(jnp.int32, (8, 128), 0)
    even = lax.rem(lax.broadcasted_iota(jnp.int32, (8, 128), 1), 2) == 0
    alive = (lane >= 16) & (lane < end)

    def total(ref, yy):
        i = 16 * yy
        mid = ref[pl.ds(i, 16), :]
        south, north = ref[pl.ds(i - 16, 16), :], ref[pl.ds(i + 16, 16), :]
        down = jnp.where(sub16 == 0, 0.0, pltpu.roll(mid, 1, 0))
        up = jnp.where(sub16 == 15, 0.0, pltpu.roll(mid, 15, 0))
        left, right = pltpu.roll(mid, 1, 1), pltpu.roll(mid, 127, 1)
        return mid, (south + north) + (down + up) + (left + right)

    def coarse_total(ref, yc):
        mid = ref[pl.ds(8 * yc, 8), :]
        south, north = ref[pl.ds(8 * yc - 8, 8), :], ref[pl.ds(8 * yc + 8, 8), :]
        down = jnp.where(sub8 == 0, 0.0, pltpu.roll(mid, 1, 0))
        up = jnp.where(sub8 == 7, 0.0, pltpu.roll(mid, 7, 0))
        left, right = pltpu.roll(mid, 2, 1), pltpu.roll(mid, 126, 1)
        return mid, (south + north) + (down + up) + (left + right)

    def smooth(src, dst, add=None):
        def row(yy):
            mid, six = total(src, yy)
            value = KEEP * mid + fine_masks[yy // 16] * six
            if add is not None:
                value = value + STEP * add[pl.ds(16 * yy, 16), :]
            dst[pl.ds(16 * yy, 16), :] = value
        return row

    def apply(src, dst):
        def row(yy):
            mid, six = total(src, yy)
            dst[pl.ds(16 * yy, 16), :] = 6.0 * mid - (1.0 / STEP) * fine_masks[yy // 16] * six
        return row

    def restrict(src, dst):
        def row(yc):
            i = 32 * yc
            u = (src[pl.ds(i, 8, stride=2), :] + src[pl.ds(i + 1, 8, stride=2), :]
                 + src[pl.ds(i + 16, 8, stride=2), :] + src[pl.ds(i + 17, 8, stride=2), :])
            pair = jnp.where(even, pltpu.roll(u, 127, 1), pltpu.roll(u, 1, 1))
            dst[pl.ds(8 * yc, 8), :] = 0.125 * (u + pair)
        return row

    def coarse_first(rhs, dst):
        def row(yc):
            mid, six = coarse_total(rhs, yc)
            dst[pl.ds(8 * yc, 8), :] = (TAU * (1.0 + KEEP)) * mid + TAU * (coarse_masks[yc // 8] * six)
        return row

    def coarse_sweep(rhs, src, dst):
        def row(yc):
            mid, six = coarse_total(src, yc)
            dst[pl.ds(8 * yc, 8), :] = (
                KEEP * mid + TAU * rhs[pl.ds(8 * yc, 8), :] + coarse_masks[yc // 8] * six)
        return row

    def corrected(rhs, first, coarse, dst):
        def pair(yc):
            add = coarse[pl.ds(8 * yc, 8), :]
            for k in range(4):
                at = pl.ds(32 * yc + (k // 2) * 16 + k % 2, 8, stride=2)
                dst[at, :] = STEP * (rhs[at, :] + first[at, :]) + add
        return pair

    def rows(fn, lo, hi):
        for i in range(lo, hi):
            fn(i)

    shrink = lambda lo, hi: (lo + 1, hi - 1)
    halve = lambda lo, hi: (-(-lo // 2), hi // 2)
    double = lambda lo, hi: (2 * lo, 2 * hi)
    stages = [
        ("g", "r", shrink, smooth(r, g)), ("q", "g", shrink, smooth(g, q)),
        ("c", "q", halve, restrict(q, c)), ("e1", "c", shrink, coarse_first(c, e1)),
        ("e2", "e1", shrink, coarse_sweep(c, e1, e2)), ("e3", "e2", shrink, coarse_sweep(c, e2, e3)),
        ("zp", "e3", double, corrected(r, g, e3, zp)), ("z1", "zp", shrink, smooth(zp, z1, r)),
        ("z0", "z1", shrink, smooth(z1, z0, r)), ("v", "z0", shrink, apply(z0, v)),
        ("g2", "v", shrink, smooth(v, g2)), ("q2", "g2", shrink, smooth(g2, q2)),
        ("c2", "q2", halve, restrict(q2, c2)),
    ]
    done = {}

    def advance(lo, hi):
        have = {"r": (lo, hi)}
        for name, source, change, fn in stages:
            new_lo, new_hi = change(*have[source])
            new_lo, new_hi = max(new_lo, NEED[name][0]), min(new_hi, NEED[name][1])
            if new_lo >= new_hi:
                break
            have[name] = (new_lo, new_hi)
            old = done.get(name)
            spans = [(new_lo, new_hi)] if old is None else [(new_lo, old[0]), (old[1], new_hi)]
            for span in spans:
                if name == "zp":
                    rows(fn, span[0] // 2, span[1] // 2)
                else:
                    rows(fn, *span)
            done[name] = (new_lo, new_hi)

    arrived(1, 0)
    arrived(-1, 0)
    assemble(1, 0)
    assemble(1, 1)
    advance(16, 32)
    for dy, b, half in ((1, 0, 1), (-1, 2, 0)):
        arrived(1, dy)
        arrived(-1, dy)
        arrived(0, dy, 0)
        assemble(b, half)
    advance(8, 40)
    for dy, b, half in ((1, 0, 0), (-1, 2, 1)):
        arrived(0, dy, 1)
        assemble(b, half)
    advance(0, 48)

    def keep_alive(value):
        return jnp.where(alive, value, 0.0)

    rz = jnp.zeros((16, 128), F32)
    curv, fine = rz, rz
    for yy in range(16, 32):
        at = pl.ds(16 * yy, 16)
        vy, gy, qy, zy = v[at, :], g2[at, :], q2[at, :], z0[at, :]
        rz = rz + r[at, :] * zy
        curv = curv + zy * vy
        fine = fine + (vy * (vy + gy + qy) + gy * qy)
    for yc in range(8, 16):
        mid, six = coarse_total(c2, yc)
        kap[pl.ds(8 * (yc - 7), 8), :] = keep_alive(KEEP * mid + coarse_masks[1] * six)
    blank = jnp.zeros((8, 128), F32)
    kap[pl.ds(0, 8), :] = blank
    kap[pl.ds(72, 8), :] = blank
    coarse = blank
    for yc in range(8, 16):
        k, six = coarse_total(kap, yc - 7)
        cc = c2[pl.ds(8 * yc, 8), :]
        coarse = coarse + (cc * (cc + k) + k * ((1.0 + KEEP) * k + QUARTER * six))
    column = lambda value: jnp.sum(keep_alive(value), axis=0, keepdims=True)
    inner = kap[pl.ds(8, 64), :]
    turned = jnp.concatenate([inner, inner], axis=0).T
    first_plane, last_plane = turned[16:17], turned[31:32]
    for k in range(2, 5):
        last_plane = jnp.where(count == k, turned[15 + 16 * k:16 + 16 * k], last_plane)
    d_face = jnp.where(lane < 64, first_plane, last_plane)
    even4 = even[:4]
    packed = lambda f: jnp.where(even4, f[:4], f[4:])
    north_face, south_face = packed(kap[pl.ds(64, 8), :]), packed(kap[pl.ds(8, 8), :])
    msg[...] = jnp.concatenate(
        [column(rz), column(curv), STEP * column(fine) + (4.0 * TAU) * column(coarse), d_face, north_face], axis=0)
    face[...] = south_face
    faces[...] = d_face
    to_head = copy_to(msg, hb.at[pl.ds(pl.multiple_of(8 * place, 8), 8)], sm.at[0], rb.at[place], head_of(px, y))
    to_south = copy_to(face, hs.at[pl.ds(pl.multiple_of(4 * place, 4), 4)], sm.at[1], rs.at[place], head_of(px, y - 1))
    to_back = copy_to(faces, hx, sm.at[2], rx, head_of(px - 1, y))
    pl.when(jnp.logical_not(is_head))(to_head.start)
    pl.when(y > 0)(to_south.start)
    pl.when((place == 0) & (px > 0))(to_back.start)

    mine = c2[pl.ds(64, 64), :]

    def shifted(value, sign):
        out = pltpu.roll(value, (16 * sign) % 128, 1)
        for k in range(2, 5):
            out = jnp.where(count == k, pltpu.roll(value, (16 * k * sign) % 128, 1), out)
        return out

    cd[0] = shifted(mine, -1)
    cu[0] = mine
    along = [copy_to(cd.at[0], cd.at[1], s2.at[0], r2.at[0], near(1, 0)),
             copy_to(cu.at[0], cu.at[1], s2.at[1], r2.at[1], near(-1, 0))]
    pl.when(s < ns - 1)(along[0].start)
    pl.when(s > 0)(along[1].start)

    def turn_back(src, dst):
        for half in range(2):
            x = keep_alive(src[pl.ds(256 + half * 128, 128), :]).T
            for k in range(4):
                dst[k, :, pl.ds(half * 128, 128)] = x[16 + 16 * k:32 + 16 * k, :]

    pl.when(s > 0)(along[0].wait_recv)
    pl.when(s < ns - 1)(along[1].wait_recv)
    lo_lane = (lane < 16) & (s > 0)
    hi_lane = (lane >= end) & (lane < end + 16) & (s < ns - 1)
    cw[pl.ds(64, 64), :] = jnp.where(
        alive, mine, jnp.where(lo_lane, cd[1], jnp.where(hi_lane, shifted(cu[1], 1), 0.0)))
    across = [copy_to(cw.at[pl.ds(64, 32)], cw.at[pl.ds(128, 32)], s2.at[2], r2.at[2], near(0, -1)),
              copy_to(cw.at[pl.ds(96, 32)], cw.at[pl.ds(32, 32)], s2.at[3], r2.at[3], near(0, 1))]
    pl.when(y > 0)(across[0].start)
    pl.when(y < ny - 1)(across[1].start)

    def member(k):
        return copy_to(msg, hb.at[pl.ds(8 * k, 8)], sm.at[0], rb.at[k], head_of(px, y))

    def beyond(k):
        return copy_to(face, hs.at[pl.ds(4 * k, 4)], sm.at[1], rs.at[k], head_of(px, y))

    def round_of(k):
        return copy_to(hall.at[len(plane_set)], hall.at[k], sh.at[k], rh.at[k], plane(*plane_set[k]))

    @pl.when(is_head)
    def _():
        hb[pl.ds(8, 8), :] = msg[...]
        for k in range(size):
            if k != 1:
                member(k).wait_recv()

        @pl.when(y < ny - 1)
        def _():
            for k in range(size):
                beyond(k).wait_recv()

        pl.when(px < nx - 1)(to_back.wait_recv)
        acc = hb[pl.ds(0, 8), :]
        for k in range(1, size):
            acc = acc + hb[pl.ds(8 * k, 8), :]
        sides = jnp.zeros((4, 128), F32)
        for k in range(size):
            sides = sides + hb[pl.ds(8 * k + 4, 4), :] * hs[pl.ds(4 * k, 4), :]
        sides = jnp.where(y < ny - 1, sides, 0.0)
        front = hb[pl.ds(3, size, stride=8), :]
        ends = pltpu.roll(front, 64, 1)
        chain = jnp.sum(ends[:size - 1] * hb[pl.ds(11, size - 1, stride=8), :], axis=0, keepdims=True)
        chain = chain + jnp.where(px < nx - 1, ends[size - 1:] * hx[...], 0.0)
        cross = jnp.where(lane < 64, chain, 0.0) + jnp.sum(sides, axis=0, keepdims=True)
        three = jnp.concatenate([acc[:2], acc[2:3] + (16.0 * TAU * QUARTER) * cross], axis=0)
        sums = jnp.sum(three, axis=1, keepdims=True)
        hall[len(plane_set)] = jnp.where(lane == 0, sums[:1], jnp.where(lane == 1, sums[1:2], sums[2:]))
        for k in range(len(plane_set)):
            round_of(k).start()

    turn_back(z0, zt)
    turn_back(v, vt)

    pl.when(y > 0)(across[1].wait_recv)
    pl.when(y < ny - 1)(across[0].wait_recv)
    outside = jnp.zeros((32, 128), F32)

    @pl.when(y == 0)
    def _():
        cw[pl.ds(32, 32), :] = outside

    @pl.when(y == ny - 1)
    def _():
        cw[pl.ds(128, 32), :] = outside

    rows(coarse_first(cw, e1), 5, 19)
    rows(coarse_sweep(cw, e1, e2), 6, 18)
    rows(coarse_sweep(cw, e2, e3), 7, 17)
    rows(corrected(v, g2, e3, zp), 7, 17)
    rows(smooth(zp, w1, v), 15, 33)
    rows(smooth(w1, w, v), 16, 32)
    turn_back(w, wt)

    def news(k):
        return copy_to(hrow, tot, st.at[k], rt, (px * size + k, y))

    @pl.when(is_head)
    def _():
        for k in range(len(plane_set)):
            round_of(k).wait_recv()
        hrow[...] = jnp.sum(hall[...], axis=0)
        for k in range(size):
            if k != 1:
                news(k).start()
        tot[...] = hrow[...]

    pl.when(jnp.logical_not(is_head))(news(0).wait_recv)
    sums = tot[...]
    pick = lambda k: jnp.broadcast_to(sums[:, k:k + 1], (1, 128))
    rz_all, curv_all, w_all = pick(0), pick(1), pick(2)
    alpha = rz_all / curv_all
    beta = alpha * (w_all / curv_all)
    for k in range(4):
        for half in range(2):
            at = pl.ds(128 * half, 128)
            zk = zt[k, :, at]
            sol_ref[k, :, at] = alpha * zk
            res_ref[k, :, at] = jnp.where(k < count, own[k, :, at], 0.0) - alpha * vt[k, :, at]
            dir_ref[k, :, at] = beta * zk - alpha * wt[k, :, at]

    for o in around:
        for copy in halo[o]:
            pl.when(there(*o))(copy.wait_send)
    pl.when(jnp.logical_not(is_head))(to_head.wait_send)
    pl.when(y > 0)(to_south.wait_send)
    pl.when((place == 0) & (px > 0))(to_back.wait_send)
    pl.when(s < ns - 1)(along[0].wait_send)
    pl.when(s > 0)(along[1].wait_send)
    pl.when(y > 0)(across[0].wait_send)
    pl.when(y < ny - 1)(across[1].wait_send)

    @pl.when(is_head)
    def _():
        for k in range(len(plane_set)):
            round_of(k).wait_send()
        for k in range(size):
            if k != 1:
                news(k).wait_send()


def flush(*refs):
    sources, targets, sem = refs[:3], refs[3:6], refs[6]
    copies = [pltpu.make_async_copy(a, b, sem.at[k]) for k, (a, b) in enumerate(zip(sources, targets))]
    for copy in copies:
        copy.start()
    for copy in copies:
        copy.wait()


def solution(mesh):
    ns, ny = mesh.shape["sfc"], mesh.shape["grp"]
    nx, nz, nc = SHAPES[ns]
    size, n_plane = nz * nc, nx * ny - 1
    dma = pltpu.SemaphoreType.DMA
    block = jax.ShapeDtypeStruct((4, E, 16 * E), F32)
    vmem = pl.BlockSpec(memory_space=pltpu.VMEM)
    hbm = pl.BlockSpec(memory_space=pltpu.HBM)
    slots = lambda k: pltpu.VMEM((k, E, 256), F32)
    fine = pltpu.VMEM((ROWS, 128), F32)
    coarse = pltpu.VMEM((COARSE, 128), F32)
    line = lambda *k: pltpu.VMEM((*k, 128), F32)

    def shards(source, layer_counts):
        parts = pl.pallas_call(
            functools.partial(kernel, (nx, nz, nc, ny)),
            out_shape=(block, block, block),
            in_specs=[hbm, hbm],
            out_specs=(vmem, vmem, vmem),
            scratch_shapes=[
                slots(4), pltpu.SMEM((1,), jnp.int32), pltpu.VMEM((E, 256), F32),
                slots(4), slots(4), slots(3), slots(3), *[fine] * 11,
                *[coarse] * 4, coarse, line(80), coarse, line(2, 64), line(2, 64), slots(4), slots(4), slots(4),
                line(8), line(4), line(1), line(8 * size), line(4 * size), line(1), line(n_plane + 1, 1),
                line(1), line(1),
                dma((2,)), dma((10,)), dma((10,)), dma((4,)), dma((4,)), dma((3,)), dma((size,)), dma((size,)),
                dma, dma((n_plane,)), dma((n_plane,)), dma((size,)), dma,
            ],
            compiler_params=pltpu.CompilerParams(
                collective_id=0, has_side_effects=True, vmem_limit_bytes=16 << 20),
        )(pltpu.with_memory_space_constraint(source, pltpu.HBM), layer_counts)
        return pl.pallas_call(
            flush, out_shape=(block, block, block), in_specs=[vmem] * 3, out_specs=(hbm,) * 3,
            scratch_shapes=[dma((3,))],
            compiler_params=pltpu.CompilerParams(vmem_limit_bytes=1 << 20),
        )(*parts)

    spec = P("sfc", None, "grp")
    return jax.shard_map(
        shards, mesh=mesh, in_specs=(spec, P("sfc")), out_specs=(spec, spec, spec), check_vma=False)
```

```python
import functools

import jax
import jax.numpy as jnp
from jax import lax
from jax.experimental import pallas as pl
from jax.experimental.pallas import tpu as pltpu
from jax.sharding import PartitionSpec as P

E = 16
OMEGA = 2.0 / 3.0
STEP = OMEGA / 6.0
KEEP = 1.0 - OMEGA
TAU = OMEGA / 1.5
QUARTER = TAU / 4.0
SHAPES = {96: (4, 12, 2), 8: (2, 2, 2)}
MESH = pl.DeviceIdType.MESH
F32 = jnp.float32
FINE = 8 + 24 * 25
COARSE = 8 + 16 * 13
NEED = dict(g=1, q=2, c=1, e1=2, e2=3, e3=4, zp=8, z1=10, z0=11, v=12, g2=13, q2=14, c2=7)


def others(*axes):
    found = [()]
    for count in axes:
        found = [f + (i,) for f in found for i in range(count)]
    far = lambda f: -sum(min(i, n - i) for i, n in zip(f, axes))
    return sorted([f for f in found if any(f)], key=far)


def fine_row(j):
    return 8 + 24 * j


def coarse_row(j):
    return 8 + 16 * j


def kernel(dims, src_hbm, cnt_ref, sol_ref, res_ref, dir_ref, *scratch):
    nx, nz, nc, ny = dims
    (own, last, ysl, ynl, below, above, r, g, q, zp, z1, z0, v, g2, q2, w,
     c, e1, e2, e3, c2, kap, cd, cu, ca, cs, cn, zt, vt, wt,
     msg, face, faces, hb, hs, hx, hall, hrow, tot,
     load_sem, s1, r1, s2, r2, sm, rb, rs, rx, sh, rh, st, rt) = scratch
    s = lax.axis_index("sfc")
    y = lax.axis_index("grp")
    ns, size = nx * nz * nc, nz * nc
    px, place = s // size, lax.rem(s, size)
    is_head = place == 1
    plane_set = others(nx, ny)
    n_plane = len(plane_set)

    loads = [pltpu.make_async_copy(src_hbm.at[:, :, pl.ds(128 * h, 128)], own.at[h], load_sem.at[h]) for h in range(2)]
    for load in loads:
        load.start()

    around = [(1, 1), (1, -1), (-1, 1), (-1, -1), (1, 0), (-1, 0), (0, 1), (0, -1)]
    d_ok = {1: s < ns - 1, -1: s > 0, 0: None}
    y_ok = {1: y < ny - 1, -1: y > 0, 0: None}

    def there(ds, dy):
        conds = [k for k in (d_ok[ds], y_ok[dy]) if k is not None]
        return functools.reduce(jnp.logical_and, conds)

    def near(ds, dy):
        return (s + ds, y + dy)

    def head_of(x, yy):
        return (x * size + 1, yy)

    def plane(dx, dy):
        return (lax.rem(px + dx, nx) * size + 1, lax.rem(y + dy, ny))

    barrier = pltpu.get_barrier_semaphore()

    def greet(target):
        pl.semaphore_signal(barrier, inc=1, device_id=target, device_id_type=MESH)

    for o in around:
        pl.when(there(*o))(functools.partial(greet, near(*o)))

    @pl.when(is_head)
    def _():
        for o in plane_set:
            greet(plane(*o))
        for k in range(size):
            if k != 1:
                greet((px * size + k, y))

        @pl.when(y < ny - 1)
        def _():
            for k in range(size):
                greet((px * size + k, y + 1))

        @pl.when(px < nx - 1)
        def _():
            greet(((px + 1) * size, y))

    one = lambda cond: jnp.where(cond, 1, 0)
    beside = (1 + one(s > 0) + one(s < ns - 1)) * (1 + one(y > 0) + one(y < ny - 1)) - 1
    heads = one(y > 0) + one((place == 0) & (px > 0)) + jnp.where(is_head, n_plane, 1)

    blank = jnp.zeros((8, 128), F32)
    for array in (r, g, zp, z1, z0, v, g2):
        for b in range(2):
            for j in range(-1, 25):
                array[b, pl.ds(fine_row(j) + 16, 8), :] = blank
    for array in (c, e1, e2, c2, kap):
        for j in range(-1, 13):
            array[pl.ds(coarse_row(j) + 8, 8), :] = blank
    kap[pl.ds(coarse_row(7), 8), :] = blank

    def clear(cond, box):
        @pl.when(cond)
        def _():
            box[...] = jnp.zeros(box.shape, F32)

    clear(s == 0, below)
    clear(s == ns - 1, above)
    clear(y == 0, ysl)
    clear(y == 0, below.at[0])
    clear(y == 0, above.at[0])
    clear(y == ny - 1, ynl)
    clear(y == ny - 1, below.at[2])
    clear(y == ny - 1, above.at[2])

    count = cnt_ref[...]
    for h in range(2):
        loads[h].wait()
        final = own[h, 0]
        for k in range(1, 4):
            final = jnp.where(count > k, own[h, k], final)
        last[h] = final
    pl.semaphore_wait(barrier, beside + heads)

    def copy_to(src, dst, ss, rs_, target):
        return pltpu.make_async_remote_copy(
            src_ref=src, dst_ref=dst, send_sem=ss, recv_sem=rs_, device_id=target, device_id_type=MESH)

    halo = {}
    made = 0
    for o in around:
        ds, dy = o
        halo[o] = []
        for part in range(2 if dy else 1):
            half = 1 - part if dy == 1 else part
            if ds:
                src, box = (last, below.at[1 - dy]) if ds == 1 else (own.at[:, 0], above.at[1 - dy])
                if dy:
                    src, box = src.at[half], box.at[half]
                if part:
                    src, box = (ref.at[pl.ds(8 if ds == 1 else 0, 8)] for ref in (src, box))
            else:
                src, box = own.at[half], (ysl if dy == 1 else ynl).at[half]
            halo[o].append(copy_to(src, box, s1.at[made], r1.at[made], near(*o)))
            made += 1
    for part in range(2):
        for o in around:
            if part < len(halo[o]):
                pl.when(there(*o))(halo[o][part].start)

    def arrived(ds, dy, part=0):
        pl.when(there(-ds, -dy))(halo[ds, dy][part].wait_recv)

    lane = lax.broadcasted_iota(jnp.int32, (8, 128), 1)
    upper = lane >= 64
    pair = lax.rem(lane, 64)
    cnt8 = count[:8]
    end = 8 + 8 * cnt8
    alive = (pair >= 8) & (pair < end)
    lo_lane = jnp.where(s > 0, 8, 0)
    hi_lane = jnp.where(s < ns - 1, 8, 0)
    there_mask = (pair >= 8 - lo_lane) & (pair < end + hi_lane)
    mask = jnp.where(there_mask, 1.0, 0.0).astype(F32)
    outer = jnp.where(upper, jnp.where(y < ny - 1, mask, 0.0), jnp.where(y > 0, mask, 0.0))
    fine_masks = [outer * STEP, outer * STEP, mask * STEP]
    coarse_masks = [outer * QUARTER, outer * QUARTER, mask * QUARTER]
    pieces = (ysl, own, ynl)

    def assemble(block):
        for b in range(2):
            stack = []
            for m in (block, 5 - block):
                take = lambda ref, *k: ref[(*k, pl.ds(b, 8, stride=2), slice(None))]
                up = take(above, m // 2, m % 2)
                stack.append(take(below, m // 2, m % 2))
                for k in range(4):
                    mine = take(pieces[m // 2], m % 2, k)
                    stack.append(jnp.where(cnt8 == k, up, mine) if k else mine)
                stack += [up, blank, blank]
            turned = jnp.concatenate(stack, axis=0).T
            for j in range(8):
                for h in range(2):
                    low, high = turned[16 * j + 8 * h:16 * j + 8 * h + 8], turned[16 * (7 - j) + 8 * h:16 * (7 - j) + 8 * h + 8]
                    value = jnp.where(upper, high, low) * fine_masks[block]
                    r[b, pl.ds(fine_row(8 * block + j) + 8 * h, 8), :] = value
                    if block == 2 and j == 7:
                        r[b, pl.ds(fine_row(24) + 8 * h, 8), :] = pltpu.roll(value, 64, 1)

    def total(ref, b, j, h):
        i = fine_row(j) + 8 * h
        load8 = lambda k: ref[b, pl.ds(k, 8), :]
        across = ref[1 - b, pl.ds(i, 8), :]
        turned = pltpu.roll(across, 127 if b else 1, 1)
        return load8(i), ((load8(i - 24) + load8(i + 24)) + (load8(i - 1) + load8(i + 1))) + (across + turned)

    def put(dst, b, j, h, value):
        dst[b, pl.ds(fine_row(j) + 8 * h, 8), :] = value
        if j == 23:
            dst[b, pl.ds(fine_row(24) + 8 * h, 8), :] = pltpu.roll(value, 64, 1)

    def smooth(src, dst, add=None):
        def row(j):
            for b in range(2):
                for h in range(2):
                    mid, six = total(src, b, j, h)
                    value = KEEP * mid + fine_masks[j // 8] * six
                    if add is not None:
                        value = value + add[b, pl.ds(fine_row(j) + 8 * h, 8), :]
                    put(dst, b, j, h, value)
        return row

    def apply(src, dst):
        def row(j):
            for b in range(2):
                for h in range(2):
                    mid, six = total(src, b, j, h)
                    put(dst, b, j, h, OMEGA * mid - fine_masks[j // 8] * six)
        return row

    def put_coarse(dst, j, value):
        dst[pl.ds(coarse_row(j), 8), :] = value
        if j == 11:
            dst[pl.ds(coarse_row(12), 8), :] = pltpu.roll(value, 64, 1)

    def restrict(src, dst):
        def row(j):
            eight = None
            for b in range(2):
                for k in range(4):
                    part = src[b, pl.ds(fine_row(2 * j + k // 2) + k % 2, 8, stride=2), :]
                    eight = part if eight is None else eight + part
            put_coarse(dst, j, (0.125 * TAU / STEP) * eight)
        return row

    def coarse_total(ref, j):
        i = coarse_row(j)
        load8 = lambda k: ref[pl.ds(k, 8), :]
        mid = load8(i)
        sides = pltpu.roll(mid, 1, 1) + pltpu.roll(mid, 127, 1)
        return mid, ((load8(i - 16) + load8(i + 16)) + (load8(i - 1) + load8(i + 1))) + sides

    def coarse_first(rhs, dst):
        def row(j):
            mid, six = coarse_total(rhs, j)
            put_coarse(dst, j, (1.0 + KEEP) * mid + coarse_masks[j // 4] * six)
        return row

    def coarse_sweep(rhs, src, dst):
        def row(j):
            mid, six = coarse_total(src, j)
            put_coarse(dst, j, (KEEP * mid + rhs[pl.ds(coarse_row(j), 8), :]) + coarse_masks[j // 4] * six)
        return row

    def corrected(rhs, first, coarse, dst):
        def row(j):
            add = coarse[pl.ds(coarse_row(j), 8), :]
            for b in range(2):
                for k in range(4):
                    fine_j = 2 * j + k // 2
                    at = pl.ds(fine_row(fine_j) + k % 2, 8, stride=2)
                    value = (rhs[b, at, :] + first[b, at, :]) + add
                    dst[b, at, :] = value
                    if fine_j == 23:
                        dst[b, pl.ds(fine_row(24) + k % 2, 8, stride=2), :] = pltpu.roll(value, 64, 1)
        return row

    def rows(fn, lo, hi):
        for j in reversed(range(lo, hi)):
            fn(j)

    shrink = lambda lo: lo + 1
    halve = lambda lo: -(-lo // 2)
    double = lambda lo: 2 * lo
    stages = [
        ("g", "r", shrink, smooth(r, g)), ("q", "g", shrink, smooth(g, q)),
        ("c", "q", halve, restrict(q, c)), ("e1", "c", shrink, coarse_first(c, e1)),
        ("e2", "e1", shrink, coarse_sweep(c, e1, e2)), ("e3", "e2", shrink, coarse_sweep(c, e2, e3)),
        ("zp", "e3", double, corrected(r, g, e3, zp)), ("z1", "zp", shrink, smooth(zp, z1, r)),
        ("z0", "z1", shrink, smooth(z1, z0, r)), ("v", "z0", shrink, apply(z0, v)),
        ("g2", "v", shrink, smooth(v, g2)), ("q2", "g2", shrink, smooth(g2, q2)),
        ("c2", "q2", halve, restrict(q2, c2)),
    ]
    coarse_names = ("c", "e1", "e2", "e3", "c2")
    done = {}

    def advance(lo):
        have = {"r": lo}
        for name, source, change, fn in stages:
            start = max(change(have[source]), NEED[name])
            stop = done.get(name, 12 if name in coarse_names else 24)
            if start >= stop:
                break
            have[name] = done[name] = start
            if name == "zp":
                rows(fn, start // 2, stop // 2)
            else:
                rows(fn, start, stop)

    arrived(1, 0)
    arrived(-1, 0)
    assemble(2)
    advance(16)
    for dy in (1, -1):
        for ds in (1, -1, 0):
            arrived(ds, dy, 0)
    assemble(1)
    advance(8)
    for dy in (1, -1):
        for ds in (1, -1, 0):
            arrived(ds, dy, 1)
    assemble(0)
    advance(0)

    rz = curv = fine = coarse = blank
    for j in range(16, 24):
        for b in range(2):
            for h in range(2):
                at = (b, pl.ds(fine_row(j) + 8 * h, 8))
                vy, gy, qy, zy = v[at], g2[at], q2[at], z0[at]
                rz = rz + r[at] * zy
                curv = curv + zy * vy
                fine = fine + (vy * ((vy + gy) + qy) + gy * qy)
    for j in range(8, 12):
        mid, six = coarse_total(c2, j)
        put_coarse(kap, j, jnp.where(alive, KEEP * mid + coarse_masks[2] * six, 0.0))
    for j in range(8, 12):
        k, six = coarse_total(kap, j)
        cc = c2[pl.ds(coarse_row(j), 8), :]
        coarse = coarse + (cc * (cc + k) + k * ((1.0 + KEEP) * k + QUARTER * six))
    column = lambda value: jnp.sum(jnp.where(alive, value, 0.0), axis=0, keepdims=True)
    inner = jnp.concatenate([kap[pl.ds(coarse_row(j), 8), :] for j in range(8, 12)], axis=0)
    turned = jnp.concatenate([inner] * 4, axis=0).T
    cnt1, lane1 = cnt8[:1], lane[:1]
    ends = []
    for h in (0, 64):
        tail = turned[h + 15:h + 16]
        for k in range(2, 5):
            tail = jnp.where(cnt1 == k, turned[h + 7 + 8 * k:h + 8 + 8 * k], tail)
        ends.append((turned[h + 8:h + 9], tail))
    d_face = jnp.where(lane1 < 64, jnp.where(lane1 < 32, ends[0][0], ends[1][0]),
                       jnp.where(lane1 < 96, ends[0][1], ends[1][1]))
    sides = kap[pl.ds(coarse_row(8), 8), :]
    swapped = pltpu.roll(sides, 64, 1)
    north_face = jnp.where(upper[:4], sides[:4], swapped[4:])
    south_face = jnp.where(upper[:4], swapped[:4], sides[4:])
    msg[...] = jnp.concatenate(
        [column(rz), column(curv), (1.0 / STEP) * column(fine) + (8.0 / TAU) * column(coarse), d_face, north_face],
        axis=0)
    face[...] = south_face
    faces[...] = d_face

    order = [0] + list(range(2, size)) + [1]
    box = jnp.where(place > 1, place - 1, 0)
    box = jnp.where(is_head, size - 1, box)
    to_head = copy_to(msg, hb.at[pl.ds(pl.multiple_of(8 * box, 8), 8)], sm.at[0], rb, head_of(px, y))
    to_south = copy_to(face, hs.at[pl.ds(pl.multiple_of(4 * box, 4), 4)], sm.at[1], rs, head_of(px, y - 1))
    to_back = copy_to(faces, hx, sm.at[2], rx, head_of(px - 1, y))
    pl.when(jnp.logical_not(is_head))(to_head.start)
    pl.when(y > 0)(to_south.start)
    pl.when((place == 0) & (px > 0))(to_back.start)

    mine = jnp.concatenate([c2[pl.ds(coarse_row(j), 8), :] for j in range(8, 12)], axis=0)
    four = lambda x: jnp.concatenate([x] * 4, axis=0)
    cnt32, alive32 = four(cnt8), four(alive)

    def shifted(value, sign):
        out = pltpu.roll(value, (8 * sign) % 128, 1)
        for k in range(2, 5):
            out = jnp.where(cnt32 == k, pltpu.roll(value, (8 * k * sign) % 128, 1), out)
        return out

    cd[0] = shifted(mine, -1)
    cu[0] = mine
    along = [copy_to(cd.at[0], cd.at[1], s2.at[0], r2.at[0], near(1, 0)),
             copy_to(cu.at[0], cu.at[1], s2.at[1], r2.at[1], near(-1, 0))]
    pl.when(s < ns - 1)(along[0].start)
    pl.when(s > 0)(along[1].start)

    pl.when(s > 0)(along[0].wait_recv)
    pl.when(s < ns - 1)(along[1].wait_recv)
    lo32 = four((pair >= 8 - lo_lane) & (pair < 8))
    hi32 = four((pair >= end) & (pair < end + hi_lane))
    ca[...] = jnp.where(alive32, mine, jnp.where(lo32, cd[1], jnp.where(hi32, shifted(cu[1], 1), 0.0)))
    across = [copy_to(ca, cn, s2.at[2], r2.at[2], near(0, -1)),
              copy_to(ca, cs, s2.at[3], r2.at[3], near(0, 1))]
    pl.when(y > 0)(across[0].start)
    pl.when(y < ny - 1)(across[1].start)

    lines = copy_to(hb.at[pl.ds(0, 8 * (size - 1))], hb.at[pl.ds(0, 8 * (size - 1))], sm.at[0], rb, head_of(px, y))
    beyond = copy_to(hs, hs, sm.at[1], rs, head_of(px, y))
    rounds = copy_to(hall.at[pl.ds(0, n_plane)], hall.at[pl.ds(0, n_plane)], sh, rh, head_of(px, y))

    def round_of(k):
        return copy_to(hall.at[n_plane], hall.at[k], sh, rh, plane(*plane_set[k]))

    @pl.when(is_head)
    def _():
        hb[pl.ds(8 * (size - 1), 8), :] = msg[...]
        lines.wait_recv()
        pl.when(y < ny - 1)(beyond.wait_recv)
        pl.when(px < nx - 1)(to_back.wait_recv)
        acc = hb[pl.ds(0, 8), :]
        for k in range(1, size):
            acc = acc + hb[pl.ds(8 * k, 8), :]
        cross = jnp.zeros((4, 128), F32)
        for k in range(size):
            cross = cross + hb[pl.ds(8 * k + 4, 4), :] * hs[pl.ds(4 * k, 4), :]
        cross = jnp.where(y < ny - 1, jnp.sum(cross, axis=0, keepdims=True), 0.0)
        where_is = {p: k for k, p in enumerate(order)}
        front = hb[pl.ds(3, size, stride=8), :]
        back = pltpu.roll(front, 64, 1)
        row_of = lambda value, p: value[where_is[p]:where_is[p] + 1]
        chain = jnp.where(px < nx - 1, row_of(back, size - 1) * hx[...], 0.0)
        chain = chain + row_of(back, 0) * row_of(front, 1) + row_of(back, 1) * row_of(front, 2)
        run = back[1:size - 2] * hb[pl.ds(19, size - 3, stride=8), :]
        chain = chain + jnp.sum(run, axis=0, keepdims=True)
        cross = cross + jnp.where(lane1 < 64, chain, 0.0)
        three = jnp.concatenate([acc[:2], acc[2:3] + 4.0 * cross], axis=0)
        sums = jnp.sum(three, axis=1, keepdims=True)
        hall[n_plane] = jnp.where(lane1 == 0, sums[:1], jnp.where(lane1 == 1, sums[1:2], sums[2:]))
        for k in range(n_plane):
            round_of(k).start()

    def turn_back(src, dst):
        for b in range(2):
            stack = []
            for j in range(8):
                for h in range(2):
                    low, high = src[b, pl.ds(fine_row(16 + j) + 8 * h, 8), :], src[b, pl.ds(fine_row(23 - j) + 8 * h, 8), :]
                    stack.append(jnp.where(alive, jnp.where(upper, high, low), 0.0))
            x = jnp.concatenate(stack, axis=0).T
            for h in range(2):
                for k in range(4):
                    at = 64 * h + 8 * (k + 1)
                    dst[h, k, pl.ds(b, 8, stride=2), :] = x[at:at + 8]

    turn_back(z0, zt)
    turn_back(v, vt)

    pl.when(y > 0)(across[1].wait_recv)
    pl.when(y < ny - 1)(across[0].wait_recv)
    for j in range(4, 12):
        if j < 8:
            at = pl.ds(8 * (7 - j), 8)
            south = jnp.where(y > 0, pltpu.roll(cs[at, :], 64, 1), 0.0)
            north = jnp.where(y < ny - 1, pltpu.roll(cn[at, :], 64, 1), 0.0)
            put_coarse(c, j, jnp.where(upper, north, south))
        else:
            put_coarse(c, j, ca[pl.ds(8 * (j - 8), 8), :])
    rows(coarse_first(c, e1), 5, 12)
    rows(coarse_sweep(c, e1, e2), 6, 12)
    rows(coarse_sweep(c, e2, e3), 7, 12)
    rows(corrected(v, g2, e3, zp), 7, 12)
    rows(smooth(zp, z1, v), 15, 24)
    rows(smooth(z1, w, v), 16, 24)
    turn_back(w, wt)

    def news(k):
        return copy_to(hrow, tot, st, rt, (px * size + k, y))

    @pl.when(is_head)
    def _():
        rounds.wait_recv()
        hrow[...] = jnp.sum(hall[...], axis=0)
        for k in range(size):
            if k != 1:
                news(k).start()
        tot[...] = hrow[...]

    pl.when(jnp.logical_not(is_head))(news(0).wait_recv)
    sums = tot[...]
    pick = lambda k: jnp.broadcast_to(sums[:, k:k + 1], (1, 128))
    rz_all, curv_all, w_all = pick(0), pick(1), pick(2)
    alpha = rz_all / curv_all
    beta = alpha * (w_all / (curv_all * (1.0 / STEP)))
    scaled = alpha * (1.0 / STEP)
    for k in range(4):
        for half in range(2):
            at = pl.ds(128 * half, 128)
            zk = zt[half, k]
            sol_ref[k, :, at] = alpha * zk
            res_ref[k, :, at] = jnp.where(count > k, own[half, k], 0.0) - scaled * vt[half, k]
            dir_ref[k, :, at] = beta * zk - alpha * wt[half, k]

    for o in around:
        for copy in halo[o]:
            pl.when(there(*o))(copy.wait_send)
    pl.when(jnp.logical_not(is_head))(to_head.wait_send)
    pl.when(y > 0)(to_south.wait_send)
    pl.when((place == 0) & (px > 0))(to_back.wait_send)
    pl.when(s < ns - 1)(along[0].wait_send)
    pl.when(s > 0)(along[1].wait_send)
    pl.when(y > 0)(across[0].wait_send)
    pl.when(y < ny - 1)(across[1].wait_send)
    told = copy_to(hall.at[pl.ds(0, size - 1)], hall.at[pl.ds(0, size - 1)], st, rt, head_of(px, y))

    @pl.when(is_head)
    def _():
        rounds.wait_send()
        told.wait_send()


def flush(*refs):
    sources, targets, sem = refs[:3], refs[3:6], refs[6]
    copies = [pltpu.make_async_copy(a, b, sem.at[k]) for k, (a, b) in enumerate(zip(sources, targets))]
    for copy in copies:
        copy.start()
    for copy in copies:
        copy.wait()


def solution(mesh):
    ns, ny = mesh.shape["sfc"], mesh.shape["grp"]
    nx, nz, nc = SHAPES[ns]
    size, n_plane = nz * nc, nx * ny - 1
    dma = pltpu.SemaphoreType.DMA
    block = jax.ShapeDtypeStruct((4, E, 16 * E), F32)
    vmem = pl.BlockSpec(memory_space=pltpu.VMEM)
    hbm = pl.BlockSpec(memory_space=pltpu.HBM)
    slots = lambda *k: pltpu.VMEM((*k, E, 128), F32)
    fine = pltpu.VMEM((2, FINE, 128), F32)
    coarse = pltpu.VMEM((COARSE, 128), F32)
    line = lambda *k: pltpu.VMEM((*k, 128), F32)

    def shards(source, layer_counts):
        counts = jnp.broadcast_to(layer_counts.reshape(1, 1), (16, 128))
        parts = pl.pallas_call(
            functools.partial(kernel, (nx, nz, nc, ny)),
            out_shape=(block, block, block),
            in_specs=[hbm, vmem],
            out_specs=(vmem, vmem, vmem),
            scratch_shapes=[
                slots(2, 4), slots(2), slots(2, 4), slots(2, 4), slots(3, 2), slots(3, 2), *[fine] * 10,
                *[coarse] * 6, line(2, 32), line(2, 32), line(32), line(32), line(32),
                slots(2, 4), slots(2, 4), slots(2, 4),
                line(8), line(4), line(1), line(8 * size), line(4 * size), line(1), line(n_plane + 1, 1),
                line(1), line(1),
                dma((2,)), dma((14,)), dma((14,)), dma((4,)), dma((4,)), dma((3,)), dma, dma,
                dma, dma, dma, dma, dma,
            ],
            compiler_params=pltpu.CompilerParams(
                collective_id=0, has_side_effects=True, vmem_limit_bytes=24 << 20),
        )(pltpu.with_memory_space_constraint(source, pltpu.HBM), counts)
        return pl.pallas_call(
            flush, out_shape=(block, block, block), in_specs=[vmem] * 3, out_specs=(hbm,) * 3,
            scratch_shapes=[dma((3,))],
            compiler_params=pltpu.CompilerParams(vmem_limit_bytes=1 << 20),
        )(*parts)

    spec = P("sfc", None, "grp")
    return jax.shard_map(
        shards, mesh=mesh, in_specs=(spec, P("sfc")), out_specs=(spec, spec, spec), check_vma=False)
```

```python
import functools

import jax
import jax.numpy as jnp
from jax import lax
from jax.experimental import pallas as pl
from jax.experimental.pallas import tpu as pltpu
from jax.sharding import PartitionSpec as P

E = 16
OMEGA = 2.0 / 3.0
STEP = OMEGA / 6.0
KEEP = 1.0 - OMEGA
TAU = OMEGA / 1.5
QUARTER = TAU / 4.0
SHAPES = {96: (4, 12, 2), 8: (2, 2, 2)}
MESH = pl.DeviceIdType.MESH
F32 = jnp.float32
FINE = 8 + 24 * 25
COARSE = 8 + 16 * 13
NEED = dict(g=1, q=2, c=1, e1=2, e2=3, e3=4, zp=8, z1=10, z0=11, v=12, g2=13, q2=14, c2=7)


def others(*axes):
    found = [()]
    for count in axes:
        found = [f + (i,) for f in found for i in range(count)]
    far = lambda f: -sum(min(i, n - i) for i, n in zip(f, axes))
    return sorted([f for f in found if any(f)], key=far)


def fine_row(j):
    return 8 + 24 * j


def coarse_row(j):
    return 8 + 16 * j


def body(dims, src_hbm, cnt_ref, sol_ref, res_ref, dir_ref, scratch, s1, s2, sm, sh, st, load_sem):
    nx, nz, nc, ny = dims
    (own, last, ysl, ynl, below, above, r, g, q, zp, z1, z0, v, g2, q2, w,
     c, e1, e2, e3, c2, kap, cd, cu, ca, cs, cn, zt, vt, wt,
     msg, face, faces, hb, hs, hx, hall, hrow, tot,
     r1, r2, rb, rs, rx, rh, rt) = scratch
    s = lax.axis_index("sfc")
    y = lax.axis_index("grp")
    ns, size = nx * nz * nc, nz * nc
    px, place = s // size, lax.rem(s, size)
    is_head = place == 1
    plane_set = others(nx, ny)
    n_plane = len(plane_set)

    loads = [pltpu.make_async_copy(src_hbm.at[:, :, pl.ds(128 * h, 128)], own.at[h], load_sem.at[h]) for h in range(2)]
    for load in loads:
        load.start()

    around = [(1, 1), (1, -1), (-1, 1), (-1, -1), (1, 0), (-1, 0), (0, 1), (0, -1)]
    d_ok = {1: s < ns - 1, -1: s > 0, 0: None}
    y_ok = {1: y < ny - 1, -1: y > 0, 0: None}

    def there(ds, dy):
        conds = [k for k in (d_ok[ds], y_ok[dy]) if k is not None]
        return functools.reduce(jnp.logical_and, conds)

    def near(ds, dy):
        return (s + ds, y + dy)

    def head_of(x, yy):
        return (x * size + 1, yy)

    def plane(dx, dy):
        return (lax.rem(px + dx, nx) * size + 1, lax.rem(y + dy, ny))

    barrier = pltpu.get_barrier_semaphore()

    def greet(target):
        pl.semaphore_signal(barrier, inc=1, device_id=target, device_id_type=MESH)

    for o in around:
        pl.when(there(*o))(functools.partial(greet, near(*o)))

    @pl.when(is_head)
    def _():
        for o in plane_set:
            greet(plane(*o))
        for k in range(size):
            if k != 1:
                greet((px * size + k, y))

        @pl.when(y < ny - 1)
        def _():
            for k in range(size):
                greet((px * size + k, y + 1))

        @pl.when(px < nx - 1)
        def _():
            greet(((px + 1) * size, y))

    one = lambda cond: jnp.where(cond, 1, 0)
    beside = (1 + one(s > 0) + one(s < ns - 1)) * (1 + one(y > 0) + one(y < ny - 1)) - 1
    heads = one(y > 0) + one((place == 0) & (px > 0)) + jnp.where(is_head, n_plane, 1)

    blank = jnp.zeros((8, 128), F32)
    for array in (r, g, zp, z1, z0, v, g2):
        for b in range(2):
            for j in range(-1, 25):
                array[b, pl.ds(fine_row(j) + 16, 8), :] = blank
    for array in (c, e1, e2, c2, kap):
        for j in range(-1, 13):
            array[pl.ds(coarse_row(j) + 8, 8), :] = blank
    kap[pl.ds(coarse_row(7), 8), :] = blank

    def clear(cond, box):
        @pl.when(cond)
        def _():
            box[...] = jnp.zeros(box.shape, F32)

    clear(s == 0, below)
    clear(s == ns - 1, above)
    clear(y == 0, ysl)
    clear(y == 0, below.at[0])
    clear(y == 0, above.at[0])
    clear(y == ny - 1, ynl)
    clear(y == ny - 1, below.at[2])
    clear(y == ny - 1, above.at[2])

    count = cnt_ref[...]
    for h in range(2):
        loads[h].wait()
        final = own[h, 0]
        for k in range(1, 4):
            final = jnp.where(count > k, own[h, k], final)
        last[h] = final
    pl.semaphore_wait(barrier, beside + heads)

    def copy_to(src, dst, ss, rs_, target):
        return pltpu.make_async_remote_copy(
            src_ref=src, dst_ref=dst, send_sem=ss, recv_sem=rs_, device_id=target, device_id_type=MESH)

    halo = {}
    made = 0
    for o in around:
        ds, dy = o
        halo[o] = []
        for part in range(2 if dy else 1):
            half = 1 - part if dy == 1 else part
            if ds:
                src, box = (last, below.at[1 - dy]) if ds == 1 else (own.at[:, 0], above.at[1 - dy])
                if dy:
                    src, box = src.at[half], box.at[half]
                if part:
                    src, box = (ref.at[pl.ds(8 if ds == 1 else 0, 8)] for ref in (src, box))
            else:
                src, box = own.at[half], (ysl if dy == 1 else ynl).at[half]
            halo[o].append(copy_to(src, box, s1.at[made], r1.at[made], near(*o)))
            made += 1
    for part in range(2):
        for o in around:
            if part < len(halo[o]):
                pl.when(there(*o))(halo[o][part].start)

    def arrived(ds, dy, part=0):
        pl.when(there(-ds, -dy))(halo[ds, dy][part].wait_recv)

    lane = lax.broadcasted_iota(jnp.int32, (8, 128), 1)
    upper = lane >= 64
    pair = lax.rem(lane, 64)
    cnt8 = count[:8]
    end = 8 + 8 * cnt8
    alive = (pair >= 8) & (pair < end)
    lo_lane = jnp.where(s > 0, 8, 0)
    hi_lane = jnp.where(s < ns - 1, 8, 0)
    there_mask = (pair >= 8 - lo_lane) & (pair < end + hi_lane)
    mask = jnp.where(there_mask, 1.0, 0.0).astype(F32)
    outer = jnp.where(upper, jnp.where(y < ny - 1, mask, 0.0), jnp.where(y > 0, mask, 0.0))
    fine_masks = [outer * STEP, outer * STEP, mask * STEP]
    coarse_masks = [outer * QUARTER, outer * QUARTER, mask * QUARTER]
    pieces = (ysl, own, ynl)

    def assemble(block):
        for b in range(2):
            stack = []
            for m in (block, 5 - block):
                take = lambda ref, *k: ref[(*k, pl.ds(b, 8, stride=2), slice(None))]
                up = take(above, m // 2, m % 2)
                stack.append(take(below, m // 2, m % 2))
                for k in range(4):
                    mine = take(pieces[m // 2], m % 2, k)
                    stack.append(jnp.where(cnt8 == k, up, mine) if k else mine)
                stack += [up, blank, blank]
            turned = jnp.concatenate(stack, axis=0).T
            for j in range(8):
                for h in range(2):
                    low, high = turned[16 * j + 8 * h:16 * j + 8 * h + 8], turned[16 * (7 - j) + 8 * h:16 * (7 - j) + 8 * h + 8]
                    value = jnp.where(upper, high, low) * fine_masks[block]
                    r[b, pl.ds(fine_row(8 * block + j) + 8 * h, 8), :] = value
                    if block == 2 and j == 7:
                        r[b, pl.ds(fine_row(24) + 8 * h, 8), :] = pltpu.roll(value, 64, 1)

    def total(ref, b, j, h):
        i = fine_row(j) + 8 * h
        load8 = lambda k: ref[b, pl.ds(k, 8), :]
        across = ref[1 - b, pl.ds(i, 8), :]
        turned = pltpu.roll(across, 127 if b else 1, 1)
        return load8(i), ((load8(i - 24) + load8(i + 24)) + (load8(i - 1) + load8(i + 1))) + (across + turned)

    def put(dst, b, j, h, value):
        dst[b, pl.ds(fine_row(j) + 8 * h, 8), :] = value
        if j == 23:
            dst[b, pl.ds(fine_row(24) + 8 * h, 8), :] = pltpu.roll(value, 64, 1)

    def smooth(src, dst, add=None):
        def row(j):
            for b in range(2):
                for h in range(2):
                    mid, six = total(src, b, j, h)
                    value = KEEP * mid + fine_masks[j // 8] * six
                    if add is not None:
                        value = value + add[b, pl.ds(fine_row(j) + 8 * h, 8), :]
                    put(dst, b, j, h, value)
        return row

    def apply(src, dst):
        def row(j):
            for b in range(2):
                for h in range(2):
                    mid, six = total(src, b, j, h)
                    put(dst, b, j, h, OMEGA * mid - fine_masks[j // 8] * six)
        return row

    def put_coarse(dst, j, value):
        dst[pl.ds(coarse_row(j), 8), :] = value
        if j == 11:
            dst[pl.ds(coarse_row(12), 8), :] = pltpu.roll(value, 64, 1)

    def restrict(src, dst):
        def row(j):
            eight = None
            for b in range(2):
                for k in range(4):
                    part = src[b, pl.ds(fine_row(2 * j + k // 2) + k % 2, 8, stride=2), :]
                    eight = part if eight is None else eight + part
            put_coarse(dst, j, (0.125 * TAU / STEP) * eight)
        return row

    def coarse_total(ref, j):
        i = coarse_row(j)
        load8 = lambda k: ref[pl.ds(k, 8), :]
        mid = load8(i)
        sides = pltpu.roll(mid, 1, 1) + pltpu.roll(mid, 127, 1)
        return mid, ((load8(i - 16) + load8(i + 16)) + (load8(i - 1) + load8(i + 1))) + sides

    def coarse_first(rhs, dst):
        def row(j):
            mid, six = coarse_total(rhs, j)
            put_coarse(dst, j, (1.0 + KEEP) * mid + coarse_masks[j // 4] * six)
        return row

    def coarse_sweep(rhs, src, dst):
        def row(j):
            mid, six = coarse_total(src, j)
            put_coarse(dst, j, (KEEP * mid + rhs[pl.ds(coarse_row(j), 8), :]) + coarse_masks[j // 4] * six)
        return row

    def corrected(rhs, first, coarse, dst):
        def row(j):
            add = coarse[pl.ds(coarse_row(j), 8), :]
            for b in range(2):
                for k in range(4):
                    fine_j = 2 * j + k // 2
                    at = pl.ds(fine_row(fine_j) + k % 2, 8, stride=2)
                    value = (rhs[b, at, :] + first[b, at, :]) + add
                    dst[b, at, :] = value
                    if fine_j == 23:
                        dst[b, pl.ds(fine_row(24) + k % 2, 8, stride=2), :] = pltpu.roll(value, 64, 1)
        return row

    def rows(fn, lo, hi):
        for j in reversed(range(lo, hi)):
            fn(j)

    shrink = lambda lo: lo + 1
    halve = lambda lo: -(-lo // 2)
    double = lambda lo: 2 * lo
    stages = [
        ("g", "r", shrink, smooth(r, g)), ("q", "g", shrink, smooth(g, q)),
        ("c", "q", halve, restrict(q, c)), ("e1", "c", shrink, coarse_first(c, e1)),
        ("e2", "e1", shrink, coarse_sweep(c, e1, e2)), ("e3", "e2", shrink, coarse_sweep(c, e2, e3)),
        ("zp", "e3", double, corrected(r, g, e3, zp)), ("z1", "zp", shrink, smooth(zp, z1, r)),
        ("z0", "z1", shrink, smooth(z1, z0, r)), ("v", "z0", shrink, apply(z0, v)),
        ("g2", "v", shrink, smooth(v, g2)), ("q2", "g2", shrink, smooth(g2, q2)),
        ("c2", "q2", halve, restrict(q2, c2)),
    ]
    coarse_names = ("c", "e1", "e2", "e3", "c2")
    done = {}

    def advance(lo):
        have = {"r": lo}
        for name, source, change, fn in stages:
            start = max(change(have[source]), NEED[name])
            stop = done.get(name, 12 if name in coarse_names else 24)
            if start >= stop:
                break
            have[name] = done[name] = start
            if name == "zp":
                rows(fn, start // 2, stop // 2)
            else:
                rows(fn, start, stop)

    arrived(1, 0)
    arrived(-1, 0)
    assemble(2)
    advance(16)
    for dy in (1, -1):
        for ds in (1, -1, 0):
            arrived(ds, dy, 0)
    assemble(1)
    advance(8)
    for dy in (1, -1):
        for ds in (1, -1, 0):
            arrived(ds, dy, 1)
    assemble(0)
    advance(0)

    rz = curv = fine = coarse = blank
    for j in range(16, 24):
        for b in range(2):
            for h in range(2):
                at = (b, pl.ds(fine_row(j) + 8 * h, 8))
                vy, gy, qy, zy = v[at], g2[at], q2[at], z0[at]
                rz = rz + r[at] * zy
                curv = curv + zy * vy
                fine = fine + (vy * ((vy + gy) + qy) + gy * qy)
    for j in range(8, 12):
        mid, six = coarse_total(c2, j)
        put_coarse(kap, j, jnp.where(alive, KEEP * mid + coarse_masks[2] * six, 0.0))
    for j in range(8, 12):
        k, six = coarse_total(kap, j)
        cc = c2[pl.ds(coarse_row(j), 8), :]
        coarse = coarse + (cc * (cc + k) + k * ((1.0 + KEEP) * k + QUARTER * six))
    column = lambda value: jnp.sum(jnp.where(alive, value, 0.0), axis=0, keepdims=True)
    inner = jnp.concatenate([kap[pl.ds(coarse_row(j), 8), :] for j in range(8, 12)], axis=0)
    turned = jnp.concatenate([inner] * 4, axis=0).T
    cnt1, lane1 = cnt8[:1], lane[:1]
    ends = []
    for h in (0, 64):
        tail = turned[h + 15:h + 16]
        for k in range(2, 5):
            tail = jnp.where(cnt1 == k, turned[h + 7 + 8 * k:h + 8 + 8 * k], tail)
        ends.append((turned[h + 8:h + 9], tail))
    d_face = jnp.where(lane1 < 64, jnp.where(lane1 < 32, ends[0][0], ends[1][0]),
                       jnp.where(lane1 < 96, ends[0][1], ends[1][1]))
    sides = kap[pl.ds(coarse_row(8), 8), :]
    swapped = pltpu.roll(sides, 64, 1)
    north_face = jnp.where(upper[:4], sides[:4], swapped[4:])
    south_face = jnp.where(upper[:4], swapped[:4], sides[4:])
    msg[...] = jnp.concatenate(
        [column(rz), column(curv), (1.0 / STEP) * column(fine) + (8.0 / TAU) * column(coarse), d_face, north_face],
        axis=0)
    face[...] = south_face
    faces[...] = d_face

    order = [0] + list(range(2, size)) + [1]
    box = jnp.where(place > 1, place - 1, 0)
    box = jnp.where(is_head, size - 1, box)
    to_head = copy_to(msg, hb.at[pl.ds(pl.multiple_of(8 * box, 8), 8)], sm.at[0], rb, head_of(px, y))
    to_south = copy_to(face, hs.at[pl.ds(pl.multiple_of(4 * box, 4), 4)], sm.at[1], rs, head_of(px, y - 1))
    to_back = copy_to(faces, hx, sm.at[2], rx, head_of(px - 1, y))
    pl.when(jnp.logical_not(is_head))(to_head.start)
    pl.when(y > 0)(to_south.start)
    pl.when((place == 0) & (px > 0))(to_back.start)

    mine = jnp.concatenate([c2[pl.ds(coarse_row(j), 8), :] for j in range(8, 12)], axis=0)
    four = lambda x: jnp.concatenate([x] * 4, axis=0)
    cnt32, alive32 = four(cnt8), four(alive)

    def shifted(value, sign):
        out = pltpu.roll(value, (8 * sign) % 128, 1)
        for k in range(2, 5):
            out = jnp.where(cnt32 == k, pltpu.roll(value, (8 * k * sign) % 128, 1), out)
        return out

    cd[0] = shifted(mine, -1)
    cu[0] = mine
    along = [copy_to(cd.at[0], cd.at[1], s2.at[0], r2.at[0], near(1, 0)),
             copy_to(cu.at[0], cu.at[1], s2.at[1], r2.at[1], near(-1, 0))]
    pl.when(s < ns - 1)(along[0].start)
    pl.when(s > 0)(along[1].start)

    pl.when(s > 0)(along[0].wait_recv)
    pl.when(s < ns - 1)(along[1].wait_recv)
    lo32 = four((pair >= 8 - lo_lane) & (pair < 8))
    hi32 = four((pair >= end) & (pair < end + hi_lane))
    ca[...] = jnp.where(alive32, mine, jnp.where(lo32, cd[1], jnp.where(hi32, shifted(cu[1], 1), 0.0)))
    across = [copy_to(ca, cn, s2.at[2], r2.at[2], near(0, -1)),
              copy_to(ca, cs, s2.at[3], r2.at[3], near(0, 1))]
    pl.when(y > 0)(across[0].start)
    pl.when(y < ny - 1)(across[1].start)

    lines = copy_to(hb.at[pl.ds(0, 8 * (size - 1))], hb.at[pl.ds(0, 8 * (size - 1))], sm.at[0], rb, head_of(px, y))
    beyond = copy_to(hs, hs, sm.at[1], rs, head_of(px, y))
    rounds = copy_to(hall.at[pl.ds(0, n_plane)], hall.at[pl.ds(0, n_plane)], sh, rh, head_of(px, y))

    def round_of(k):
        return copy_to(hall.at[n_plane], hall.at[k], sh, rh, plane(*plane_set[k]))

    @pl.when(is_head)
    def _():
        hb[pl.ds(8 * (size - 1), 8), :] = msg[...]
        lines.wait_recv()
        pl.when(y < ny - 1)(beyond.wait_recv)
        pl.when(px < nx - 1)(to_back.wait_recv)
        acc = hb[pl.ds(0, 8), :]
        for k in range(1, size):
            acc = acc + hb[pl.ds(8 * k, 8), :]
        cross = jnp.zeros((4, 128), F32)
        for k in range(size):
            cross = cross + hb[pl.ds(8 * k + 4, 4), :] * hs[pl.ds(4 * k, 4), :]
        cross = jnp.where(y < ny - 1, jnp.sum(cross, axis=0, keepdims=True), 0.0)
        where_is = {p: k for k, p in enumerate(order)}
        front = hb[pl.ds(3, size, stride=8), :]
        back = pltpu.roll(front, 64, 1)
        row_of = lambda value, p: value[where_is[p]:where_is[p] + 1]
        chain = jnp.where(px < nx - 1, row_of(back, size - 1) * hx[...], 0.0)
        chain = chain + row_of(back, 0) * row_of(front, 1) + row_of(back, 1) * row_of(front, 2)
        run = back[1:size - 2] * hb[pl.ds(19, size - 3, stride=8), :]
        chain = chain + jnp.sum(run, axis=0, keepdims=True)
        cross = cross + jnp.where(lane1 < 64, chain, 0.0)
        three = jnp.concatenate([acc[:2], acc[2:3] + 4.0 * cross], axis=0)
        sums = jnp.sum(three, axis=1, keepdims=True)
        hall[n_plane] = jnp.where(lane1 == 0, sums[:1], jnp.where(lane1 == 1, sums[1:2], sums[2:]))
        for k in range(n_plane):
            round_of(k).start()

    def turn_back(src, dst):
        for b in range(2):
            stack = []
            for j in range(8):
                for h in range(2):
                    low, high = src[b, pl.ds(fine_row(16 + j) + 8 * h, 8), :], src[b, pl.ds(fine_row(23 - j) + 8 * h, 8), :]
                    stack.append(jnp.where(alive, jnp.where(upper, high, low), 0.0))
            x = jnp.concatenate(stack, axis=0).T
            for h in range(2):
                for k in range(4):
                    at = 64 * h + 8 * (k + 1)
                    dst[h, k, pl.ds(b, 8, stride=2), :] = x[at:at + 8]

    turn_back(z0, zt)
    turn_back(v, vt)

    pl.when(y > 0)(across[1].wait_recv)
    pl.when(y < ny - 1)(across[0].wait_recv)
    for j in range(4, 12):
        if j < 8:
            at = pl.ds(8 * (7 - j), 8)
            south = jnp.where(y > 0, pltpu.roll(cs[at, :], 64, 1), 0.0)
            north = jnp.where(y < ny - 1, pltpu.roll(cn[at, :], 64, 1), 0.0)
            put_coarse(c, j, jnp.where(upper, north, south))
        else:
            put_coarse(c, j, ca[pl.ds(8 * (j - 8), 8), :])
    rows(coarse_first(c, e1), 5, 12)
    rows(coarse_sweep(c, e1, e2), 6, 12)
    rows(coarse_sweep(c, e2, e3), 7, 12)
    rows(corrected(v, g2, e3, zp), 7, 12)
    rows(smooth(zp, z1, v), 15, 24)
    rows(smooth(z1, w, v), 16, 24)
    turn_back(w, wt)

    def news(k, yy):
        return copy_to(hrow, tot, st, rt, (px * size + k, yy))

    is_first = is_head & (px == 0) & (y == 0)
    tells = is_head & jnp.logical_not(is_first)
    tells_two = is_head & (px == 0) & (y == 1)

    @pl.when(is_head)
    def _():
        rounds.wait_recv()
        total_row = jnp.sum(hall[...], axis=0)
        hrow[...] = total_row
        tot[...] = total_row

    @pl.when(tells_two)
    def _():
        for k in list(range(2, size)) + [0]:
            news(k, 0).start()

    @pl.when(tells)
    def _():
        for k in [0] + list(range(2, size)):
            news(k, y).start()

    pl.when(jnp.logical_not(is_head))(news(0, y).wait_recv)
    sums = tot[...]
    pick = lambda k: jnp.broadcast_to(sums[:, k:k + 1], (1, 128))
    rz_all, curv_all, w_all = pick(0), pick(1), pick(2)
    alpha = rz_all / curv_all
    beta = alpha * (w_all / (curv_all * (1.0 / STEP)))
    scaled = alpha * (1.0 / STEP)
    for k in range(4):
        for half in range(2):
            at = pl.ds(128 * half, 128)
            zk = zt[half, k]
            sol_ref[k, :, at] = alpha * zk
            res_ref[k, :, at] = jnp.where(count > k, own[half, k], 0.0) - scaled * vt[half, k]
            dir_ref[k, :, at] = beta * zk - alpha * wt[half, k]

    for o in around:
        for copy in halo[o]:
            pl.when(there(*o))(copy.wait_send)
    pl.when(jnp.logical_not(is_head))(to_head.wait_send)
    pl.when(y > 0)(to_south.wait_send)
    pl.when((place == 0) & (px > 0))(to_back.wait_send)
    pl.when(s < ns - 1)(along[0].wait_send)
    pl.when(s > 0)(along[1].wait_send)
    pl.when(y > 0)(across[0].wait_send)
    pl.when(y < ny - 1)(across[1].wait_send)
    told = copy_to(hall.at[pl.ds(0, size - 1)], hall.at[pl.ds(0, size - 1)], st, rt, head_of(px, y))

    pl.when(is_head)(rounds.wait_send)
    pl.when(tells)(told.wait_send)
    pl.when(tells_two)(told.wait_send)


def kernel(dims, src_hbm, cnt_ref, sol_ref, res_ref, dir_ref, *scratch):
    dma = pltpu.SemaphoreType.DMA
    pl.run_scoped(
        functools.partial(body, dims, src_hbm, cnt_ref, sol_ref, res_ref, dir_ref, scratch),
        dma((14,)), dma((4,)), dma((3,)), dma, dma, dma((2,)))


def flush(*refs):
    sources, targets, sem = refs[:3], refs[3:6], refs[6]
    copies = [pltpu.make_async_copy(a, b, sem.at[k]) for k, (a, b) in enumerate(zip(sources, targets))]
    for copy in copies:
        copy.start()
    for copy in copies:
        copy.wait()


def solution(mesh):
    ns, ny = mesh.shape["sfc"], mesh.shape["grp"]
    nx, nz, nc = SHAPES[ns]
    size, n_plane = nz * nc, nx * ny - 1
    dma = pltpu.SemaphoreType.DMA
    block = jax.ShapeDtypeStruct((4, E, 16 * E), F32)
    vmem = pl.BlockSpec(memory_space=pltpu.VMEM)
    hbm = pl.BlockSpec(memory_space=pltpu.HBM)
    slots = lambda *k: pltpu.VMEM((*k, E, 128), F32)
    fine = pltpu.VMEM((2, FINE, 128), F32)
    coarse = pltpu.VMEM((COARSE, 128), F32)
    line = lambda *k: pltpu.VMEM((*k, 128), F32)

    def shards(source, layer_counts):
        counts = jnp.broadcast_to(layer_counts.reshape(1, 1), (16, 128))
        parts = pl.pallas_call(
            functools.partial(kernel, (nx, nz, nc, ny)),
            out_shape=(block, block, block),
            in_specs=[hbm, vmem],
            out_specs=(vmem, vmem, vmem),
            scratch_shapes=[
                slots(2, 4), slots(2), slots(2, 4), slots(2, 4), slots(3, 2), slots(3, 2), *[fine] * 10,
                *[coarse] * 6, line(2, 32), line(2, 32), line(32), line(32), line(32),
                slots(2, 4), slots(2, 4), slots(2, 4),
                line(8), line(4), line(1), line(8 * size), line(4 * size), line(1), line(n_plane + 1, 1),
                line(1), line(1),
                dma((14,)), dma((4,)), dma, dma, dma, dma, dma,
            ],
            compiler_params=pltpu.CompilerParams(
                collective_id=0, has_side_effects=True, vmem_limit_bytes=24 << 20),
        )(pltpu.with_memory_space_constraint(source, pltpu.HBM), counts)
        return pl.pallas_call(
            flush, out_shape=(block, block, block), in_specs=[vmem] * 3, out_specs=(hbm,) * 3,
            scratch_shapes=[dma((3,))],
            compiler_params=pltpu.CompilerParams(vmem_limit_bytes=1 << 20),
        )(*parts)

    spec = P("sfc", None, "grp")
    return jax.shard_map(
        shards, mesh=mesh, in_specs=(spec, P("sfc")), out_specs=(spec, spec, spec), check_vma=False)
```

```python
import functools

import jax
import jax.numpy as jnp
from jax import lax
from jax.experimental import pallas as pl
from jax.experimental.pallas import tpu as pltpu
from jax.sharding import PartitionSpec as P

E = 16
OMEGA = 2.0 / 3.0
STEP = OMEGA / 6.0
KEEP = 1.0 - OMEGA
TAU = OMEGA / 1.5
QUARTER = TAU / 4.0
SHAPES = {96: (4, 12, 2), 8: (2, 2, 2)}
MESH = pl.DeviceIdType.MESH
F32 = jnp.float32
FINE = 8 + 24 * 25
COARSE = 8 + 16 * 13
NEED = dict(g=1, q=2, c=1, e1=2, e2=3, e3=4, zp=8, z1=10, z0=11, v=12, g2=13, q2=14, c2=7)


def others(*axes):
    found = [()]
    for count in axes:
        found = [f + (i,) for f in found for i in range(count)]
    far = lambda f: -sum(min(i, n - i) for i, n in zip(f, axes))
    return sorted([f for f in found if any(f)], key=far)


def tree(values):
    while len(values) > 1:
        values = [a + b for a, b in zip(values[::2], values[1::2])] + values[len(values) // 2 * 2:]
    return values[0]


def fine_row(j):
    return 8 + 24 * j


def coarse_row(j):
    return 8 + 16 * j


def body(dims, src_hbm, cnt_ref, sol_ref, res_ref, dir_ref, scratch, s1, s2, sm, sh, st, load_sem):
    nx, nz, nc, ny = dims
    (own, last, ysl, ynl, below, above, r, g, q, zp, z1, z0, v, g2, q2, w,
     c, e1, e2, e3, c2, kap, cd, cu, ca, cs, cn, zt, vt, wt,
     msg, face, faces, hb, hs, hx, hall, hrow, tot,
     r1, r2, rb, rs, rx, rh, rt) = scratch
    s = lax.axis_index("sfc")
    y = lax.axis_index("grp")
    ns, size = nx * nz * nc, nz * nc
    px, place = s // size, lax.rem(s, size)
    is_head = place == 1
    plane_set = others(nx, ny)
    n_plane = len(plane_set)

    loads = [pltpu.make_async_copy(src_hbm.at[:, :, pl.ds(128 * h, 128)], own.at[h], load_sem.at[h]) for h in range(2)]
    for load in loads:
        load.start()

    around = [(1, 1), (1, -1), (-1, 1), (-1, -1), (1, 0), (-1, 0), (0, 1), (0, -1)]
    d_ok = {1: s < ns - 1, -1: s > 0, 0: None}
    y_ok = {1: y < ny - 1, -1: y > 0, 0: None}

    def there(ds, dy):
        conds = [k for k in (d_ok[ds], y_ok[dy]) if k is not None]
        return functools.reduce(jnp.logical_and, conds)

    def near(ds, dy):
        return (s + ds, y + dy)

    def head_of(x, yy):
        return (x * size + 1, yy)

    def plane(dx, dy):
        return (lax.rem(px + dx, nx) * size + 1, lax.rem(y + dy, ny))

    barrier = pltpu.get_barrier_semaphore()

    def greet(target):
        pl.semaphore_signal(barrier, inc=1, device_id=target, device_id_type=MESH)

    for o in around:
        pl.when(there(*o))(functools.partial(greet, near(*o)))

    @pl.when(is_head)
    def _():
        for o in plane_set:
            greet(plane(*o))
        for k in range(size):
            if k != 1:
                greet((px * size + k, y))

        @pl.when(y < ny - 1)
        def _():
            for k in range(size):
                greet((px * size + k, y + 1))

        @pl.when(px < nx - 1)
        def _():
            greet(((px + 1) * size, y))

    one = lambda cond: jnp.where(cond, 1, 0)
    beside = (1 + one(s > 0) + one(s < ns - 1)) * (1 + one(y > 0) + one(y < ny - 1)) - 1
    heads = one(y > 0) + one((place == 0) & (px > 0)) + jnp.where(is_head, n_plane, 1)

    blank = jnp.zeros((8, 128), F32)
    for array in (r, g, zp, z1, z0, v, g2):
        for b in range(2):
            for j in range(-1, 25):
                array[b, pl.ds(fine_row(j) + 16, 8), :] = blank
    for array in (c, e1, e2, c2, kap):
        for j in range(-1, 13):
            array[pl.ds(coarse_row(j) + 8, 8), :] = blank
    kap[pl.ds(coarse_row(7), 8), :] = blank

    def clear(cond, box):
        @pl.when(cond)
        def _():
            box[...] = jnp.zeros(box.shape, F32)

    clear(s == 0, below)
    clear(s == ns - 1, above)
    clear(y == 0, ysl)
    clear(y == 0, below.at[0])
    clear(y == 0, above.at[0])
    clear(y == ny - 1, ynl)
    clear(y == ny - 1, below.at[2])
    clear(y == ny - 1, above.at[2])

    count = cnt_ref[...]
    for h in range(2):
        loads[h].wait()
        final = own[h, 0]
        for k in range(1, 4):
            final = jnp.where(count > k, own[h, k], final)
        last[h] = final
    pl.semaphore_wait(barrier, beside + heads)

    def copy_to(src, dst, ss, rs_, target):
        return pltpu.make_async_remote_copy(
            src_ref=src, dst_ref=dst, send_sem=ss, recv_sem=rs_, device_id=target, device_id_type=MESH)

    halo = {}
    made = 0
    for o in around:
        ds, dy = o
        halo[o] = []
        for part in range(2 if dy else 1):
            half = 1 - part if dy == 1 else part
            if ds:
                src, box = (last, below.at[1 - dy]) if ds == 1 else (own.at[:, 0], above.at[1 - dy])
                if dy:
                    src, box = src.at[half], box.at[half]
                if part:
                    src, box = (ref.at[pl.ds(8 if ds == 1 else 0, 8)] for ref in (src, box))
            else:
                src, box = own.at[half], (ysl if dy == 1 else ynl).at[half]
            halo[o].append(copy_to(src, box, s1.at[made], r1.at[made], near(*o)))
            made += 1
    for part in range(2):
        for o in around:
            if part < len(halo[o]):
                pl.when(there(*o))(halo[o][part].start)

    def arrived(ds, dy, part=0):
        pl.when(there(-ds, -dy))(halo[ds, dy][part].wait_recv)

    lane = lax.broadcasted_iota(jnp.int32, (8, 128), 1)
    upper = lane >= 64
    pair = lax.rem(lane, 64)
    cnt8 = count[:8]
    end = 8 + 8 * cnt8
    alive = (pair >= 8) & (pair < end)
    lo_lane = jnp.where(s > 0, 8, 0)
    hi_lane = jnp.where(s < ns - 1, 8, 0)
    there_mask = (pair >= 8 - lo_lane) & (pair < end + hi_lane)
    mask = jnp.where(there_mask, 1.0, 0.0).astype(F32)
    outer = jnp.where(upper, jnp.where(y < ny - 1, mask, 0.0), jnp.where(y > 0, mask, 0.0))
    fine_masks = [outer * STEP, outer * STEP, mask * STEP]
    coarse_masks = [outer * QUARTER, outer * QUARTER, mask * QUARTER]
    pieces = (ysl, own, ynl)

    def assemble(block):
        for b in range(2):
            stack = []
            for m in (block, 5 - block):
                take = lambda ref, *k: ref[(*k, pl.ds(b, 8, stride=2), slice(None))]
                up = take(above, m // 2, m % 2)
                stack.append(take(below, m // 2, m % 2))
                for k in range(4):
                    mine = take(pieces[m // 2], m % 2, k)
                    stack.append(jnp.where(cnt8 == k, up, mine) if k else mine)
                stack += [up, blank, blank]
            turned = jnp.concatenate(stack, axis=0).T
            for j in range(8):
                for h in range(2):
                    low, high = turned[16 * j + 8 * h:16 * j + 8 * h + 8], turned[16 * (7 - j) + 8 * h:16 * (7 - j) + 8 * h + 8]
                    value = jnp.where(upper, high, low) * fine_masks[block]
                    r[b, pl.ds(fine_row(8 * block + j) + 8 * h, 8), :] = value
                    if block == 2 and j == 7:
                        r[b, pl.ds(fine_row(24) + 8 * h, 8), :] = pltpu.roll(value, 64, 1)

    def total(ref, b, j, h):
        i = fine_row(j) + 8 * h
        load8 = lambda k: ref[b, pl.ds(k, 8), :]
        across = ref[1 - b, pl.ds(i, 8), :]
        turned = pltpu.roll(across, 127 if b else 1, 1)
        return load8(i), ((load8(i - 24) + load8(i + 24)) + (load8(i - 1) + load8(i + 1))) + (across + turned)

    def put(dst, b, j, h, value):
        dst[b, pl.ds(fine_row(j) + 8 * h, 8), :] = value
        if j == 23:
            dst[b, pl.ds(fine_row(24) + 8 * h, 8), :] = pltpu.roll(value, 64, 1)

    def smooth(src, dst, add=None):
        def row(j):
            for b in range(2):
                for h in range(2):
                    mid, six = total(src, b, j, h)
                    value = KEEP * mid + fine_masks[j // 8] * six
                    if add is not None:
                        value = value + add[b, pl.ds(fine_row(j) + 8 * h, 8), :]
                    put(dst, b, j, h, value)
        return row

    def apply(src, dst):
        def row(j):
            for b in range(2):
                for h in range(2):
                    mid, six = total(src, b, j, h)
                    put(dst, b, j, h, OMEGA * mid - fine_masks[j // 8] * six)
        return row

    def put_coarse(dst, j, value):
        dst[pl.ds(coarse_row(j), 8), :] = value
        if j == 11:
            dst[pl.ds(coarse_row(12), 8), :] = pltpu.roll(value, 64, 1)

    def restrict(src, dst):
        def row(j):
            eight = None
            for b in range(2):
                for k in range(4):
                    part = src[b, pl.ds(fine_row(2 * j + k // 2) + k % 2, 8, stride=2), :]
                    eight = part if eight is None else eight + part
            put_coarse(dst, j, (0.125 * TAU / STEP) * eight)
        return row

    def coarse_total(ref, j):
        i = coarse_row(j)
        load8 = lambda k: ref[pl.ds(k, 8), :]
        mid = load8(i)
        sides = pltpu.roll(mid, 1, 1) + pltpu.roll(mid, 127, 1)
        return mid, ((load8(i - 16) + load8(i + 16)) + (load8(i - 1) + load8(i + 1))) + sides

    def coarse_first(rhs, dst):
        def row(j):
            mid, six = coarse_total(rhs, j)
            put_coarse(dst, j, (1.0 + KEEP) * mid + coarse_masks[j // 4] * six)
        return row

    def coarse_sweep(rhs, src, dst):
        def row(j):
            mid, six = coarse_total(src, j)
            put_coarse(dst, j, (KEEP * mid + rhs[pl.ds(coarse_row(j), 8), :]) + coarse_masks[j // 4] * six)
        return row

    def corrected(rhs, first, coarse, dst):
        def row(j):
            add = coarse[pl.ds(coarse_row(j), 8), :]
            for b in range(2):
                for k in range(4):
                    fine_j = 2 * j + k // 2
                    at = pl.ds(fine_row(fine_j) + k % 2, 8, stride=2)
                    value = (rhs[b, at, :] + first[b, at, :]) + add
                    dst[b, at, :] = value
                    if fine_j == 23:
                        dst[b, pl.ds(fine_row(24) + k % 2, 8, stride=2), :] = pltpu.roll(value, 64, 1)
        return row

    def rows(fn, lo, hi):
        for j in reversed(range(lo, hi)):
            fn(j)

    shrink = lambda lo: lo + 1
    halve = lambda lo: -(-lo // 2)
    double = lambda lo: 2 * lo
    stages = [
        ("g", "r", shrink, smooth(r, g)), ("q", "g", shrink, smooth(g, q)),
        ("c", "q", halve, restrict(q, c)), ("e1", "c", shrink, coarse_first(c, e1)),
        ("e2", "e1", shrink, coarse_sweep(c, e1, e2)), ("e3", "e2", shrink, coarse_sweep(c, e2, e3)),
        ("zp", "e3", double, corrected(r, g, e3, zp)), ("z1", "zp", shrink, smooth(zp, z1, r)),
        ("z0", "z1", shrink, smooth(z1, z0, r)), ("v", "z0", shrink, apply(z0, v)),
        ("g2", "v", shrink, smooth(v, g2)), ("q2", "g2", shrink, smooth(g2, q2)),
        ("c2", "q2", halve, restrict(q2, c2)),
    ]
    coarse_names = ("c", "e1", "e2", "e3", "c2")
    done = {}

    def advance(lo, until=None):
        have = {"r": lo}
        for name, source, change, fn in stages:
            if name == until:
                break
            start = max(change(have[source]), NEED[name])
            stop = done.get(name, 12 if name in coarse_names else 24)
            if start >= stop:
                break
            have[name] = done[name] = start
            if name == "zp":
                rows(fn, start // 2, stop // 2)
            else:
                rows(fn, start, stop)

    arrived(1, 0)
    arrived(-1, 0)
    assemble(2)
    advance(16)
    for dy in (1, -1):
        for ds in (1, -1, 0):
            arrived(ds, dy, 0)
    assemble(1)
    advance(8, 'g2')
    for dy in (1, -1):
        for ds in (1, -1, 0):
            arrived(ds, dy, 1)
    assemble(0)
    advance(0)

    rz = curv = fine = coarse = blank
    for j in range(16, 24):
        for b in range(2):
            for h in range(2):
                at = (b, pl.ds(fine_row(j) + 8 * h, 8))
                vy, gy, qy, zy = v[at], g2[at], q2[at], z0[at]
                rz = rz + r[at] * zy
                curv = curv + zy * vy
                fine = fine + (vy * ((vy + gy) + qy) + gy * qy)
    for j in range(8, 12):
        mid, six = coarse_total(c2, j)
        put_coarse(kap, j, jnp.where(alive, KEEP * mid + coarse_masks[2] * six, 0.0))
    for j in range(8, 12):
        k, six = coarse_total(kap, j)
        cc = c2[pl.ds(coarse_row(j), 8), :]
        coarse = coarse + (cc * (cc + k) + k * ((1.0 + KEEP) * k + QUARTER * six))
    column = lambda value: jnp.sum(jnp.where(alive, value, 0.0), axis=0, keepdims=True)
    inner = jnp.concatenate([kap[pl.ds(coarse_row(j), 8), :] for j in range(8, 12)], axis=0)
    turned = jnp.concatenate([inner] * 4, axis=0).T
    cnt1, lane1 = cnt8[:1], lane[:1]
    ends = []
    for h in (0, 64):
        tail = turned[h + 15:h + 16]
        for k in range(2, 5):
            tail = jnp.where(cnt1 == k, turned[h + 7 + 8 * k:h + 8 + 8 * k], tail)
        ends.append((turned[h + 8:h + 9], tail))
    second = lax.rem(lane1, 64) >= 32
    first_face, last_face = (jnp.where(second, ends[1][k], ends[0][k]) for k in range(2))
    swap = jnp.where(lax.rem(place, 2) == 1, 64, 0)
    d_face = jnp.where((lane1 >= swap) & (lane1 < swap + 64), first_face, last_face)
    sides = kap[pl.ds(coarse_row(8), 8), :]
    swapped = pltpu.roll(sides, 64, 1)
    north_face = jnp.where(upper[:4], sides[:4], swapped[4:])
    south_face = jnp.where(upper[:4], swapped[:4], sides[4:])
    msg[...] = jnp.concatenate(
        [column(rz), column(curv), (1.0 / STEP) * column(fine) + (8.0 / TAU) * column(coarse), d_face, north_face],
        axis=0)
    face[...] = south_face
    faces[...] = d_face

    order = [0] + list(range(2, size)) + [1]
    box = jnp.where(place > 1, place - 1, 0)
    box = jnp.where(is_head, size - 1, box)
    to_head = copy_to(msg, hb.at[pl.ds(pl.multiple_of(8 * box, 8), 8)], sm.at[0], rb, head_of(px, y))
    to_south = copy_to(face, hs.at[pl.ds(pl.multiple_of(4 * box, 4), 4)], sm.at[1], rs, head_of(px, y - 1))
    to_back = copy_to(faces, hx, sm.at[2], rx, head_of(px - 1, y))
    pl.when(jnp.logical_not(is_head))(to_head.start)
    pl.when(y > 0)(to_south.start)
    pl.when((place == 0) & (px > 0))(to_back.start)

    mine = jnp.concatenate([c2[pl.ds(coarse_row(j), 8), :] for j in range(8, 12)], axis=0)
    four = lambda x: jnp.concatenate([x] * 4, axis=0)
    cnt32, alive32 = four(cnt8), four(alive)

    def shifted(value, sign):
        out = pltpu.roll(value, (8 * sign) % 128, 1)
        for k in range(2, 5):
            out = jnp.where(cnt32 == k, pltpu.roll(value, (8 * k * sign) % 128, 1), out)
        return out

    cd[0] = shifted(mine, -1)
    cu[0] = mine
    along = [copy_to(cd.at[0], cd.at[1], s2.at[0], r2.at[0], near(1, 0)),
             copy_to(cu.at[0], cu.at[1], s2.at[1], r2.at[1], near(-1, 0))]
    pl.when(s < ns - 1)(along[0].start)
    pl.when(s > 0)(along[1].start)

    pl.when(s > 0)(along[0].wait_recv)
    pl.when(s < ns - 1)(along[1].wait_recv)
    lo32 = four((pair >= 8 - lo_lane) & (pair < 8))
    hi32 = four((pair >= end) & (pair < end + hi_lane))
    ca[...] = jnp.where(alive32, mine, jnp.where(lo32, cd[1], jnp.where(hi32, shifted(cu[1], 1), 0.0)))
    across = [copy_to(ca, cn, s2.at[2], r2.at[2], near(0, -1)),
              copy_to(ca, cs, s2.at[3], r2.at[3], near(0, 1))]
    pl.when(y > 0)(across[0].start)
    pl.when(y < ny - 1)(across[1].start)

    lines = copy_to(hb.at[pl.ds(0, 8 * (size - 1))], hb.at[pl.ds(0, 8 * (size - 1))], sm.at[0], rb, head_of(px, y))
    beyond = copy_to(hs, hs, sm.at[1], rs, head_of(px, y))
    rounds = copy_to(hall.at[pl.ds(0, n_plane)], hall.at[pl.ds(0, n_plane)], sh, rh, head_of(px, y))

    def round_of(k):
        return copy_to(hall.at[n_plane], hall.at[k], sh, rh, plane(*plane_set[k]))

    @pl.when(is_head)
    def _():
        hb[pl.ds(8 * (size - 1), 8), :] = msg[...]
        lines.wait_recv()
        pl.when(y < ny - 1)(beyond.wait_recv)
        pl.when(px < nx - 1)(to_back.wait_recv)
        acc = tree([hb[pl.ds(8 * k, 8), :] for k in range(size)])
        cross = tree([hb[pl.ds(8 * k + 4, 4), :] * hs[pl.ds(4 * k, 4), :] for k in range(size)])
        cross = jnp.where(y < ny - 1, jnp.sum(cross, axis=0, keepdims=True), 0.0)
        where_is = {p: k for k, p in enumerate(order)}
        row_at = lambda p: hb[pl.ds(8 * where_is[p] + 3, 1), :]
        pairs = [[], []]
        for p in range(size - 1):
            pairs[p % 2].append(row_at(p) * row_at(p + 1))
        pairs[1].append(jnp.where(px < nx - 1, row_at(size - 1) * hx[...], 0.0))
        cross = cross + jnp.where(lane1 < 64, tree(pairs[1]), tree(pairs[0]))
        three = jnp.concatenate([acc[:2], acc[2:3] + 4.0 * cross], axis=0)
        sums = jnp.sum(three, axis=1, keepdims=True)
        hall[n_plane] = jnp.where(lane1 == 0, sums[:1], jnp.where(lane1 == 1, sums[1:2], sums[2:]))
        for k in range(n_plane):
            round_of(k).start()

    def turn_back(src, dst):
        for b in range(2):
            stack = []
            for j in range(8):
                for h in range(2):
                    low, high = src[b, pl.ds(fine_row(16 + j) + 8 * h, 8), :], src[b, pl.ds(fine_row(23 - j) + 8 * h, 8), :]
                    stack.append(jnp.where(alive, jnp.where(upper, high, low), 0.0))
            x = jnp.concatenate(stack, axis=0).T
            for h in range(2):
                for k in range(4):
                    at = 64 * h + 8 * (k + 1)
                    dst[h, k, pl.ds(b, 8, stride=2), :] = x[at:at + 8]

    turn_back(z0, zt)
    turn_back(v, vt)

    pl.when(y > 0)(across[1].wait_recv)
    pl.when(y < ny - 1)(across[0].wait_recv)
    for j in range(4, 12):
        if j < 8:
            at = pl.ds(8 * (7 - j), 8)
            south = jnp.where(y > 0, pltpu.roll(cs[at, :], 64, 1), 0.0)
            north = jnp.where(y < ny - 1, pltpu.roll(cn[at, :], 64, 1), 0.0)
            put_coarse(c, j, jnp.where(upper, north, south))
        else:
            put_coarse(c, j, ca[pl.ds(8 * (j - 8), 8), :])
    rows(coarse_first(c, e1), 5, 12)
    rows(coarse_sweep(c, e1, e2), 6, 12)
    rows(coarse_sweep(c, e2, e3), 7, 12)
    rows(corrected(v, g2, e3, zp), 7, 12)
    rows(smooth(zp, z1, v), 15, 24)
    rows(smooth(z1, w, v), 16, 24)
    turn_back(w, wt)

    def news(k, yy):
        return copy_to(hrow, tot, st, rt, (px * size + k, yy))

    is_first = is_head & (px == 0) & (y == 0)
    tells = is_head & jnp.logical_not(is_first)
    tells_two = is_head & (px == 0) & (y == 1)

    @pl.when(is_head)
    def _():
        rounds.wait_recv()
        total_row = tree([hall[k] for k in range(n_plane + 1)])
        hrow[...] = total_row
        tot[...] = total_row

    @pl.when(tells_two)
    def _():
        for k in list(range(2, size)) + [0]:
            news(k, 0).start()

    @pl.when(tells)
    def _():
        for k in [0] + list(range(2, size)):
            news(k, y).start()

    pl.when(jnp.logical_not(is_head))(news(0, y).wait_recv)
    sums = tot[...]
    pick = lambda k: jnp.broadcast_to(sums[:, k:k + 1], (1, 128))
    rz_all, curv_all, w_all = pick(0), pick(1), pick(2)
    alpha = rz_all / curv_all
    beta = alpha * (w_all / (curv_all * (1.0 / STEP)))
    scaled = alpha * (1.0 / STEP)
    for k in range(4):
        for half in range(2):
            at = pl.ds(128 * half, 128)
            zk = zt[half, k]
            sol_ref[k, :, at] = alpha * zk
            res_ref[k, :, at] = jnp.where(count > k, own[half, k], 0.0) - scaled * vt[half, k]
            dir_ref[k, :, at] = beta * zk - alpha * wt[half, k]

    for o in around:
        for copy in halo[o]:
            pl.when(there(*o))(copy.wait_send)
    pl.when(jnp.logical_not(is_head))(to_head.wait_send)
    pl.when(y > 0)(to_south.wait_send)
    pl.when((place == 0) & (px > 0))(to_back.wait_send)
    pl.when(s < ns - 1)(along[0].wait_send)
    pl.when(s > 0)(along[1].wait_send)
    pl.when(y > 0)(across[0].wait_send)
    pl.when(y < ny - 1)(across[1].wait_send)
    told = copy_to(hall.at[pl.ds(0, size - 1)], hall.at[pl.ds(0, size - 1)], st, rt, head_of(px, y))

    pl.when(is_head)(rounds.wait_send)
    pl.when(tells)(told.wait_send)
    pl.when(tells_two)(told.wait_send)


def kernel(dims, src_hbm, cnt_ref, sol_ref, res_ref, dir_ref, *scratch):
    dma = pltpu.SemaphoreType.DMA
    pl.run_scoped(
        functools.partial(body, dims, src_hbm, cnt_ref, sol_ref, res_ref, dir_ref, scratch),
        dma((14,)), dma((4,)), dma((3,)), dma, dma, dma((2,)))


def flush(*refs):
    sources, targets, sem = refs[:3], refs[3:6], refs[6]
    copies = [pltpu.make_async_copy(a, b, sem.at[k]) for k, (a, b) in enumerate(zip(sources, targets))]
    for copy in copies:
        copy.start()
    for copy in copies:
        copy.wait()


def solution(mesh):
    ns, ny = mesh.shape["sfc"], mesh.shape["grp"]
    nx, nz, nc = SHAPES[ns]
    size, n_plane = nz * nc, nx * ny - 1
    dma = pltpu.SemaphoreType.DMA
    block = jax.ShapeDtypeStruct((4, E, 16 * E), F32)
    vmem = pl.BlockSpec(memory_space=pltpu.VMEM)
    hbm = pl.BlockSpec(memory_space=pltpu.HBM)
    slots = lambda *k: pltpu.VMEM((*k, E, 128), F32)
    fine = pltpu.VMEM((2, FINE, 128), F32)
    coarse = pltpu.VMEM((COARSE, 128), F32)
    line = lambda *k: pltpu.VMEM((*k, 128), F32)

    def shards(source, layer_counts):
        counts = jnp.broadcast_to(layer_counts.reshape(1, 1), (16, 128))
        parts = pl.pallas_call(
            functools.partial(kernel, (nx, nz, nc, ny)),
            out_shape=(block, block, block),
            in_specs=[hbm, vmem],
            out_specs=(vmem, vmem, vmem),
            scratch_shapes=[
                slots(2, 4), slots(2), slots(2, 4), slots(2, 4), slots(3, 2), slots(3, 2), *[fine] * 10,
                *[coarse] * 6, line(2, 32), line(2, 32), line(32), line(32), line(32),
                slots(2, 4), slots(2, 4), slots(2, 4),
                line(8), line(4), line(1), line(8 * size), line(4 * size), line(1), line(n_plane + 1, 1),
                line(1), line(1),
                dma((14,)), dma((4,)), dma, dma, dma, dma, dma,
            ],
            compiler_params=pltpu.CompilerParams(
                collective_id=0, has_side_effects=True, vmem_limit_bytes=24 << 20),
        )(pltpu.with_memory_space_constraint(source, pltpu.HBM), counts)
        return pl.pallas_call(
            flush, out_shape=(block, block, block), in_specs=[vmem] * 3, out_specs=(hbm,) * 3,
            scratch_shapes=[dma((3,))],
            compiler_params=pltpu.CompilerParams(vmem_limit_bytes=1 << 20),
        )(*parts)

    spec = P("sfc", None, "grp")
    return jax.shard_map(
        shards, mesh=mesh, in_specs=(spec, P("sfc")), out_specs=(spec, spec, spec), check_vma=False)
```

```python
import functools

import jax
import jax.numpy as jnp
from jax import lax
from jax.experimental import pallas as pl
from jax.experimental.pallas import tpu as pltpu
from jax.sharding import PartitionSpec as P

E = 16
OMEGA = 2.0 / 3.0
STEP = OMEGA / 6.0
KEEP = 1.0 - OMEGA
TAU = OMEGA / 1.5
QUARTER = TAU / 4.0
SHAPES = {96: (4, 12, 2), 8: (2, 2, 2)}
MESH = pl.DeviceIdType.MESH
F32 = jnp.float32
FINE = 8 + 24 * 25
COARSE = 8 + 16 * 13
NEED = dict(g=1, q=2, c=1, e1=2, e2=3, e3=4, zp=8, z1=10, z0=11, v=12, g2=13, q2=14, c2=7)


def others(*axes):
    found = [()]
    for count in axes:
        found = [f + (i,) for f in found for i in range(count)]
    far = lambda f: -sum(min(i, n - i) for i, n in zip(f, axes))
    return sorted([f for f in found if any(f)], key=far)


def tree(values):
    while len(values) > 1:
        values = [a + b for a, b in zip(values[::2], values[1::2])] + values[len(values) // 2 * 2:]
    return values[0]


def fine_row(j):
    return 8 + 24 * j


def coarse_row(j):
    return 8 + 16 * j


def body(dims, src_hbm, cnt_ref, sol_ref, res_ref, dir_ref, scratch,
         s1, r1, s2, r2, sm, rb, rs, rx, sh, rh, st, rt, load_sem):
    nx, nz, nc, ny = dims
    (own, last, ysl, ynl, below, above, r, g, q, zp, z1, z0, v, g2, q2, w,
     c, e1, e2, e3, c2, kap, cd, cu, ca, cs, cn, zt, vt, wt,
     msg, face, faces, hb, hs, hx, hall, hrow, tot) = scratch
    s = lax.axis_index("sfc")
    y = lax.axis_index("grp")
    ns, size = nx * nz * nc, nz * nc
    px, place = s // size, lax.rem(s, size)
    is_head = place == 1
    plane_set = others(nx, ny)
    n_plane = len(plane_set)

    loads = [pltpu.make_async_copy(src_hbm.at[:, :, pl.ds(128 * h, 128)], own.at[h], load_sem.at[h]) for h in range(2)]
    for load in loads:
        load.start()

    around = [(1, 1), (1, -1), (-1, 1), (-1, -1), (1, 0), (-1, 0), (0, 1), (0, -1)]
    d_ok = {1: s < ns - 1, -1: s > 0, 0: None}
    y_ok = {1: y < ny - 1, -1: y > 0, 0: None}

    def there(ds, dy):
        conds = [k for k in (d_ok[ds], y_ok[dy]) if k is not None]
        return functools.reduce(jnp.logical_and, conds)

    def beside_of(k, step, count):
        if step == 0:
            return k
        return jnp.where(k < count - 1, k + 1, 0) if step == 1 else jnp.where(k > 0, k - 1, count - 1)

    def near(ds, dy):
        return (beside_of(s, ds, ns), beside_of(y, dy, ny))

    def head_of(x, yy):
        return (x * size + 1, yy)

    def plane(dx, dy):
        return (lax.rem(px + dx, nx) * size + 1, lax.rem(y + dy, ny))

    barrier = pltpu.get_barrier_semaphore()

    def greet(target):
        pl.semaphore_signal(barrier, inc=1, device_id=target, device_id_type=MESH)

    for o in around:
        pl.when(there(*o))(functools.partial(greet, near(*o)))

    @pl.when(is_head)
    def _():
        for o in plane_set:
            greet(plane(*o))
        for k in range(size):
            if k != 1:
                greet((px * size + k, y))

        @pl.when(y < ny - 1)
        def _():
            for k in range(size):
                greet((px * size + k, beside_of(y, 1, ny)))

        @pl.when(px < nx - 1)
        def _():
            greet((beside_of(px, 1, nx) * size, y))

    one = lambda cond: jnp.where(cond, 1, 0)
    beside = (1 + one(s > 0) + one(s < ns - 1)) * (1 + one(y > 0) + one(y < ny - 1)) - 1
    heads = one(y > 0) + one((place == 0) & (px > 0)) + jnp.where(is_head, n_plane, 1)

    blank = jnp.zeros((8, 128), F32)
    for array in (r, g, zp, z1, z0, v, g2):
        for b in range(2):
            for j in range(-1, 25):
                array[b, pl.ds(fine_row(j) + 16, 8), :] = blank
    for array in (c, e1, e2, c2, kap):
        for j in range(-1, 13):
            array[pl.ds(coarse_row(j) + 8, 8), :] = blank
    kap[pl.ds(coarse_row(7), 8), :] = blank

    def clear(cond, box):
        @pl.when(cond)
        def _():
            box[...] = jnp.zeros(box.shape, F32)

    clear(s == 0, below)
    clear(s == ns - 1, above)
    clear(y == 0, ysl)
    clear(y == 0, below.at[0])
    clear(y == 0, above.at[0])
    clear(y == ny - 1, ynl)
    clear(y == ny - 1, below.at[2])
    clear(y == ny - 1, above.at[2])

    count = cnt_ref[...]
    for h in range(2):
        loads[h].wait()
        final = own[h, 0]
        for k in range(1, 4):
            final = jnp.where(count > k, own[h, k], final)
        last[h] = final
    pl.semaphore_wait(barrier, beside + heads)

    def copy_to(src, dst, ss, rs_, target):
        return pltpu.make_async_remote_copy(
            src_ref=src, dst_ref=dst, send_sem=ss, recv_sem=rs_, device_id=target, device_id_type=MESH)

    halo = {}
    made = 0
    for o in around:
        ds, dy = o
        halo[o] = []
        for part in range(2 if dy else 1):
            half = 1 - part if dy == 1 else part
            if ds:
                src, box = (last, below.at[1 - dy]) if ds == 1 else (own.at[:, 0], above.at[1 - dy])
                if dy:
                    src, box = src.at[half], box.at[half]
                if part:
                    src, box = (ref.at[pl.ds(8 if ds == 1 else 0, 8)] for ref in (src, box))
            else:
                src, box = own.at[half], (ysl if dy == 1 else ynl).at[half]
            halo[o].append(copy_to(src, box, s1.at[made], r1.at[made], near(*o)))
            made += 1
    for part in range(2):
        for o in around:
            if part < len(halo[o]):
                pl.when(there(*o))(halo[o][part].start)

    def arrived(ds, dy, part=0):
        pl.when(there(-ds, -dy))(halo[ds, dy][part].wait_recv)

    lane = lax.broadcasted_iota(jnp.int32, (8, 128), 1)
    upper = lane >= 64
    pair = lax.rem(lane, 64)
    cnt8 = count[:8]
    end = 8 + 8 * cnt8
    alive = (pair >= 8) & (pair < end)
    lo_lane = jnp.where(s > 0, 8, 0)
    hi_lane = jnp.where(s < ns - 1, 8, 0)
    there_mask = (pair >= 8 - lo_lane) & (pair < end + hi_lane)
    mask = jnp.where(there_mask, 1.0, 0.0).astype(F32)
    outer = jnp.where(upper, jnp.where(y < ny - 1, mask, 0.0), jnp.where(y > 0, mask, 0.0))
    fine_masks = [outer * STEP, outer * STEP, mask * STEP]
    coarse_masks = [outer * QUARTER, outer * QUARTER, mask * QUARTER]
    pieces = (ysl, own, ynl)

    def assemble(block):
        for b in range(2):
            stack = []
            for m in (block, 5 - block):
                take = lambda ref, *k: ref[(*k, pl.ds(b, 8, stride=2), slice(None))]
                up = take(above, m // 2, m % 2)
                stack.append(take(below, m // 2, m % 2))
                for k in range(4):
                    mine = take(pieces[m // 2], m % 2, k)
                    stack.append(jnp.where(cnt8 == k, up, mine) if k else mine)
                stack += [up, blank, blank]
            turned = jnp.concatenate(stack, axis=0).T
            for j in range(8):
                for h in range(2):
                    low, high = turned[16 * j + 8 * h:16 * j + 8 * h + 8], turned[16 * (7 - j) + 8 * h:16 * (7 - j) + 8 * h + 8]
                    value = jnp.where(upper, high, low) * fine_masks[block]
                    r[b, pl.ds(fine_row(8 * block + j) + 8 * h, 8), :] = value
                    if block == 2 and j == 7:
                        r[b, pl.ds(fine_row(24) + 8 * h, 8), :] = pltpu.roll(value, 64, 1)

    def total(ref, b, j, h):
        i = fine_row(j) + 8 * h
        load8 = lambda k: ref[b, pl.ds(k, 8), :]
        across = ref[1 - b, pl.ds(i, 8), :]
        turned = pltpu.roll(across, 127 if b else 1, 1)
        return load8(i), ((load8(i - 24) + load8(i + 24)) + (load8(i - 1) + load8(i + 1))) + (across + turned)

    def put(dst, b, j, h, value):
        dst[b, pl.ds(fine_row(j) + 8 * h, 8), :] = value
        if j == 23:
            dst[b, pl.ds(fine_row(24) + 8 * h, 8), :] = pltpu.roll(value, 64, 1)

    def smooth(src, dst, add=None):
        def row(j):
            for b in range(2):
                for h in range(2):
                    mid, six = total(src, b, j, h)
                    value = KEEP * mid + fine_masks[j // 8] * six
                    if add is not None:
                        value = value + add[b, pl.ds(fine_row(j) + 8 * h, 8), :]
                    put(dst, b, j, h, value)
        return row

    def apply(src, dst):
        def row(j):
            for b in range(2):
                for h in range(2):
                    mid, six = total(src, b, j, h)
                    put(dst, b, j, h, OMEGA * mid - fine_masks[j // 8] * six)
        return row

    def put_coarse(dst, j, value):
        dst[pl.ds(coarse_row(j), 8), :] = value
        if j == 11:
            dst[pl.ds(coarse_row(12), 8), :] = pltpu.roll(value, 64, 1)

    def restrict(src, dst):
        def row(j):
            eight = None
            for b in range(2):
                for k in range(4):
                    part = src[b, pl.ds(fine_row(2 * j + k // 2) + k % 2, 8, stride=2), :]
                    eight = part if eight is None else eight + part
            put_coarse(dst, j, (0.125 * TAU / STEP) * eight)
        return row

    def coarse_total(ref, j):
        i = coarse_row(j)
        load8 = lambda k: ref[pl.ds(k, 8), :]
        mid = load8(i)
        sides = pltpu.roll(mid, 1, 1) + pltpu.roll(mid, 127, 1)
        return mid, ((load8(i - 16) + load8(i + 16)) + (load8(i - 1) + load8(i + 1))) + sides

    def coarse_first(rhs, dst):
        def row(j):
            mid, six = coarse_total(rhs, j)
            put_coarse(dst, j, (1.0 + KEEP) * mid + coarse_masks[j // 4] * six)
        return row

    def coarse_sweep(rhs, src, dst):
        def row(j):
            mid, six = coarse_total(src, j)
            put_coarse(dst, j, (KEEP * mid + rhs[pl.ds(coarse_row(j), 8), :]) + coarse_masks[j // 4] * six)
        return row

    def corrected(rhs, first, coarse, dst):
        def row(j):
            add = coarse[pl.ds(coarse_row(j), 8), :]
            for b in range(2):
                for k in range(4):
                    fine_j = 2 * j + k // 2
                    at = pl.ds(fine_row(fine_j) + k % 2, 8, stride=2)
                    value = (rhs[b, at, :] + first[b, at, :]) + add
                    dst[b, at, :] = value
                    if fine_j == 23:
                        dst[b, pl.ds(fine_row(24) + k % 2, 8, stride=2), :] = pltpu.roll(value, 64, 1)
        return row

    def rows(fn, lo, hi):
        for j in reversed(range(lo, hi)):
            fn(j)

    shrink = lambda lo: lo + 1
    halve = lambda lo: -(-lo // 2)
    double = lambda lo: 2 * lo
    stages = [
        ("g", "r", shrink, smooth(r, g)), ("q", "g", shrink, smooth(g, q)),
        ("c", "q", halve, restrict(q, c)), ("e1", "c", shrink, coarse_first(c, e1)),
        ("e2", "e1", shrink, coarse_sweep(c, e1, e2)), ("e3", "e2", shrink, coarse_sweep(c, e2, e3)),
        ("zp", "e3", double, corrected(r, g, e3, zp)), ("z1", "zp", shrink, smooth(zp, z1, r)),
        ("z0", "z1", shrink, smooth(z1, z0, r)), ("v", "z0", shrink, apply(z0, v)),
        ("g2", "v", shrink, smooth(v, g2)), ("q2", "g2", shrink, smooth(g2, q2)),
        ("c2", "q2", halve, restrict(q2, c2)),
    ]
    coarse_names = ("c", "e1", "e2", "e3", "c2")
    done = {}

    def advance(lo, until=None):
        have = {"r": lo}
        for name, source, change, fn in stages:
            if name == until:
                break
            start = max(change(have[source]), NEED[name])
            stop = done.get(name, 12 if name in coarse_names else 24)
            if start >= stop:
                break
            have[name] = done[name] = start
            if name == "zp":
                rows(fn, start // 2, stop // 2)
            else:
                rows(fn, start, stop)

    arrived(1, 0)
    arrived(-1, 0)
    assemble(2)
    advance(16)
    for dy in (1, -1):
        for ds in (1, -1, 0):
            arrived(ds, dy, 0)
    assemble(1)
    advance(8, 'g2')
    for dy in (1, -1):
        for ds in (1, -1, 0):
            arrived(ds, dy, 1)
    assemble(0)
    advance(0)

    rz = curv = fine = coarse = blank
    for j in range(16, 24):
        for b in range(2):
            for h in range(2):
                at = (b, pl.ds(fine_row(j) + 8 * h, 8))
                vy, gy, qy, zy = v[at], g2[at], q2[at], z0[at]
                rz = rz + r[at] * zy
                curv = curv + zy * vy
                fine = fine + (vy * ((vy + gy) + qy) + gy * qy)
    for j in range(8, 12):
        mid, six = coarse_total(c2, j)
        put_coarse(kap, j, jnp.where(alive, KEEP * mid + coarse_masks[2] * six, 0.0))
    for j in range(8, 12):
        k, six = coarse_total(kap, j)
        cc = c2[pl.ds(coarse_row(j), 8), :]
        coarse = coarse + (cc * (cc + k) + k * ((1.0 + KEEP) * k + QUARTER * six))
    column = lambda value: jnp.sum(jnp.where(alive, value, 0.0), axis=0, keepdims=True)
    inner = jnp.concatenate([kap[pl.ds(coarse_row(j), 8), :] for j in range(8, 12)], axis=0)
    turned = jnp.concatenate([inner] * 4, axis=0).T
    cnt1, lane1 = cnt8[:1], lane[:1]
    ends = []
    for h in (0, 64):
        tail = turned[h + 15:h + 16]
        for k in range(2, 5):
            tail = jnp.where(cnt1 == k, turned[h + 7 + 8 * k:h + 8 + 8 * k], tail)
        ends.append((turned[h + 8:h + 9], tail))
    second = lax.rem(lane1, 64) >= 32
    first_face, last_face = (jnp.where(second, ends[1][k], ends[0][k]) for k in range(2))
    swap = jnp.where(lax.rem(place, 2) == 1, 64, 0)
    d_face = jnp.where((lane1 >= swap) & (lane1 < swap + 64), first_face, last_face)
    sides = kap[pl.ds(coarse_row(8), 8), :]
    swapped = pltpu.roll(sides, 64, 1)
    north_face = jnp.where(upper[:4], sides[:4], swapped[4:])
    south_face = jnp.where(upper[:4], swapped[:4], sides[4:])
    msg[...] = jnp.concatenate(
        [column(rz), column(curv), (1.0 / STEP) * column(fine) + (8.0 / TAU) * column(coarse), d_face, north_face],
        axis=0)
    face[...] = south_face
    faces[...] = d_face

    order = [0] + list(range(2, size)) + [1]
    box = jnp.where(place > 1, place - 1, 0)
    box = jnp.where(is_head, size - 1, box)
    to_head = copy_to(msg, hb.at[pl.ds(pl.multiple_of(8 * box, 8), 8)], sm.at[0], rb, head_of(px, y))
    to_south = copy_to(face, hs.at[pl.ds(pl.multiple_of(4 * box, 4), 4)], sm.at[1], rs, head_of(px, beside_of(y, -1, ny)))
    to_back = copy_to(faces, hx, sm.at[2], rx, head_of(beside_of(px, -1, nx), y))
    pl.when(jnp.logical_not(is_head))(to_head.start)
    pl.when(y > 0)(to_south.start)
    pl.when((place == 0) & (px > 0))(to_back.start)

    mine = jnp.concatenate([c2[pl.ds(coarse_row(j), 8), :] for j in range(8, 12)], axis=0)
    four = lambda x: jnp.concatenate([x] * 4, axis=0)
    cnt32, alive32 = four(cnt8), four(alive)

    def shifted(value, sign):
        out = pltpu.roll(value, (8 * sign) % 128, 1)
        for k in range(2, 5):
            out = jnp.where(cnt32 == k, pltpu.roll(value, (8 * k * sign) % 128, 1), out)
        return out

    cd[0] = shifted(mine, -1)
    cu[0] = mine
    along = [copy_to(cd.at[0], cd.at[1], s2.at[0], r2.at[0], near(1, 0)),
             copy_to(cu.at[0], cu.at[1], s2.at[1], r2.at[1], near(-1, 0))]
    pl.when(s < ns - 1)(along[0].start)
    pl.when(s > 0)(along[1].start)

    pl.when(s > 0)(along[0].wait_recv)
    pl.when(s < ns - 1)(along[1].wait_recv)
    lo32 = four((pair >= 8 - lo_lane) & (pair < 8))
    hi32 = four((pair >= end) & (pair < end + hi_lane))
    ca[...] = jnp.where(alive32, mine, jnp.where(lo32, cd[1], jnp.where(hi32, shifted(cu[1], 1), 0.0)))
    across = [copy_to(ca, cn, s2.at[2], r2.at[2], near(0, -1)),
              copy_to(ca, cs, s2.at[3], r2.at[3], near(0, 1))]
    pl.when(y > 0)(across[0].start)
    pl.when(y < ny - 1)(across[1].start)

    lines = copy_to(hb.at[pl.ds(0, 8 * (size - 1))], hb.at[pl.ds(0, 8 * (size - 1))], sm.at[0], rb, head_of(px, y))
    beyond = copy_to(hs, hs, sm.at[1], rs, head_of(px, y))
    rounds = copy_to(hall.at[pl.ds(0, n_plane)], hall.at[pl.ds(0, n_plane)], sh, rh, head_of(px, y))

    def round_of(k):
        return copy_to(hall.at[n_plane], hall.at[k], sh, rh, plane(*plane_set[k]))

    @pl.when(is_head)
    def _():
        hb[pl.ds(8 * (size - 1), 8), :] = msg[...]
        lines.wait_recv()
        pl.when(y < ny - 1)(beyond.wait_recv)
        pl.when(px < nx - 1)(to_back.wait_recv)
        acc = tree([hb[pl.ds(8 * k, 8), :] for k in range(size)])
        cross = tree([hb[pl.ds(8 * k + 4, 4), :] * hs[pl.ds(4 * k, 4), :] for k in range(size)])
        cross = jnp.where(y < ny - 1, jnp.sum(cross, axis=0, keepdims=True), 0.0)
        where_is = {p: k for k, p in enumerate(order)}
        row_at = lambda p: hb[pl.ds(8 * where_is[p] + 3, 1), :]
        pairs = [[], []]
        for p in range(size - 1):
            pairs[p % 2].append(row_at(p) * row_at(p + 1))
        pairs[1].append(jnp.where(px < nx - 1, row_at(size - 1) * hx[...], 0.0))
        cross = cross + jnp.where(lane1 < 64, tree(pairs[1]), tree(pairs[0]))
        three = jnp.concatenate([acc[:2], acc[2:3] + 4.0 * cross], axis=0)
        sums = jnp.sum(three, axis=1, keepdims=True)
        hall[n_plane] = jnp.where(lane1 == 0, sums[:1], jnp.where(lane1 == 1, sums[1:2], sums[2:]))
        for k in range(n_plane):
            round_of(k).start()

    def turn_back(src, dst):
        for b in range(2):
            stack = []
            for j in range(8):
                for h in range(2):
                    low, high = src[b, pl.ds(fine_row(16 + j) + 8 * h, 8), :], src[b, pl.ds(fine_row(23 - j) + 8 * h, 8), :]
                    stack.append(jnp.where(alive, jnp.where(upper, high, low), 0.0))
            x = jnp.concatenate(stack, axis=0).T
            for h in range(2):
                for k in range(4):
                    at = 64 * h + 8 * (k + 1)
                    dst[h, k, pl.ds(b, 8, stride=2), :] = x[at:at + 8]

    turn_back(z0, zt)
    turn_back(v, vt)

    pl.when(y > 0)(across[1].wait_recv)
    pl.when(y < ny - 1)(across[0].wait_recv)
    for j in range(4, 12):
        if j < 8:
            at = pl.ds(8 * (7 - j), 8)
            south = jnp.where(y > 0, pltpu.roll(cs[at, :], 64, 1), 0.0)
            north = jnp.where(y < ny - 1, pltpu.roll(cn[at, :], 64, 1), 0.0)
            put_coarse(c, j, jnp.where(upper, north, south))
        else:
            put_coarse(c, j, ca[pl.ds(8 * (j - 8), 8), :])
    rows(coarse_first(c, e1), 5, 12)
    rows(coarse_sweep(c, e1, e2), 6, 12)
    rows(coarse_sweep(c, e2, e3), 7, 12)
    rows(corrected(v, g2, e3, zp), 7, 12)
    rows(smooth(zp, z1, v), 15, 24)
    rows(smooth(z1, w, v), 16, 24)
    turn_back(w, wt)

    def news(k, yy):
        return copy_to(hrow, tot, st, rt, (px * size + k, yy))

    is_first = is_head & (px == 0) & (y == 0)
    tells = is_head & jnp.logical_not(is_first)
    tells_two = is_head & (px == 0) & (y == 1)

    @pl.when(is_head)
    def _():
        rounds.wait_recv()
        total_row = tree([hall[k] for k in range(n_plane + 1)])
        hrow[...] = total_row
        tot[...] = total_row

    @pl.when(tells_two)
    def _():
        for k in list(range(2, size)) + [0]:
            news(k, 0).start()

    @pl.when(tells)
    def _():
        for k in [0] + list(range(2, size)):
            news(k, y).start()

    pl.when(jnp.logical_not(is_head))(news(0, y).wait_recv)
    sums = tot[...]
    pick = lambda k: jnp.broadcast_to(sums[:, k:k + 1], (1, 128))
    rz_all, curv_all, w_all = pick(0), pick(1), pick(2)
    alpha = rz_all / curv_all
    beta = alpha * (w_all / (curv_all * (1.0 / STEP)))
    scaled = alpha * (1.0 / STEP)
    for k in range(4):
        for half in range(2):
            at = pl.ds(128 * half, 128)
            zk = zt[half, k]
            sol_ref[k, :, at] = alpha * zk
            res_ref[k, :, at] = jnp.where(count > k, own[half, k], 0.0) - scaled * vt[half, k]
            dir_ref[k, :, at] = beta * zk - alpha * wt[half, k]

    for o in around:
        for copy in halo[o]:
            pl.when(there(*o))(copy.wait_send)
    pl.when(jnp.logical_not(is_head))(to_head.wait_send)
    pl.when(y > 0)(to_south.wait_send)
    pl.when((place == 0) & (px > 0))(to_back.wait_send)
    pl.when(s < ns - 1)(along[0].wait_send)
    pl.when(s > 0)(along[1].wait_send)
    pl.when(y > 0)(across[0].wait_send)
    pl.when(y < ny - 1)(across[1].wait_send)
    told = copy_to(hall.at[pl.ds(0, size - 1)], hall.at[pl.ds(0, size - 1)], st, rt, head_of(px, y))

    pl.when(is_head)(rounds.wait_send)
    pl.when(tells)(told.wait_send)
    pl.when(tells_two)(told.wait_send)


def kernel(dims, src_hbm, cnt_ref, sol_ref, res_ref, dir_ref, *scratch):
    dma = pltpu.SemaphoreType.DMA
    pl.run_scoped(
        functools.partial(body, dims, src_hbm, cnt_ref, sol_ref, res_ref, dir_ref, scratch),
        dma((14,)), dma((14,)), dma((4,)), dma((4,)), dma((3,)), *[dma] * 7, dma((2,)))


def flush(*refs):
    sources, targets, sem = refs[:3], refs[3:6], refs[6]
    copies = [pltpu.make_async_copy(a, b, sem.at[k]) for k, (a, b) in enumerate(zip(sources, targets))]
    for copy in copies:
        copy.start()
    for copy in copies:
        copy.wait()


def solution(mesh):
    ns, ny = mesh.shape["sfc"], mesh.shape["grp"]
    nx, nz, nc = SHAPES[ns]
    size, n_plane = nz * nc, nx * ny - 1
    dma = pltpu.SemaphoreType.DMA
    block = jax.ShapeDtypeStruct((4, E, 16 * E), F32)
    vmem = pl.BlockSpec(memory_space=pltpu.VMEM)
    hbm = pl.BlockSpec(memory_space=pltpu.HBM)
    slots = lambda *k: pltpu.VMEM((*k, E, 128), F32)
    fine = pltpu.VMEM((2, FINE, 128), F32)
    coarse = pltpu.VMEM((COARSE, 128), F32)
    line = lambda *k: pltpu.VMEM((*k, 128), F32)

    def shards(source, layer_counts):
        counts = jnp.broadcast_to(layer_counts.reshape(1, 1), (16, 128))
        parts = pl.pallas_call(
            functools.partial(kernel, (nx, nz, nc, ny)),
            out_shape=(block, block, block),
            in_specs=[hbm, vmem],
            out_specs=(vmem, vmem, vmem),
            scratch_shapes=[
                slots(2, 4), slots(2), slots(2, 4), slots(2, 4), slots(3, 2), slots(3, 2), *[fine] * 10,
                *[coarse] * 6, line(2, 32), line(2, 32), line(32), line(32), line(32),
                slots(2, 4), slots(2, 4), slots(2, 4),
                line(8), line(4), line(1), line(8 * size), line(4 * size), line(1), line(n_plane + 1, 1),
                line(1), line(1),
            ],
            compiler_params=pltpu.CompilerParams(
                collective_id=0, has_side_effects=True, vmem_limit_bytes=24 << 20),
        )(pltpu.with_memory_space_constraint(source, pltpu.HBM), counts)
        return pl.pallas_call(
            flush, out_shape=(block, block, block), in_specs=[vmem] * 3, out_specs=(hbm,) * 3,
            scratch_shapes=[dma((3,))],
            compiler_params=pltpu.CompilerParams(vmem_limit_bytes=1 << 20),
        )(*parts)

    spec = P("sfc", None, "grp")
    return jax.shard_map(
        shards, mesh=mesh, in_specs=(spec, P("sfc")), out_specs=(spec, spec, spec), check_vma=False)
```

```python
import functools

import jax
import jax.numpy as jnp
from jax import lax
from jax.experimental import pallas as pl
from jax.experimental.pallas import tpu as pltpu
from jax.sharding import PartitionSpec as P

E = 16
OMEGA = 2.0 / 3.0
STEP = OMEGA / 6.0
KEEP = 1.0 - OMEGA
TAU = OMEGA / 1.5
QUARTER = TAU / 4.0
SHAPES = {96: (4, 12, 2), 8: (2, 2, 2)}
MESH = pl.DeviceIdType.MESH
F32 = jnp.float32
FINE = 8 + 24 * 25
COARSE = 8 + 16 * 13
NEED = dict(g=1, q=2, c=1, e1=2, e2=3, e3=4, zp=8, z1=10, z0=11, v=12, g2=13, q2=14, c2=7)


def others(*axes):
    found = [()]
    for count in axes:
        found = [f + (i,) for f in found for i in range(count)]
    far = lambda f: -sum(min(i, n - i) for i, n in zip(f, axes))
    return sorted([f for f in found if any(f)], key=far)


def tree(values):
    while len(values) > 1:
        values = [a + b for a, b in zip(values[::2], values[1::2])] + values[len(values) // 2 * 2:]
    return values[0]


def fine_row(j):
    return 8 + 24 * j


def coarse_row(j):
    return 8 + 16 * j


def body(dims, src_hbm, cnt_ref, sol_ref, res_ref, dir_ref, scratch,
         s1, r1, s2, r2, sm, rb, rs, rx, sh, rh, st, rt, load_sem):
    nx, nz, nc, ny = dims
    (own, last, ysl, ynl, below, above, r, g, q, zp, z1, z0, v, g2, q2, w,
     c, e1, e2, e3, c2, kap, cd, cu, ca, cs, cn, zt, vt, wt,
     msg, face, faces, hb, hs, hx, hall, hrow, tot) = scratch
    s = lax.axis_index("sfc")
    y = lax.axis_index("grp")
    ns, size = nx * nz * nc, nz * nc
    px, place = s // size, lax.rem(s, size)
    is_head = place == 1
    plane_set = others(nx, ny)
    n_plane = len(plane_set)

    loads = [pltpu.make_async_copy(src_hbm.at[:, :, pl.ds(128 * h, 128)], own.at[h], load_sem.at[h]) for h in range(2)]
    for load in loads:
        load.start()

    around = [(1, 1), (1, -1), (-1, 1), (-1, -1), (1, 0), (-1, 0), (0, 1), (0, -1)]
    d_ok = {1: s < ns - 1, -1: s > 0, 0: None}
    y_ok = {1: y < ny - 1, -1: y > 0, 0: None}

    def there(ds, dy):
        conds = [k for k in (d_ok[ds], y_ok[dy]) if k is not None]
        return functools.reduce(jnp.logical_and, conds)

    def beside_of(k, step, count):
        if step == 0:
            return k
        return jnp.where(k < count - 1, k + 1, 0) if step == 1 else jnp.where(k > 0, k - 1, count - 1)

    def near(ds, dy):
        return (beside_of(s, ds, ns), beside_of(y, dy, ny))

    def head_of(x, yy):
        return (x * size + 1, yy)

    def plane(dx, dy):
        return (lax.rem(px + dx, nx) * size + 1, lax.rem(y + dy, ny))

    barrier = pltpu.get_barrier_semaphore()

    def greet(target):
        pl.semaphore_signal(barrier, inc=1, device_id=target, device_id_type=MESH)

    for o in around:
        pl.when(there(*o))(functools.partial(greet, near(*o)))

    @pl.when(is_head)
    def _():
        for o in plane_set:
            greet(plane(*o))
        for k in range(size):
            if k != 1:
                greet((px * size + k, y))

        @pl.when(y < ny - 1)
        def _():
            for k in range(size):
                greet((px * size + k, beside_of(y, 1, ny)))

        @pl.when(px < nx - 1)
        def _():
            greet((beside_of(px, 1, nx) * size, y))

    one = lambda cond: jnp.where(cond, 1, 0)
    beside = (1 + one(s > 0) + one(s < ns - 1)) * (1 + one(y > 0) + one(y < ny - 1)) - 1
    heads = one(y > 0) + one((place == 0) & (px > 0)) + jnp.where(is_head, n_plane, 1)

    blank = jnp.zeros((8, 128), F32)
    for array in (r, g, zp, z1, z0, v, g2):
        for b in range(2):
            for j in range(-1, 25):
                array[b, pl.ds(fine_row(j) + 16, 8), :] = blank
    for array in (c, e1, e2, c2, kap):
        for j in range(-1, 13):
            array[pl.ds(coarse_row(j) + 8, 8), :] = blank
    kap[pl.ds(coarse_row(7), 8), :] = blank

    def clear(cond, box):
        @pl.when(cond)
        def _():
            box[...] = jnp.zeros(box.shape, F32)

    clear(s == 0, below)
    clear(s == ns - 1, above)
    clear(y == 0, ysl)
    clear(y == 0, below.at[0])
    clear(y == 0, above.at[0])
    clear(y == ny - 1, ynl)
    clear(y == ny - 1, below.at[2])
    clear(y == ny - 1, above.at[2])

    count = cnt_ref[...]
    for h in range(2):
        loads[h].wait()
        final = own[h, 0]
        for k in range(1, 4):
            final = jnp.where(count > k, own[h, k], final)
        last[h] = final
    pl.semaphore_wait(barrier, beside + heads)

    def copy_to(src, dst, ss, rs_, target):
        return pltpu.make_async_remote_copy(
            src_ref=src, dst_ref=dst, send_sem=ss, recv_sem=rs_, device_id=target, device_id_type=MESH)

    halo = {}
    made = 0
    for o in around:
        ds, dy = o
        halo[o] = []
        for part in range(2 if dy else 1):
            half = 1 - part if dy == 1 else part
            if ds:
                src, box = (last, below.at[1 - dy]) if ds == 1 else (own.at[:, 0], above.at[1 - dy])
                if dy:
                    src, box = src.at[half], box.at[half]
                if part:
                    src, box = (ref.at[pl.ds(8 if ds == 1 else 0, 8)] for ref in (src, box))
            else:
                src, box = own.at[half], (ysl if dy == 1 else ynl).at[half]
            halo[o].append(copy_to(src, box, s1.at[made], r1.at[made], near(*o)))
            made += 1
    for part in range(2):
        for o in around:
            if part < len(halo[o]):
                pl.when(there(*o))(halo[o][part].start)

    def arrived(ds, dy, part=0):
        pl.when(there(-ds, -dy))(halo[ds, dy][part].wait_recv)

    lane = lax.broadcasted_iota(jnp.int32, (8, 128), 1)
    upper = lane >= 64
    pair = lax.rem(lane, 64)
    cnt8 = count[:8]
    end = 8 + 8 * cnt8
    alive = (pair >= 8) & (pair < end)
    lo_lane = jnp.where(s > 0, 8, 0)
    hi_lane = jnp.where(s < ns - 1, 8, 0)
    there_mask = (pair >= 8 - lo_lane) & (pair < end + hi_lane)
    mask = jnp.where(there_mask, 1.0, 0.0).astype(F32)
    outer = jnp.where(upper, jnp.where(y < ny - 1, mask, 0.0), jnp.where(y > 0, mask, 0.0))
    fine_masks = [outer * STEP, outer * STEP, mask * STEP]
    coarse_masks = [outer * QUARTER, outer * QUARTER, mask * QUARTER]
    pieces = (ysl, own, ynl)

    def assemble(block):
        for b in range(2):
            stack = []
            for m in (block, 5 - block):
                take = lambda ref, *k: ref[(*k, pl.ds(b, 8, stride=2), slice(None))]
                up = take(above, m // 2, m % 2)
                stack.append(take(below, m // 2, m % 2))
                for k in range(4):
                    mine = take(pieces[m // 2], m % 2, k)
                    stack.append(jnp.where(cnt8 == k, up, mine) if k else mine)
                stack += [up, blank, blank]
            turned = jnp.concatenate(stack, axis=0).T
            for j in range(8):
                for h in range(2):
                    low, high = turned[16 * j + 8 * h:16 * j + 8 * h + 8], turned[16 * (7 - j) + 8 * h:16 * (7 - j) + 8 * h + 8]
                    value = jnp.where(upper, high, low) * fine_masks[block]
                    r[b, pl.ds(fine_row(8 * block + j) + 8 * h, 8), :] = value
                    if block == 2 and j == 7:
                        r[b, pl.ds(fine_row(24) + 8 * h, 8), :] = pltpu.roll(value, 64, 1)

    def total(ref, b, j, h):
        i = fine_row(j) + 8 * h
        load8 = lambda k: ref[b, pl.ds(k, 8), :]
        across = ref[1 - b, pl.ds(i, 8), :]
        turned = pltpu.roll(across, 127 if b else 1, 1)
        return load8(i), ((load8(i - 24) + load8(i + 24)) + (load8(i - 1) + load8(i + 1))) + (across + turned)

    def put(dst, b, j, h, value):
        dst[b, pl.ds(fine_row(j) + 8 * h, 8), :] = value
        if j == 23:
            dst[b, pl.ds(fine_row(24) + 8 * h, 8), :] = pltpu.roll(value, 64, 1)

    def smooth(src, dst, add=None):
        def row(j):
            for b in range(2):
                for h in range(2):
                    mid, six = total(src, b, j, h)
                    value = KEEP * mid + fine_masks[j // 8] * six
                    if add is not None:
                        value = value + add[b, pl.ds(fine_row(j) + 8 * h, 8), :]
                    put(dst, b, j, h, value)
        return row

    def apply(src, dst):
        def row(j):
            for b in range(2):
                for h in range(2):
                    mid, six = total(src, b, j, h)
                    put(dst, b, j, h, OMEGA * mid - fine_masks[j // 8] * six)
        return row

    def put_coarse(dst, j, value):
        dst[pl.ds(coarse_row(j), 8), :] = value
        if j == 11:
            dst[pl.ds(coarse_row(12), 8), :] = pltpu.roll(value, 64, 1)

    def restrict(src, dst):
        def row(j):
            eight = None
            for b in range(2):
                for k in range(4):
                    part = src[b, pl.ds(fine_row(2 * j + k // 2) + k % 2, 8, stride=2), :]
                    eight = part if eight is None else eight + part
            put_coarse(dst, j, (0.125 * TAU / STEP) * eight)
        return row

    def coarse_total(ref, j):
        i = coarse_row(j)
        load8 = lambda k: ref[pl.ds(k, 8), :]
        mid = load8(i)
        sides = pltpu.roll(mid, 1, 1) + pltpu.roll(mid, 127, 1)
        return mid, ((load8(i - 16) + load8(i + 16)) + (load8(i - 1) + load8(i + 1))) + sides

    def coarse_first(rhs, dst):
        def row(j):
            mid, six = coarse_total(rhs, j)
            put_coarse(dst, j, (1.0 + KEEP) * mid + coarse_masks[j // 4] * six)
        return row

    def coarse_sweep(rhs, src, dst):
        def row(j):
            mid, six = coarse_total(src, j)
            put_coarse(dst, j, (KEEP * mid + rhs[pl.ds(coarse_row(j), 8), :]) + coarse_masks[j // 4] * six)
        return row

    def corrected(rhs, first, coarse, dst):
        def row(j):
            add = coarse[pl.ds(coarse_row(j), 8), :]
            for b in range(2):
                for k in range(4):
                    fine_j = 2 * j + k // 2
                    at = pl.ds(fine_row(fine_j) + k % 2, 8, stride=2)
                    value = (rhs[b, at, :] + first[b, at, :]) + add
                    dst[b, at, :] = value
                    if fine_j == 23:
                        dst[b, pl.ds(fine_row(24) + k % 2, 8, stride=2), :] = pltpu.roll(value, 64, 1)
        return row

    def rows(fn, lo, hi):
        for j in reversed(range(lo, hi)):
            fn(j)

    shrink = lambda lo: lo + 1
    halve = lambda lo: -(-lo // 2)
    double = lambda lo: 2 * lo
    stages = [
        ("g", "r", shrink, smooth(r, g)), ("q", "g", shrink, smooth(g, q)),
        ("c", "q", halve, restrict(q, c)), ("e1", "c", shrink, coarse_first(c, e1)),
        ("e2", "e1", shrink, coarse_sweep(c, e1, e2)), ("e3", "e2", shrink, coarse_sweep(c, e2, e3)),
        ("zp", "e3", double, corrected(r, g, e3, zp)), ("z1", "zp", shrink, smooth(zp, z1, r)),
        ("z0", "z1", shrink, smooth(z1, z0, r)), ("v", "z0", shrink, apply(z0, v)),
        ("g2", "v", shrink, smooth(v, g2)), ("q2", "g2", shrink, smooth(g2, q2)),
        ("c2", "q2", halve, restrict(q2, c2)),
    ]
    coarse_names = ("c", "e1", "e2", "e3", "c2")
    done = {}

    def advance(lo, until=None):
        have = {"r": lo}
        for name, source, change, fn in stages:
            if name == until:
                break
            start = max(change(have[source]), NEED[name])
            stop = done.get(name, 12 if name in coarse_names else 24)
            if start >= stop:
                break
            have[name] = done[name] = start
            if name == "zp":
                rows(fn, start // 2, stop // 2)
            else:
                rows(fn, start, stop)

    arrived(1, 0)
    arrived(-1, 0)
    assemble(2)
    advance(16)
    for dy in (1, -1):
        for ds in (1, -1, 0):
            arrived(ds, dy, 0)
    assemble(1)
    advance(8, 'z0')
    for dy in (1, -1):
        for ds in (1, -1, 0):
            arrived(ds, dy, 1)
    assemble(0)
    advance(0)

    rz = curv = fine = coarse = blank
    for j in range(16, 24):
        for b in range(2):
            for h in range(2):
                at = (b, pl.ds(fine_row(j) + 8 * h, 8))
                vy, gy, qy, zy = v[at], g2[at], q2[at], z0[at]
                rz = rz + r[at] * zy
                curv = curv + zy * vy
                fine = fine + (vy * ((vy + gy) + qy) + gy * qy)
    for j in range(8, 12):
        mid, six = coarse_total(c2, j)
        put_coarse(kap, j, jnp.where(alive, KEEP * mid + coarse_masks[2] * six, 0.0))
    for j in range(8, 12):
        k, six = coarse_total(kap, j)
        cc = c2[pl.ds(coarse_row(j), 8), :]
        coarse = coarse + (cc * (cc + k) + k * ((1.0 + KEEP) * k + QUARTER * six))
    column = lambda value: jnp.sum(jnp.where(alive, value, 0.0), axis=0, keepdims=True)
    inner = jnp.concatenate([kap[pl.ds(coarse_row(j), 8), :] for j in range(8, 12)], axis=0)
    turned = jnp.concatenate([inner] * 4, axis=0).T
    cnt1, lane1 = cnt8[:1], lane[:1]
    ends = []
    for h in (0, 64):
        tail = turned[h + 15:h + 16]
        for k in range(2, 5):
            tail = jnp.where(cnt1 == k, turned[h + 7 + 8 * k:h + 8 + 8 * k], tail)
        ends.append((turned[h + 8:h + 9], tail))
    second = lax.rem(lane1, 64) >= 32
    first_face, last_face = (jnp.where(second, ends[1][k], ends[0][k]) for k in range(2))
    swap = jnp.where(lax.rem(place, 2) == 1, 64, 0)
    d_face = jnp.where((lane1 >= swap) & (lane1 < swap + 64), first_face, last_face)
    sides = kap[pl.ds(coarse_row(8), 8), :]
    swapped = pltpu.roll(sides, 64, 1)
    north_face = jnp.where(upper[:4], sides[:4], swapped[4:])
    south_face = jnp.where(upper[:4], swapped[:4], sides[4:])
    msg[...] = jnp.concatenate(
        [column(rz), column(curv), (1.0 / STEP) * column(fine) + (8.0 / TAU) * column(coarse), d_face, north_face],
        axis=0)
    face[...] = south_face
    faces[...] = d_face

    order = [0] + list(range(2, size)) + [1]
    box = jnp.where(place > 1, place - 1, 0)
    box = jnp.where(is_head, size - 1, box)
    to_head = copy_to(msg, hb.at[pl.ds(pl.multiple_of(8 * box, 8), 8)], sm.at[0], rb, head_of(px, y))
    to_south = copy_to(face, hs.at[pl.ds(pl.multiple_of(4 * box, 4), 4)], sm.at[1], rs, head_of(px, beside_of(y, -1, ny)))
    to_back = copy_to(faces, hx, sm.at[2], rx, head_of(beside_of(px, -1, nx), y))
    pl.when(jnp.logical_not(is_head))(to_head.start)
    pl.when(y > 0)(to_south.start)
    pl.when((place == 0) & (px > 0))(to_back.start)

    mine = jnp.concatenate([c2[pl.ds(coarse_row(j), 8), :] for j in range(8, 12)], axis=0)
    four = lambda x: jnp.concatenate([x] * 4, axis=0)
    cnt32, alive32 = four(cnt8), four(alive)

    def shifted(value, sign):
        out = pltpu.roll(value, (8 * sign) % 128, 1)
        for k in range(2, 5):
            out = jnp.where(cnt32 == k, pltpu.roll(value, (8 * k * sign) % 128, 1), out)
        return out

    cd[0] = shifted(mine, -1)
    cu[0] = mine
    along = [copy_to(cd.at[0], cd.at[1], s2.at[0], r2.at[0], near(1, 0)),
             copy_to(cu.at[0], cu.at[1], s2.at[1], r2.at[1], near(-1, 0))]
    pl.when(s < ns - 1)(along[0].start)
    pl.when(s > 0)(along[1].start)

    pl.when(s > 0)(along[0].wait_recv)
    pl.when(s < ns - 1)(along[1].wait_recv)
    lo32 = four((pair >= 8 - lo_lane) & (pair < 8))
    hi32 = four((pair >= end) & (pair < end + hi_lane))
    ca[...] = jnp.where(alive32, mine, jnp.where(lo32, cd[1], jnp.where(hi32, shifted(cu[1], 1), 0.0)))
    across = [copy_to(ca, cn, s2.at[2], r2.at[2], near(0, -1)),
              copy_to(ca, cs, s2.at[3], r2.at[3], near(0, 1))]
    pl.when(y > 0)(across[0].start)
    pl.when(y < ny - 1)(across[1].start)

    lines = copy_to(hb.at[pl.ds(0, 8 * (size - 1))], hb.at[pl.ds(0, 8 * (size - 1))], sm.at[0], rb, head_of(px, y))
    beyond = copy_to(hs, hs, sm.at[1], rs, head_of(px, y))
    rounds = copy_to(hall.at[pl.ds(0, n_plane)], hall.at[pl.ds(0, n_plane)], sh, rh, head_of(px, y))

    def round_of(k):
        return copy_to(hall.at[n_plane], hall.at[k], sh, rh, plane(*plane_set[k]))

    @pl.when(is_head)
    def _():
        hb[pl.ds(8 * (size - 1), 8), :] = msg[...]
        lines.wait_recv()
        pl.when(y < ny - 1)(beyond.wait_recv)
        pl.when(px < nx - 1)(to_back.wait_recv)
        acc = tree([hb[pl.ds(8 * k, 8), :] for k in range(size)])
        cross = tree([hb[pl.ds(8 * k + 4, 4), :] * hs[pl.ds(4 * k, 4), :] for k in range(size)])
        cross = jnp.where(y < ny - 1, jnp.sum(cross, axis=0, keepdims=True), 0.0)
        where_is = {p: k for k, p in enumerate(order)}
        row_at = lambda p: hb[pl.ds(8 * where_is[p] + 3, 1), :]
        pairs = [[], []]
        for p in range(size - 1):
            pairs[p % 2].append(row_at(p) * row_at(p + 1))
        pairs[1].append(jnp.where(px < nx - 1, row_at(size - 1) * hx[...], 0.0))
        cross = cross + jnp.where(lane1 < 64, tree(pairs[1]), tree(pairs[0]))
        three = jnp.concatenate([acc[:2], acc[2:3] + 4.0 * cross], axis=0)
        sums = jnp.sum(three, axis=1, keepdims=True)
        hall[n_plane] = jnp.where(lane1 == 0, sums[:1], jnp.where(lane1 == 1, sums[1:2], sums[2:]))
        for k in range(n_plane):
            round_of(k).start()

    def turn_back(src, dst):
        for b in range(2):
            stack = []
            for j in range(8):
                for h in range(2):
                    low, high = src[b, pl.ds(fine_row(16 + j) + 8 * h, 8), :], src[b, pl.ds(fine_row(23 - j) + 8 * h, 8), :]
                    stack.append(jnp.where(alive, jnp.where(upper, high, low), 0.0))
            x = jnp.concatenate(stack, axis=0).T
            for h in range(2):
                for k in range(4):
                    at = 64 * h + 8 * (k + 1)
                    dst[h, k, pl.ds(b, 8, stride=2), :] = x[at:at + 8]

    turn_back(z0, zt)
    turn_back(v, vt)

    pl.when(y > 0)(across[1].wait_recv)
    pl.when(y < ny - 1)(across[0].wait_recv)
    for j in range(4, 12):
        if j < 8:
            at = pl.ds(8 * (7 - j), 8)
            south = jnp.where(y > 0, pltpu.roll(cs[at, :], 64, 1), 0.0)
            north = jnp.where(y < ny - 1, pltpu.roll(cn[at, :], 64, 1), 0.0)
            put_coarse(c, j, jnp.where(upper, north, south))
        else:
            put_coarse(c, j, ca[pl.ds(8 * (j - 8), 8), :])
    rows(coarse_first(c, e1), 5, 12)
    rows(coarse_sweep(c, e1, e2), 6, 12)
    rows(coarse_sweep(c, e2, e3), 7, 12)
    rows(corrected(v, g2, e3, zp), 7, 12)
    rows(smooth(zp, z1, v), 15, 24)
    rows(smooth(z1, w, v), 16, 24)
    turn_back(w, wt)

    for o in around:
        for copy in halo[o]:
            pl.when(there(*o))(copy.wait_send)
    pl.when(jnp.logical_not(is_head))(to_head.wait_send)
    pl.when(y > 0)(to_south.wait_send)
    pl.when((place == 0) & (px > 0))(to_back.wait_send)
    pl.when(s < ns - 1)(along[0].wait_send)
    pl.when(s > 0)(along[1].wait_send)
    pl.when(y > 0)(across[0].wait_send)
    pl.when(y < ny - 1)(across[1].wait_send)
    pl.when(is_head)(rounds.wait_send)

    def news(k, yy):
        return copy_to(hrow, tot, st, rt, (px * size + k, yy))

    is_first = is_head & (px == 0) & (y == 0)
    tells = is_head & jnp.logical_not(is_first)
    tells_two = is_head & (px == 0) & (y == 1)

    @pl.when(is_head)
    def _():
        rounds.wait_recv()
        total_row = tree([hall[k] for k in range(n_plane + 1)])
        hrow[...] = total_row
        tot[...] = total_row

    @pl.when(tells_two)
    def _():
        for k in list(range(2, size)) + [0]:
            news(k, 0).start()

    @pl.when(tells)
    def _():
        for k in [0] + list(range(2, size)):
            news(k, y).start()

    pl.when(jnp.logical_not(is_head))(news(0, y).wait_recv)
    sums = tot[...]
    pick = lambda k: jnp.broadcast_to(sums[:, k:k + 1], (1, 128))
    rz_all, curv_all, w_all = pick(0), pick(1), pick(2)
    alpha = rz_all / curv_all
    beta = alpha * (w_all / (curv_all * (1.0 / STEP)))
    scaled = alpha * (1.0 / STEP)
    for k in range(4):
        for half in range(2):
            at = pl.ds(128 * half, 128)
            zk = zt[half, k]
            sol_ref[k, :, at] = alpha * zk
            res_ref[k, :, at] = jnp.where(count > k, own[half, k], 0.0) - scaled * vt[half, k]
            dir_ref[k, :, at] = beta * zk - alpha * wt[half, k]

    told = copy_to(hall.at[pl.ds(0, size - 1)], hall.at[pl.ds(0, size - 1)], st, rt, head_of(px, y))

    pl.when(tells)(told.wait_send)
    pl.when(tells_two)(told.wait_send)


def kernel(dims, src_hbm, cnt_ref, sol_ref, res_ref, dir_ref, *scratch):
    dma = pltpu.SemaphoreType.DMA
    pl.run_scoped(
        functools.partial(body, dims, src_hbm, cnt_ref, sol_ref, res_ref, dir_ref, scratch),
        dma((14,)), dma((14,)), dma((4,)), dma((4,)), dma((3,)), *[dma] * 7, dma((2,)))


def flush(*refs):
    sources, targets, sem = refs[:3], refs[3:6], refs[6]
    copies = [pltpu.make_async_copy(a, b, sem.at[k]) for k, (a, b) in enumerate(zip(sources, targets))]
    for copy in copies:
        copy.start()
    for copy in copies:
        copy.wait()


def solution(mesh):
    ns, ny = mesh.shape["sfc"], mesh.shape["grp"]
    nx, nz, nc = SHAPES[ns]
    size, n_plane = nz * nc, nx * ny - 1
    dma = pltpu.SemaphoreType.DMA
    block = jax.ShapeDtypeStruct((4, E, 16 * E), F32)
    vmem = pl.BlockSpec(memory_space=pltpu.VMEM)
    hbm = pl.BlockSpec(memory_space=pltpu.HBM)
    slots = lambda *k: pltpu.VMEM((*k, E, 128), F32)
    fine = pltpu.VMEM((2, FINE, 128), F32)
    coarse = pltpu.VMEM((COARSE, 128), F32)
    line = lambda *k: pltpu.VMEM((*k, 128), F32)

    def shards(source, layer_counts):
        counts = jnp.broadcast_to(layer_counts.reshape(1, 1), (16, 128))
        parts = pl.pallas_call(
            functools.partial(kernel, (nx, nz, nc, ny)),
            out_shape=(block, block, block),
            in_specs=[hbm, vmem],
            out_specs=(vmem, vmem, vmem),
            scratch_shapes=[
                slots(2, 4), slots(2), slots(2, 4), slots(2, 4), slots(3, 2), slots(3, 2), *[fine] * 10,
                *[coarse] * 6, line(2, 32), line(2, 32), line(32), line(32), line(32),
                slots(2, 4), slots(2, 4), slots(2, 4),
                line(8), line(4), line(1), line(8 * size), line(4 * size), line(1), line(n_plane + 1, 1),
                line(1), line(1),
            ],
            compiler_params=pltpu.CompilerParams(
                collective_id=0, has_side_effects=True, vmem_limit_bytes=24 << 20),
        )(pltpu.with_memory_space_constraint(source, pltpu.HBM), counts)
        return pl.pallas_call(
            flush, out_shape=(block, block, block), in_specs=[vmem] * 3, out_specs=(hbm,) * 3,
            scratch_shapes=[dma((3,))],
            compiler_params=pltpu.CompilerParams(vmem_limit_bytes=1 << 20),
        )(*parts)

    spec = P("sfc", None, "grp")
    return jax.shard_map(
        shards, mesh=mesh, in_specs=(spec, P("sfc")), out_specs=(spec, spec, spec), check_vma=False)
```

```python
import functools

import jax
import jax.numpy as jnp
from jax import lax
from jax.experimental import pallas as pl
from jax.experimental.pallas import tpu as pltpu
from jax.sharding import PartitionSpec as P

E = 16
OMEGA = 2.0 / 3.0
STEP = OMEGA / 6.0
KEEP = 1.0 - OMEGA
TAU = OMEGA / 1.5
QUARTER = TAU / 4.0
SHAPES = {96: (4, 12, 2), 8: (2, 2, 2)}
MESH = pl.DeviceIdType.MESH
F32 = jnp.float32
FINE = 8 + 24 * 25
COARSE = 8 + 16 * 13
NEED = dict(g=1, q=2, c=1, e1=2, e2=3, e3=4, zp=8, z1=10, z0=11, v=12, g2=13, q2=14, c2=7)


def others(*axes):
    found = [()]
    for count in axes:
        found = [f + (i,) for f in found for i in range(count)]
    far = lambda f: -sum(min(i, n - i) for i, n in zip(f, axes))
    return sorted([f for f in found if any(f)], key=far)


def tree(values):
    while len(values) > 1:
        values = [a + b for a, b in zip(values[::2], values[1::2])] + values[len(values) // 2 * 2:]
    return values[0]


def fine_row(j):
    return 8 + 24 * j


def coarse_row(j):
    return 8 + 16 * j


def body(dims, src_hbm, cnt_ref, sol_ref, res_ref, dir_ref, scratch,
         s1, r1, s2, r2, sm, rb, rs, rx, sh, rh, st, rt, load_sem):
    nx, nz, nc, ny = dims
    (own, last, ysl, ynl, below, above, r, g, q, zp, z1, z0, v, g2, q2, w,
     c, e1, e2, e3, c2, kap, cd, cu, ca, cs, cn, zt, vt, wt,
     msg, face, faces, hb, hs, hx, hall, hrow, tot) = scratch
    s = lax.axis_index("sfc")
    y = lax.axis_index("grp")
    ns, size = nx * nz * nc, nz * nc
    px, place = s // size, lax.rem(s, size)
    is_head = place == 1
    plane_set = others(nx, ny)
    n_plane = len(plane_set)

    loads = [pltpu.make_async_copy(src_hbm.at[:, :, pl.ds(128 * h, 128)], own.at[h], load_sem.at[h]) for h in range(2)]
    for load in loads:
        load.start()

    around = [(1, 1), (1, -1), (-1, 1), (-1, -1), (1, 0), (-1, 0), (0, 1), (0, -1)]
    d_ok = {1: s < ns - 1, -1: s > 0, 0: None}
    y_ok = {1: y < ny - 1, -1: y > 0, 0: None}

    def there(ds, dy):
        conds = [k for k in (d_ok[ds], y_ok[dy]) if k is not None]
        return functools.reduce(jnp.logical_and, conds)

    def beside_of(k, step, count):
        if step == 0:
            return k
        return jnp.where(k < count - 1, k + 1, 0) if step == 1 else jnp.where(k > 0, k - 1, count - 1)

    def near(ds, dy):
        return (beside_of(s, ds, ns), beside_of(y, dy, ny))

    def head_of(x, yy):
        return (x * size + 1, yy)

    def plane(dx, dy):
        return (lax.rem(px + dx, nx) * size + 1, lax.rem(y + dy, ny))

    barrier = pltpu.get_barrier_semaphore()

    def greet(target):
        pl.semaphore_signal(barrier, inc=1, device_id=target, device_id_type=MESH)

    for o in around[6:] + around[:6]:
        pl.when(there(*o))(functools.partial(greet, near(*o)))

    @pl.when(is_head)
    def _():
        for o in plane_set:
            greet(plane(*o))
        for k in range(size):
            if k != 1:
                greet((px * size + k, y))

        @pl.when(y < ny - 1)
        def _():
            for k in range(size):
                greet((px * size + k, beside_of(y, 1, ny)))

        @pl.when(px < nx - 1)
        def _():
            greet((beside_of(px, 1, nx) * size, y))

    one = lambda cond: jnp.where(cond, 1, 0)
    beside = (1 + one(s > 0) + one(s < ns - 1)) * (1 + one(y > 0) + one(y < ny - 1)) - 1
    heads = one(y > 0) + one((place == 0) & (px > 0)) + jnp.where(is_head, n_plane, 1)

    blank = jnp.zeros((8, 128), F32)
    for array in (r, g, zp, z1, z0, v, g2):
        for b in range(2):
            for j in range(-1, 25):
                array[b, pl.ds(fine_row(j) + 16, 8), :] = blank
    for array in (c, e1, e2, c2, kap):
        for j in range(-1, 13):
            array[pl.ds(coarse_row(j) + 8, 8), :] = blank
    kap[pl.ds(coarse_row(7), 8), :] = blank

    def clear(cond, box):
        @pl.when(cond)
        def _():
            box[...] = jnp.zeros(box.shape, F32)

    clear(s == 0, below)
    clear(s == ns - 1, above)
    clear(y == 0, ysl)
    clear(y == 0, below.at[0])
    clear(y == 0, above.at[0])
    clear(y == ny - 1, ynl)
    clear(y == ny - 1, below.at[2])
    clear(y == ny - 1, above.at[2])

    count = cnt_ref[...]
    for h in range(2):
        loads[h].wait()
        final = own[h, 0]
        for k in range(1, 4):
            final = jnp.where(count > k, own[h, k], final)
        last[h] = final
    pl.semaphore_wait(barrier, beside + heads)

    def copy_to(src, dst, ss, rs_, target):
        return pltpu.make_async_remote_copy(
            src_ref=src, dst_ref=dst, send_sem=ss, recv_sem=rs_, device_id=target, device_id_type=MESH)

    halo = {}
    made = 0
    for o in around:
        ds, dy = o
        halo[o] = []
        for part in range(2 if dy else 1):
            half = 1 - part if dy == 1 else part
            if ds:
                src, box = (last, below.at[1 - dy]) if ds == 1 else (own.at[:, 0], above.at[1 - dy])
                if dy:
                    src, box = src.at[half], box.at[half]
                if part:
                    src, box = (ref.at[pl.ds(8 if ds == 1 else 0, 8)] for ref in (src, box))
            else:
                src, box = own.at[half], (ysl if dy == 1 else ynl).at[half]
            halo[o].append(copy_to(src, box, s1.at[made], r1.at[made], near(*o)))
            made += 1
    for o, part in (
            *[(o, 0) for o in around[4:6]],
            *[(o, 0) for o in around[:4]],
            *[(o, 1) for o in around[:4]],
            *[(o, 0) for o in around[6:]],
            *[(o, 1) for o in around[6:]],
    ):
        pl.when(there(*o))(halo[o][part].start)

    def arrived(ds, dy, part=0):
        pl.when(there(-ds, -dy))(halo[ds, dy][part].wait_recv)

    lane = lax.broadcasted_iota(jnp.int32, (8, 128), 1)
    upper = lane >= 64
    pair = lax.rem(lane, 64)
    cnt8 = count[:8]
    end = 8 + 8 * cnt8
    alive = (pair >= 8) & (pair < end)
    lo_lane = jnp.where(s > 0, 8, 0)
    hi_lane = jnp.where(s < ns - 1, 8, 0)
    there_mask = (pair >= 8 - lo_lane) & (pair < end + hi_lane)
    mask = jnp.where(there_mask, 1.0, 0.0).astype(F32)
    outer = jnp.where(upper, jnp.where(y < ny - 1, mask, 0.0), jnp.where(y > 0, mask, 0.0))
    fine_masks = [outer * STEP, outer * STEP, mask * STEP]
    coarse_masks = [outer * QUARTER, outer * QUARTER, mask * QUARTER]
    pieces = (ysl, own, ynl)

    def assemble(block):
        for b in range(2):
            stack = []
            for m in (block, 5 - block):
                take = lambda ref, *k: ref[(*k, pl.ds(b, 8, stride=2), slice(None))]
                up = take(above, m // 2, m % 2)
                stack.append(take(below, m // 2, m % 2))
                for k in range(4):
                    mine = take(pieces[m // 2], m % 2, k)
                    stack.append(jnp.where(cnt8 == k, up, mine) if k else mine)
                stack += [up, blank, blank]
            turned = jnp.concatenate(stack, axis=0).T
            for j in range(8):
                for h in range(2):
                    low, high = turned[16 * j + 8 * h:16 * j + 8 * h + 8], turned[16 * (7 - j) + 8 * h:16 * (7 - j) + 8 * h + 8]
                    value = jnp.where(upper, high, low) * fine_masks[block]
                    r[b, pl.ds(fine_row(8 * block + j) + 8 * h, 8), :] = value
                    if block == 2 and j == 7:
                        r[b, pl.ds(fine_row(24) + 8 * h, 8), :] = pltpu.roll(value, 64, 1)

    def total(ref, b, j, h):
        i = fine_row(j) + 8 * h
        load8 = lambda k: ref[b, pl.ds(k, 8), :]
        across = ref[1 - b, pl.ds(i, 8), :]
        turned = pltpu.roll(across, 127 if b else 1, 1)
        return load8(i), ((load8(i - 24) + load8(i + 24)) + (load8(i - 1) + load8(i + 1))) + (across + turned)

    def put(dst, b, j, h, value):
        dst[b, pl.ds(fine_row(j) + 8 * h, 8), :] = value
        if j == 23:
            dst[b, pl.ds(fine_row(24) + 8 * h, 8), :] = pltpu.roll(value, 64, 1)

    def smooth(src, dst, add=None):
        def row(j):
            for b in range(2):
                for h in range(2):
                    mid, six = total(src, b, j, h)
                    value = KEEP * mid + fine_masks[j // 8] * six
                    if add is not None:
                        value = value + add[b, pl.ds(fine_row(j) + 8 * h, 8), :]
                    put(dst, b, j, h, value)
        return row

    def apply(src, dst):
        def row(j):
            for b in range(2):
                for h in range(2):
                    mid, six = total(src, b, j, h)
                    put(dst, b, j, h, OMEGA * mid - fine_masks[j // 8] * six)
        return row

    def put_coarse(dst, j, value):
        dst[pl.ds(coarse_row(j), 8), :] = value
        if j == 11:
            dst[pl.ds(coarse_row(12), 8), :] = pltpu.roll(value, 64, 1)

    def restrict(src, dst):
        def row(j):
            eight = None
            for b in range(2):
                for k in range(4):
                    part = src[b, pl.ds(fine_row(2 * j + k // 2) + k % 2, 8, stride=2), :]
                    eight = part if eight is None else eight + part
            put_coarse(dst, j, (0.125 * TAU / STEP) * eight)
        return row

    def coarse_total(ref, j):
        i = coarse_row(j)
        load8 = lambda k: ref[pl.ds(k, 8), :]
        mid = load8(i)
        sides = pltpu.roll(mid, 1, 1) + pltpu.roll(mid, 127, 1)
        return mid, ((load8(i - 16) + load8(i + 16)) + (load8(i - 1) + load8(i + 1))) + sides

    def coarse_first(rhs, dst):
        def row(j):
            mid, six = coarse_total(rhs, j)
            put_coarse(dst, j, (1.0 + KEEP) * mid + coarse_masks[j // 4] * six)
        return row

    def coarse_sweep(rhs, src, dst):
        def row(j):
            mid, six = coarse_total(src, j)
            put_coarse(dst, j, (KEEP * mid + rhs[pl.ds(coarse_row(j), 8), :]) + coarse_masks[j // 4] * six)
        return row

    def corrected(rhs, first, coarse, dst):
        def row(j):
            add = coarse[pl.ds(coarse_row(j), 8), :]
            for b in range(2):
                for k in range(4):
                    fine_j = 2 * j + k // 2
                    at = pl.ds(fine_row(fine_j) + k % 2, 8, stride=2)
                    value = (rhs[b, at, :] + first[b, at, :]) + add
                    dst[b, at, :] = value
                    if fine_j == 23:
                        dst[b, pl.ds(fine_row(24) + k % 2, 8, stride=2), :] = pltpu.roll(value, 64, 1)
        return row

    def rows(fn, lo, hi):
        for j in reversed(range(lo, hi)):
            fn(j)

    shrink = lambda lo: lo + 1
    halve = lambda lo: -(-lo // 2)
    double = lambda lo: 2 * lo
    stages = [
        ("g", "r", shrink, smooth(r, g)), ("q", "g", shrink, smooth(g, q)),
        ("c", "q", halve, restrict(q, c)), ("e1", "c", shrink, coarse_first(c, e1)),
        ("e2", "e1", shrink, coarse_sweep(c, e1, e2)), ("e3", "e2", shrink, coarse_sweep(c, e2, e3)),
        ("zp", "e3", double, corrected(r, g, e3, zp)), ("z1", "zp", shrink, smooth(zp, z1, r)),
        ("z0", "z1", shrink, smooth(z1, z0, r)), ("v", "z0", shrink, apply(z0, v)),
        ("g2", "v", shrink, smooth(v, g2)), ("q2", "g2", shrink, smooth(g2, q2)),
        ("c2", "q2", halve, restrict(q2, c2)),
    ]
    coarse_names = ("c", "e1", "e2", "e3", "c2")
    done = {}

    def advance(lo, until=None):
        have = {"r": lo}
        for name, source, change, fn in stages:
            if name == until:
                break
            start = max(change(have[source]), NEED[name])
            stop = done.get(name, 12 if name in coarse_names else 24)
            if start >= stop:
                break
            have[name] = done[name] = start
            if name == "zp":
                rows(fn, start // 2, stop // 2)
            else:
                rows(fn, start, stop)

    arrived(1, 0)
    arrived(-1, 0)
    assemble(2)
    advance(16)
    for dy in (1, -1):
        for ds in (1, -1, 0):
            arrived(ds, dy, 0)
    assemble(1)
    advance(8, 'z0')
    for dy in (1, -1):
        for ds in (1, -1, 0):
            arrived(ds, dy, 1)
    assemble(0)
    advance(0)

    rz = curv = fine = coarse = blank
    for j in range(16, 24):
        for b in range(2):
            for h in range(2):
                at = (b, pl.ds(fine_row(j) + 8 * h, 8))
                vy, gy, qy, zy = v[at], g2[at], q2[at], z0[at]
                rz = rz + r[at] * zy
                curv = curv + zy * vy
                fine = fine + (vy * ((vy + gy) + qy) + gy * qy)
    for j in range(8, 12):
        mid, six = coarse_total(c2, j)
        put_coarse(kap, j, jnp.where(alive, KEEP * mid + coarse_masks[2] * six, 0.0))
    for j in range(8, 12):
        k, six = coarse_total(kap, j)
        cc = c2[pl.ds(coarse_row(j), 8), :]
        coarse = coarse + (cc * (cc + k) + k * ((1.0 + KEEP) * k + QUARTER * six))
    column = lambda value: jnp.sum(jnp.where(alive, value, 0.0), axis=0, keepdims=True)
    inner = jnp.concatenate([kap[pl.ds(coarse_row(j), 8), :] for j in range(8, 12)], axis=0)
    turned = jnp.concatenate([inner] * 4, axis=0).T
    cnt1, lane1 = cnt8[:1], lane[:1]
    ends = []
    for h in (0, 64):
        tail = turned[h + 15:h + 16]
        for k in range(2, 5):
            tail = jnp.where(cnt1 == k, turned[h + 7 + 8 * k:h + 8 + 8 * k], tail)
        ends.append((turned[h + 8:h + 9], tail))
    second = lax.rem(lane1, 64) >= 32
    first_face, last_face = (jnp.where(second, ends[1][k], ends[0][k]) for k in range(2))
    swap = jnp.where(lax.rem(place, 2) == 1, 64, 0)
    d_face = jnp.where((lane1 >= swap) & (lane1 < swap + 64), first_face, last_face)
    sides = kap[pl.ds(coarse_row(8), 8), :]
    swapped = pltpu.roll(sides, 64, 1)
    north_face = jnp.where(upper[:4], sides[:4], swapped[4:])
    south_face = jnp.where(upper[:4], swapped[:4], sides[4:])
    msg[...] = jnp.concatenate(
        [column(rz), column(curv), (1.0 / STEP) * column(fine) + (8.0 / TAU) * column(coarse), d_face, north_face],
        axis=0)
    face[...] = south_face
    faces[...] = d_face

    order = [0] + list(range(2, size)) + [1]
    box = jnp.where(place > 1, place - 1, 0)
    box = jnp.where(is_head, size - 1, box)
    to_head = copy_to(msg, hb.at[pl.ds(pl.multiple_of(8 * box, 8), 8)], sm.at[0], rb, head_of(px, y))
    to_south = copy_to(face, hs.at[pl.ds(pl.multiple_of(4 * box, 4), 4)], sm.at[1], rs, head_of(px, beside_of(y, -1, ny)))
    to_back = copy_to(faces, hx, sm.at[2], rx, head_of(beside_of(px, -1, nx), y))
    pl.when(jnp.logical_not(is_head))(to_head.start)
    pl.when(y > 0)(to_south.start)
    pl.when((place == 0) & (px > 0))(to_back.start)

    mine = jnp.concatenate([c2[pl.ds(coarse_row(j), 8), :] for j in range(8, 12)], axis=0)
    four = lambda x: jnp.concatenate([x] * 4, axis=0)
    cnt32, alive32 = four(cnt8), four(alive)

    def shifted(value, sign):
        out = pltpu.roll(value, (8 * sign) % 128, 1)
        for k in range(2, 5):
            out = jnp.where(cnt32 == k, pltpu.roll(value, (8 * k * sign) % 128, 1), out)
        return out

    cd[0] = shifted(mine, -1)
    cu[0] = mine
    along = [copy_to(cd.at[0], cd.at[1], s2.at[0], r2.at[0], near(1, 0)),
             copy_to(cu.at[0], cu.at[1], s2.at[1], r2.at[1], near(-1, 0))]
    pl.when(s < ns - 1)(along[0].start)
    pl.when(s > 0)(along[1].start)

    pl.when(s > 0)(along[0].wait_recv)
    pl.when(s < ns - 1)(along[1].wait_recv)
    lo32 = four((pair >= 8 - lo_lane) & (pair < 8))
    hi32 = four((pair >= end) & (pair < end + hi_lane))
    ca[...] = jnp.where(alive32, mine, jnp.where(lo32, cd[1], jnp.where(hi32, shifted(cu[1], 1), 0.0)))
    across = [copy_to(ca, cn, s2.at[2], r2.at[2], near(0, -1)),
              copy_to(ca, cs, s2.at[3], r2.at[3], near(0, 1))]
    pl.when(y > 0)(across[0].start)
    pl.when(y < ny - 1)(across[1].start)

    lines = copy_to(hb.at[pl.ds(0, 8 * (size - 1))], hb.at[pl.ds(0, 8 * (size - 1))], sm.at[0], rb, head_of(px, y))
    beyond = copy_to(hs, hs, sm.at[1], rs, head_of(px, y))
    rounds = copy_to(hall.at[pl.ds(0, n_plane)], hall.at[pl.ds(0, n_plane)], sh, rh, head_of(px, y))

    def round_of(k):
        return copy_to(hall.at[n_plane], hall.at[k], sh, rh, plane(*plane_set[k]))

    @pl.when(is_head)
    def _():
        hb[pl.ds(8 * (size - 1), 8), :] = msg[...]
        lines.wait_recv()
        pl.when(y < ny - 1)(beyond.wait_recv)
        pl.when(px < nx - 1)(to_back.wait_recv)
        acc = tree([hb[pl.ds(8 * k, 8), :] for k in range(size)])
        cross = tree([hb[pl.ds(8 * k + 4, 4), :] * hs[pl.ds(4 * k, 4), :] for k in range(size)])
        cross = jnp.where(y < ny - 1, jnp.sum(cross, axis=0, keepdims=True), 0.0)
        where_is = {p: k for k, p in enumerate(order)}
        row_at = lambda p: hb[pl.ds(8 * where_is[p] + 3, 1), :]
        pairs = [[], []]
        for p in range(size - 1):
            pairs[p % 2].append(row_at(p) * row_at(p + 1))
        pairs[1].append(jnp.where(px < nx - 1, row_at(size - 1) * hx[...], 0.0))
        cross = cross + jnp.where(lane1 < 64, tree(pairs[1]), tree(pairs[0]))
        three = jnp.concatenate([acc[:2], acc[2:3] + 4.0 * cross], axis=0)
        sums = jnp.sum(three, axis=1, keepdims=True)
        hall[n_plane] = jnp.where(lane1 == 0, sums[:1], jnp.where(lane1 == 1, sums[1:2], sums[2:]))
        for k in range(n_plane):
            round_of(k).start()

    def turn_back(src, dst):
        for b in range(2):
            stack = []
            for j in range(8):
                for h in range(2):
                    low, high = src[b, pl.ds(fine_row(16 + j) + 8 * h, 8), :], src[b, pl.ds(fine_row(23 - j) + 8 * h, 8), :]
                    stack.append(jnp.where(alive, jnp.where(upper, high, low), 0.0))
            x = jnp.concatenate(stack, axis=0).T
            for h in range(2):
                for k in range(4):
                    at = 64 * h + 8 * (k + 1)
                    dst[h, k, pl.ds(b, 8, stride=2), :] = x[at:at + 8]

    turn_back(z0, zt)
    turn_back(v, vt)

    pl.when(y > 0)(across[1].wait_recv)
    pl.when(y < ny - 1)(across[0].wait_recv)
    for j in range(4, 12):
        if j < 8:
            at = pl.ds(8 * (7 - j), 8)
            south = jnp.where(y > 0, pltpu.roll(cs[at, :], 64, 1), 0.0)
            north = jnp.where(y < ny - 1, pltpu.roll(cn[at, :], 64, 1), 0.0)
            put_coarse(c, j, jnp.where(upper, north, south))
        else:
            put_coarse(c, j, ca[pl.ds(8 * (j - 8), 8), :])
    rows(coarse_first(c, e1), 5, 12)
    rows(coarse_sweep(c, e1, e2), 6, 12)
    rows(coarse_sweep(c, e2, e3), 7, 12)
    rows(corrected(v, g2, e3, zp), 7, 12)
    rows(smooth(zp, z1, v), 15, 24)
    rows(smooth(z1, w, v), 16, 24)
    turn_back(w, wt)

    for o in around:
        for copy in halo[o]:
            pl.when(there(*o))(copy.wait_send)
    pl.when(jnp.logical_not(is_head))(to_head.wait_send)
    pl.when(y > 0)(to_south.wait_send)
    pl.when((place == 0) & (px > 0))(to_back.wait_send)
    pl.when(s < ns - 1)(along[0].wait_send)
    pl.when(s > 0)(along[1].wait_send)
    pl.when(y > 0)(across[0].wait_send)
    pl.when(y < ny - 1)(across[1].wait_send)
    pl.when(is_head)(rounds.wait_send)

    def news(k, yy):
        return copy_to(hrow, tot, st, rt, (px * size + k, yy))

    is_first = is_head & (px == 0) & (y == 0)
    tells = is_head & jnp.logical_not(is_first)
    tells_two = is_head & (px == 0) & (y == 1)

    @pl.when(is_head)
    def _():
        rounds.wait_recv()
        total_row = tree([hall[k] for k in range(n_plane + 1)])
        hrow[...] = total_row
        tot[...] = total_row

    @pl.when(tells_two)
    def _():
        for k in list(range(2, size)) + [0]:
            news(k, 0).start()

    @pl.when(tells)
    def _():
        for k in [0] + list(range(2, size)):
            news(k, y).start()

    pl.when(jnp.logical_not(is_head))(news(0, y).wait_recv)
    sums = tot[...]
    pick = lambda k: jnp.broadcast_to(sums[:, k:k + 1], (1, 128))
    rz_all, curv_all, w_all = pick(0), pick(1), pick(2)
    alpha = rz_all / curv_all
    beta = alpha * (w_all / (curv_all * (1.0 / STEP)))
    scaled = alpha * (1.0 / STEP)
    for k in range(4):
        for half in range(2):
            at = pl.ds(128 * half, 128)
            zk = zt[half, k]
            sol_ref[k, :, at] = alpha * zk
            res_ref[k, :, at] = jnp.where(count > k, own[half, k], 0.0) - scaled * vt[half, k]
            dir_ref[k, :, at] = beta * zk - alpha * wt[half, k]

    told = copy_to(hall.at[pl.ds(0, size - 1)], hall.at[pl.ds(0, size - 1)], st, rt, head_of(px, y))

    pl.when(tells)(told.wait_send)
    pl.when(tells_two)(told.wait_send)


def kernel(dims, src_hbm, cnt_ref, sol_ref, res_ref, dir_ref, *scratch):
    dma = pltpu.SemaphoreType.DMA
    pl.run_scoped(
        functools.partial(body, dims, src_hbm, cnt_ref, sol_ref, res_ref, dir_ref, scratch),
        dma((14,)), dma((14,)), dma((4,)), dma((4,)), dma((3,)), *[dma] * 7, dma((2,)))


def flush(*refs):
    sources, targets, sem = refs[:3], refs[3:6], refs[6]
    copies = [pltpu.make_async_copy(a, b, sem.at[k]) for k, (a, b) in enumerate(zip(sources, targets))]
    for copy in copies:
        copy.start()
    for copy in copies:
        copy.wait()


def solution(mesh):
    ns, ny = mesh.shape["sfc"], mesh.shape["grp"]
    nx, nz, nc = SHAPES[ns]
    size, n_plane = nz * nc, nx * ny - 1
    dma = pltpu.SemaphoreType.DMA
    block = jax.ShapeDtypeStruct((4, E, 16 * E), F32)
    vmem = pl.BlockSpec(memory_space=pltpu.VMEM)
    hbm = pl.BlockSpec(memory_space=pltpu.HBM)
    slots = lambda *k: pltpu.VMEM((*k, E, 128), F32)
    fine = pltpu.VMEM((2, FINE, 128), F32)
    coarse = pltpu.VMEM((COARSE, 128), F32)
    line = lambda *k: pltpu.VMEM((*k, 128), F32)

    def shards(source, layer_counts):
        counts = jnp.broadcast_to(layer_counts.reshape(1, 1), (16, 128))
        parts = pl.pallas_call(
            functools.partial(kernel, (nx, nz, nc, ny)),
            out_shape=(block, block, block),
            in_specs=[hbm, vmem],
            out_specs=(vmem, vmem, vmem),
            scratch_shapes=[
                slots(2, 4), slots(2), slots(2, 4), slots(2, 4), slots(3, 2), slots(3, 2), *[fine] * 10,
                *[coarse] * 6, line(2, 32), line(2, 32), line(32), line(32), line(32),
                slots(2, 4), slots(2, 4), slots(2, 4),
                line(8), line(4), line(1), line(8 * size), line(4 * size), line(1), line(n_plane + 1, 1),
                line(1), line(1),
            ],
            compiler_params=pltpu.CompilerParams(
                collective_id=0, has_side_effects=True, vmem_limit_bytes=24 << 20),
        )(pltpu.with_memory_space_constraint(source, pltpu.HBM), counts)
        return pl.pallas_call(
            flush, out_shape=(block, block, block), in_specs=[vmem] * 3, out_specs=(hbm,) * 3,
            scratch_shapes=[dma((3,))],
            compiler_params=pltpu.CompilerParams(vmem_limit_bytes=1 << 20),
        )(*parts)

    spec = P("sfc", None, "grp")
    return jax.shard_map(
        shards, mesh=mesh, in_specs=(spec, P("sfc")), out_specs=(spec, spec, spec), check_vma=False)
```

```python
import functools

import jax
import jax.numpy as jnp
from jax import lax
from jax.experimental import pallas as pl
from jax.experimental.pallas import tpu as pltpu
from jax.sharding import PartitionSpec as P

E = 16
OMEGA = 2.0 / 3.0
STEP = OMEGA / 6.0
KEEP = 1.0 - OMEGA
TAU = OMEGA / 1.5
QUARTER = TAU / 4.0
SHAPES = {96: (4, 12, 2), 8: (2, 2, 2)}
MESH = pl.DeviceIdType.MESH
F32 = jnp.float32
FINE = 8 + 24 * 25
COARSE = 8 + 16 * 13
NEED = dict(g=1, q=2, c=1, e1=2, e2=3, e3=4, zp=8, z1=10, z0=11, v=12, g2=13, q2=14, c2=7)


def others(*axes):
    found = [()]
    for count in axes:
        found = [f + (i,) for f in found for i in range(count)]
    late = [tuple(-i % n for i, n in zip(f, axes)) for f in found]
    rank = {f: (-min(l[-1], axes[-1] - l[-1]), -l[0]) for f, l in zip(found, late)}
    return sorted([f for f in found if any(f)], key=rank.get)


def tree(values):
    while len(values) > 1:
        values = [a + b for a, b in zip(values[::2], values[1::2])] + values[len(values) // 2 * 2:]
    return values[0]


def fine_row(j):
    return 8 + 24 * j


def coarse_row(j):
    return 8 + 16 * j


def body(dims, src_hbm, cnt_ref, sol_ref, res_ref, dir_ref, scratch,
         s1, r1, s2, r2, sm, rb, rs, rx, sh, rh, st, rt, load_sem):
    nx, nz, nc, ny = dims
    (own, last, ysl, ynl, below, above, r, g, q, zp, z1, z0, v, g2, q2, w,
     c, e1, e2, e3, c2, kap, cd, cu, ca, cs, cn, zt, vt, wt,
     msg, face, faces, hb, hs, hx, hall, hrow, tot) = scratch
    s = lax.axis_index("sfc")
    y = lax.axis_index("grp")
    ns, size = nx * nz * nc, nz * nc
    px, place = s // size, lax.rem(s, size)
    is_head = place == 1
    plane_set = others(nx, ny)
    n_plane = len(plane_set)

    loads = [pltpu.make_async_copy(src_hbm.at[:, :, pl.ds(128 * h, 128)], own.at[h], load_sem.at[h]) for h in range(2)]
    for load in loads:
        load.start()

    around = [(1, 1), (1, -1), (-1, 1), (-1, -1), (1, 0), (-1, 0), (0, 1), (0, -1)]
    d_ok = {1: s < ns - 1, -1: s > 0, 0: None}
    y_ok = {1: y < ny - 1, -1: y > 0, 0: None}

    def there(ds, dy):
        conds = [k for k in (d_ok[ds], y_ok[dy]) if k is not None]
        return functools.reduce(jnp.logical_and, conds)

    def beside_of(k, step, count):
        if step == 0:
            return k
        return jnp.where(k < count - 1, k + 1, 0) if step == 1 else jnp.where(k > 0, k - 1, count - 1)

    def near(ds, dy):
        return (beside_of(s, ds, ns), beside_of(y, dy, ny))

    def head_of(x, yy):
        return (x * size + 1, yy)

    def plane(dx, dy):
        return (lax.rem(px + dx, nx) * size + 1, lax.rem(y + dy, ny))

    barrier = pltpu.get_barrier_semaphore()

    def greet(target):
        pl.semaphore_signal(barrier, inc=1, device_id=target, device_id_type=MESH)

    for o in around[6:] + around[:6]:
        pl.when(there(*o))(functools.partial(greet, near(*o)))

    @pl.when(is_head)
    def _():
        for o in plane_set:
            greet(plane(*o))
        for k in range(size):
            if k != 1:
                greet((px * size + k, y))

        @pl.when(y < ny - 1)
        def _():
            for k in range(size):
                greet((px * size + k, beside_of(y, 1, ny)))

        @pl.when(px < nx - 1)
        def _():
            greet((beside_of(px, 1, nx) * size, y))

    one = lambda cond: jnp.where(cond, 1, 0)
    beside = (1 + one(s > 0) + one(s < ns - 1)) * (1 + one(y > 0) + one(y < ny - 1)) - 1
    heads = one(y > 0) + one((place == 0) & (px > 0)) + jnp.where(is_head, n_plane, 1)

    blank = jnp.zeros((8, 128), F32)
    for array in (r, g, zp, z1, z0, v, g2):
        for b in range(2):
            for j in range(-1, 25):
                array[b, pl.ds(fine_row(j) + 16, 8), :] = blank
    for array in (c, e1, e2, c2, kap):
        for j in range(-1, 13):
            array[pl.ds(coarse_row(j) + 8, 8), :] = blank
    kap[pl.ds(coarse_row(7), 8), :] = blank

    def clear(cond, box):
        @pl.when(cond)
        def _():
            box[...] = jnp.zeros(box.shape, F32)

    clear(s == 0, below)
    clear(s == ns - 1, above)
    clear(y == 0, ysl)
    clear(y == 0, below.at[0])
    clear(y == 0, above.at[0])
    clear(y == ny - 1, ynl)
    clear(y == ny - 1, below.at[2])
    clear(y == ny - 1, above.at[2])

    count = cnt_ref[...]
    for h in range(2):
        loads[h].wait()
        final = own[h, 0]
        for k in range(1, 4):
            final = jnp.where(count > k, own[h, k], final)
        last[h] = final
    pl.semaphore_wait(barrier, beside + heads)

    def copy_to(src, dst, ss, rs_, target):
        return pltpu.make_async_remote_copy(
            src_ref=src, dst_ref=dst, send_sem=ss, recv_sem=rs_, device_id=target, device_id_type=MESH)

    halo = {}
    made = 0
    for o in around:
        ds, dy = o
        halo[o] = []
        for part in range(2 if dy else 1):
            half = 1 - part if dy == 1 else part
            if ds:
                src, box = (last, below.at[1 - dy]) if ds == 1 else (own.at[:, 0], above.at[1 - dy])
                if dy:
                    src, box = src.at[half], box.at[half]
                if part:
                    src, box = (ref.at[pl.ds(8 if ds == 1 else 0, 8)] for ref in (src, box))
            else:
                src, box = own.at[half], (ysl if dy == 1 else ynl).at[half]
            halo[o].append(copy_to(src, box, s1.at[made], r1.at[made], near(*o)))
            made += 1
    for o, part in (
            *[(o, 0) for o in around[4:6]],
            *[(o, 0) for o in around[:4]],
            *[(o, 1) for o in around[:4]],
            *[(o, 0) for o in around[6:]],
            *[(o, 1) for o in around[6:]],
    ):
        pl.when(there(*o))(halo[o][part].start)

    def arrived(ds, dy, part=0):
        pl.when(there(-ds, -dy))(halo[ds, dy][part].wait_recv)

    lane = lax.broadcasted_iota(jnp.int32, (8, 128), 1)
    upper = lane >= 64
    pair = lax.rem(lane, 64)
    cnt8 = count[:8]
    end = 8 + 8 * cnt8
    alive = (pair >= 8) & (pair < end)
    lo_lane = jnp.where(s > 0, 8, 0)
    hi_lane = jnp.where(s < ns - 1, 8, 0)
    there_mask = (pair >= 8 - lo_lane) & (pair < end + hi_lane)
    mask = jnp.where(there_mask, 1.0, 0.0).astype(F32)
    outer = jnp.where(upper, jnp.where(y < ny - 1, mask, 0.0), jnp.where(y > 0, mask, 0.0))
    fine_masks = [outer * STEP, outer * STEP, mask * STEP]
    coarse_masks = [outer * QUARTER, outer * QUARTER, mask * QUARTER]
    pieces = (ysl, own, ynl)

    def assemble(block):
        for b in range(2):
            stack = []
            for m in (block, 5 - block):
                take = lambda ref, *k: ref[(*k, pl.ds(b, 8, stride=2), slice(None))]
                up = take(above, m // 2, m % 2)
                stack.append(take(below, m // 2, m % 2))
                for k in range(4):
                    mine = take(pieces[m // 2], m % 2, k)
                    stack.append(jnp.where(cnt8 == k, up, mine) if k else mine)
                stack += [up, blank, blank]
            turned = jnp.concatenate(stack, axis=0).T
            for j in range(8):
                for h in range(2):
                    low, high = turned[16 * j + 8 * h:16 * j + 8 * h + 8], turned[16 * (7 - j) + 8 * h:16 * (7 - j) + 8 * h + 8]
                    value = jnp.where(upper, high, low) * fine_masks[block]
                    r[b, pl.ds(fine_row(8 * block + j) + 8 * h, 8), :] = value
                    if block == 2 and j == 7:
                        r[b, pl.ds(fine_row(24) + 8 * h, 8), :] = pltpu.roll(value, 64, 1)

    def total(ref, b, j, h):
        i = fine_row(j) + 8 * h
        load8 = lambda k: ref[b, pl.ds(k, 8), :]
        across = ref[1 - b, pl.ds(i, 8), :]
        turned = pltpu.roll(across, 127 if b else 1, 1)
        return load8(i), ((load8(i - 24) + load8(i + 24)) + (load8(i - 1) + load8(i + 1))) + (across + turned)

    def put(dst, b, j, h, value):
        dst[b, pl.ds(fine_row(j) + 8 * h, 8), :] = value
        if j == 23:
            dst[b, pl.ds(fine_row(24) + 8 * h, 8), :] = pltpu.roll(value, 64, 1)

    def smooth(src, dst, add=None):
        def row(j):
            for b in range(2):
                for h in range(2):
                    mid, six = total(src, b, j, h)
                    value = KEEP * mid + fine_masks[j // 8] * six
                    if add is not None:
                        value = value + add[b, pl.ds(fine_row(j) + 8 * h, 8), :]
                    put(dst, b, j, h, value)
        return row

    def apply(src, dst):
        def row(j):
            for b in range(2):
                for h in range(2):
                    mid, six = total(src, b, j, h)
                    put(dst, b, j, h, OMEGA * mid - fine_masks[j // 8] * six)
        return row

    def put_coarse(dst, j, value):
        dst[pl.ds(coarse_row(j), 8), :] = value
        if j == 11:
            dst[pl.ds(coarse_row(12), 8), :] = pltpu.roll(value, 64, 1)

    def restrict(src, dst):
        def row(j):
            eight = None
            for b in range(2):
                for k in range(4):
                    part = src[b, pl.ds(fine_row(2 * j + k // 2) + k % 2, 8, stride=2), :]
                    eight = part if eight is None else eight + part
            put_coarse(dst, j, (0.125 * TAU / STEP) * eight)
        return row

    def coarse_total(ref, j):
        i = coarse_row(j)
        load8 = lambda k: ref[pl.ds(k, 8), :]
        mid = load8(i)
        sides = pltpu.roll(mid, 1, 1) + pltpu.roll(mid, 127, 1)
        return mid, ((load8(i - 16) + load8(i + 16)) + (load8(i - 1) + load8(i + 1))) + sides

    def coarse_first(rhs, dst):
        def row(j):
            mid, six = coarse_total(rhs, j)
            put_coarse(dst, j, (1.0 + KEEP) * mid + coarse_masks[j // 4] * six)
        return row

    def coarse_sweep(rhs, src, dst):
        def row(j):
            mid, six = coarse_total(src, j)
            put_coarse(dst, j, (KEEP * mid + rhs[pl.ds(coarse_row(j), 8), :]) + coarse_masks[j // 4] * six)
        return row

    def corrected(rhs, first, coarse, dst):
        def row(j):
            add = coarse[pl.ds(coarse_row(j), 8), :]
            for b in range(2):
                for k in range(4):
                    fine_j = 2 * j + k // 2
                    at = pl.ds(fine_row(fine_j) + k % 2, 8, stride=2)
                    value = (rhs[b, at, :] + first[b, at, :]) + add
                    dst[b, at, :] = value
                    if fine_j == 23:
                        dst[b, pl.ds(fine_row(24) + k % 2, 8, stride=2), :] = pltpu.roll(value, 64, 1)
        return row

    def rows(fn, lo, hi):
        for j in reversed(range(lo, hi)):
            fn(j)

    shrink = lambda lo: lo + 1
    halve = lambda lo: -(-lo // 2)
    double = lambda lo: 2 * lo
    stages = [
        ("g", "r", shrink, smooth(r, g)), ("q", "g", shrink, smooth(g, q)),
        ("c", "q", halve, restrict(q, c)), ("e1", "c", shrink, coarse_first(c, e1)),
        ("e2", "e1", shrink, coarse_sweep(c, e1, e2)), ("e3", "e2", shrink, coarse_sweep(c, e2, e3)),
        ("zp", "e3", double, corrected(r, g, e3, zp)), ("z1", "zp", shrink, smooth(zp, z1, r)),
        ("z0", "z1", shrink, smooth(z1, z0, r)), ("v", "z0", shrink, apply(z0, v)),
        ("g2", "v", shrink, smooth(v, g2)), ("q2", "g2", shrink, smooth(g2, q2)),
        ("c2", "q2", halve, restrict(q2, c2)),
    ]
    coarse_names = ("c", "e1", "e2", "e3", "c2")
    done = {}

    def advance(lo, until=None):
        have = {"r": lo}
        for name, source, change, fn in stages:
            if name == until:
                break
            start = max(change(have[source]), NEED[name])
            stop = done.get(name, 12 if name in coarse_names else 24)
            if start >= stop:
                break
            have[name] = done[name] = start
            if name == "zp":
                rows(fn, start // 2, stop // 2)
            else:
                rows(fn, start, stop)

    arrived(1, 0)
    arrived(-1, 0)
    assemble(2)
    advance(16)
    for dy in (1, -1):
        for ds in (1, -1, 0):
            arrived(ds, dy, 0)
    assemble(1)
    advance(8, 'z0')
    for dy in (1, -1):
        for ds in (1, -1, 0):
            arrived(ds, dy, 1)
    assemble(0)
    advance(0)

    rz = curv = fine = coarse = blank
    for j in range(16, 24):
        for b in range(2):
            for h in range(2):
                at = (b, pl.ds(fine_row(j) + 8 * h, 8))
                vy, gy, qy, zy = v[at], g2[at], q2[at], z0[at]
                rz = rz + r[at] * zy
                curv = curv + zy * vy
                fine = fine + (vy * ((vy + gy) + qy) + gy * qy)
    for j in range(8, 12):
        mid, six = coarse_total(c2, j)
        put_coarse(kap, j, jnp.where(alive, KEEP * mid + coarse_masks[2] * six, 0.0))
    for j in range(8, 12):
        k, six = coarse_total(kap, j)
        cc = c2[pl.ds(coarse_row(j), 8), :]
        coarse = coarse + (cc * (cc + k) + k * ((1.0 + KEEP) * k + QUARTER * six))
    column = lambda value: jnp.sum(jnp.where(alive, value, 0.0), axis=0, keepdims=True)
    inner = jnp.concatenate([kap[pl.ds(coarse_row(j), 8), :] for j in range(8, 12)], axis=0)
    turned = jnp.concatenate([inner] * 4, axis=0).T
    cnt1, lane1 = cnt8[:1], lane[:1]
    ends = []
    for h in (0, 64):
        tail = turned[h + 15:h + 16]
        for k in range(2, 5):
            tail = jnp.where(cnt1 == k, turned[h + 7 + 8 * k:h + 8 + 8 * k], tail)
        ends.append((turned[h + 8:h + 9], tail))
    second = lax.rem(lane1, 64) >= 32
    first_face, last_face = (jnp.where(second, ends[1][k], ends[0][k]) for k in range(2))
    swap = jnp.where(lax.rem(place, 2) == 1, 64, 0)
    d_face = jnp.where((lane1 >= swap) & (lane1 < swap + 64), first_face, last_face)
    sides = kap[pl.ds(coarse_row(8), 8), :]
    swapped = pltpu.roll(sides, 64, 1)
    north_face = jnp.where(upper[:4], sides[:4], swapped[4:])
    south_face = jnp.where(upper[:4], swapped[:4], sides[4:])
    msg[...] = jnp.concatenate(
        [column(rz), column(curv), (1.0 / STEP) * column(fine) + (8.0 / TAU) * column(coarse), d_face, north_face],
        axis=0)
    face[...] = south_face
    faces[...] = d_face

    order = [0] + list(range(2, size)) + [1]
    box = jnp.where(place > 1, place - 1, 0)
    box = jnp.where(is_head, size - 1, box)
    to_head = copy_to(msg, hb.at[pl.ds(pl.multiple_of(8 * box, 8), 8)], sm.at[0], rb, head_of(px, y))
    to_south = copy_to(face, hs.at[pl.ds(pl.multiple_of(4 * box, 4), 4)], sm.at[1], rs, head_of(px, beside_of(y, -1, ny)))
    to_back = copy_to(faces, hx, sm.at[2], rx, head_of(beside_of(px, -1, nx), y))
    pl.when(jnp.logical_not(is_head))(to_head.start)
    pl.when(y > 0)(to_south.start)
    pl.when((place == 0) & (px > 0))(to_back.start)

    mine = jnp.concatenate([c2[pl.ds(coarse_row(j), 8), :] for j in range(8, 12)], axis=0)
    four = lambda x: jnp.concatenate([x] * 4, axis=0)
    cnt32, alive32 = four(cnt8), four(alive)

    def shifted(value, sign):
        out = pltpu.roll(value, (8 * sign) % 128, 1)
        for k in range(2, 5):
            out = jnp.where(cnt32 == k, pltpu.roll(value, (8 * k * sign) % 128, 1), out)
        return out

    cd[0] = shifted(mine, -1)
    cu[0] = mine
    along = [copy_to(cd.at[0], cd.at[1], s2.at[0], r2.at[0], near(1, 0)),
             copy_to(cu.at[0], cu.at[1], s2.at[1], r2.at[1], near(-1, 0))]
    pl.when(s < ns - 1)(along[0].start)
    pl.when(s > 0)(along[1].start)

    pl.when(s > 0)(along[0].wait_recv)
    pl.when(s < ns - 1)(along[1].wait_recv)
    lo32 = four((pair >= 8 - lo_lane) & (pair < 8))
    hi32 = four((pair >= end) & (pair < end + hi_lane))
    ca[...] = jnp.where(alive32, mine, jnp.where(lo32, cd[1], jnp.where(hi32, shifted(cu[1], 1), 0.0)))
    across = [copy_to(ca, cn, s2.at[2], r2.at[2], near(0, -1)),
              copy_to(ca, cs, s2.at[3], r2.at[3], near(0, 1))]
    pl.when(y > 0)(across[0].start)
    pl.when(y < ny - 1)(across[1].start)

    lines = copy_to(hb.at[pl.ds(0, 8 * (size - 1))], hb.at[pl.ds(0, 8 * (size - 1))], sm.at[0], rb, head_of(px, y))
    beyond = copy_to(hs, hs, sm.at[1], rs, head_of(px, y))
    rounds = copy_to(hall.at[pl.ds(0, n_plane)], hall.at[pl.ds(0, n_plane)], sh, rh, head_of(px, y))

    def round_of(k):
        return copy_to(hall.at[n_plane], hall.at[k], sh, rh, plane(*plane_set[k]))

    @pl.when(is_head)
    def _():
        hb[pl.ds(8 * (size - 1), 8), :] = msg[...]
        lines.wait_recv()
        pl.when(y < ny - 1)(beyond.wait_recv)
        pl.when(px < nx - 1)(to_back.wait_recv)
        acc = tree([hb[pl.ds(8 * k, 8), :] for k in range(size)])
        cross = tree([hb[pl.ds(8 * k + 4, 4), :] * hs[pl.ds(4 * k, 4), :] for k in range(size)])
        cross = jnp.where(y < ny - 1, jnp.sum(cross, axis=0, keepdims=True), 0.0)
        where_is = {p: k for k, p in enumerate(order)}
        row_at = lambda p: hb[pl.ds(8 * where_is[p] + 3, 1), :]
        pairs = [[], []]
        for p in range(size - 1):
            pairs[p % 2].append(row_at(p) * row_at(p + 1))
        pairs[1].append(jnp.where(px < nx - 1, row_at(size - 1) * hx[...], 0.0))
        cross = cross + jnp.where(lane1 < 64, tree(pairs[1]), tree(pairs[0]))
        three = jnp.concatenate([acc[:2], acc[2:3] + 4.0 * cross], axis=0)
        sums = jnp.sum(three, axis=1, keepdims=True)
        hall[n_plane] = jnp.where(lane1 == 0, sums[:1], jnp.where(lane1 == 1, sums[1:2], sums[2:]))
        for k in range(n_plane):
            round_of(k).start()

    def turn_back(src, dst):
        for b in range(2):
            stack = []
            for j in range(8):
                for h in range(2):
                    low, high = src[b, pl.ds(fine_row(16 + j) + 8 * h, 8), :], src[b, pl.ds(fine_row(23 - j) + 8 * h, 8), :]
                    stack.append(jnp.where(alive, jnp.where(upper, high, low), 0.0))
            x = jnp.concatenate(stack, axis=0).T
            for h in range(2):
                for k in range(4):
                    at = 64 * h + 8 * (k + 1)
                    dst[h, k, pl.ds(b, 8, stride=2), :] = x[at:at + 8]

    turn_back(z0, zt)
    turn_back(v, vt)

    pl.when(y > 0)(across[1].wait_recv)
    pl.when(y < ny - 1)(across[0].wait_recv)
    for j in range(4, 12):
        if j < 8:
            at = pl.ds(8 * (7 - j), 8)
            south = jnp.where(y > 0, pltpu.roll(cs[at, :], 64, 1), 0.0)
            north = jnp.where(y < ny - 1, pltpu.roll(cn[at, :], 64, 1), 0.0)
            put_coarse(c, j, jnp.where(upper, north, south))
        else:
            put_coarse(c, j, ca[pl.ds(8 * (j - 8), 8), :])
    rows(coarse_first(c, e1), 5, 12)
    rows(coarse_sweep(c, e1, e2), 6, 12)
    rows(coarse_sweep(c, e2, e3), 7, 12)
    rows(corrected(v, g2, e3, zp), 7, 12)
    rows(smooth(zp, z1, v), 15, 24)
    rows(smooth(z1, w, v), 16, 24)
    turn_back(w, wt)

    for o in around:
        for copy in halo[o]:
            pl.when(there(*o))(copy.wait_send)
    pl.when(jnp.logical_not(is_head))(to_head.wait_send)
    pl.when(y > 0)(to_south.wait_send)
    pl.when((place == 0) & (px > 0))(to_back.wait_send)
    pl.when(s < ns - 1)(along[0].wait_send)
    pl.when(s > 0)(along[1].wait_send)
    pl.when(y > 0)(across[0].wait_send)
    pl.when(y < ny - 1)(across[1].wait_send)
    pl.when(is_head)(rounds.wait_send)

    def news(k, yy):
        return copy_to(hrow, tot, st, rt, (px * size + k, yy))

    is_first = is_head & (px == 0) & (y == 0)
    tells = is_head & jnp.logical_not(is_first)
    tells_two = is_head & (px == 0) & (y == 1)

    @pl.when(is_head)
    def _():
        rounds.wait_recv()
        total_row = tree([hall[k] for k in range(n_plane + 1)])
        hrow[...] = total_row
        tot[...] = total_row

    @pl.when(tells_two)
    def _():
        for k in list(range(2, size)) + [0]:
            news(k, 0).start()

    @pl.when(tells)
    def _():
        for k in [0] + list(range(2, size)):
            news(k, y).start()

    pl.when(jnp.logical_not(is_head))(news(0, y).wait_recv)
    sums = tot[...]
    pick = lambda k: jnp.broadcast_to(sums[:, k:k + 1], (1, 128))
    rz_all, curv_all, w_all = pick(0), pick(1), pick(2)
    alpha = rz_all / curv_all
    beta = alpha * (w_all / (curv_all * (1.0 / STEP)))
    scaled = alpha * (1.0 / STEP)
    for k in range(4):
        for half in range(2):
            at = pl.ds(128 * half, 128)
            zk = zt[half, k]
            sol_ref[k, :, at] = alpha * zk
            res_ref[k, :, at] = jnp.where(count > k, own[half, k], 0.0) - scaled * vt[half, k]
            dir_ref[k, :, at] = beta * zk - alpha * wt[half, k]

    told = copy_to(hall.at[pl.ds(0, size - 1)], hall.at[pl.ds(0, size - 1)], st, rt, head_of(px, y))

    pl.when(tells)(told.wait_send)
    pl.when(tells_two)(told.wait_send)


def kernel(dims, src_hbm, cnt_ref, sol_ref, res_ref, dir_ref, *scratch):
    dma = pltpu.SemaphoreType.DMA
    pl.run_scoped(
        functools.partial(body, dims, src_hbm, cnt_ref, sol_ref, res_ref, dir_ref, scratch),
        dma((14,)), dma((14,)), dma((4,)), dma((4,)), dma((3,)), *[dma] * 7, dma((2,)))


def flush(*refs):
    sources, targets, sem = refs[:3], refs[3:6], refs[6]
    copies = [pltpu.make_async_copy(a, b, sem.at[k]) for k, (a, b) in enumerate(zip(sources, targets))]
    for copy in copies:
        copy.start()
    for copy in copies:
        copy.wait()


def solution(mesh):
    ns, ny = mesh.shape["sfc"], mesh.shape["grp"]
    nx, nz, nc = SHAPES[ns]
    size, n_plane = nz * nc, nx * ny - 1
    dma = pltpu.SemaphoreType.DMA
    block = jax.ShapeDtypeStruct((4, E, 16 * E), F32)
    vmem = pl.BlockSpec(memory_space=pltpu.VMEM)
    hbm = pl.BlockSpec(memory_space=pltpu.HBM)
    slots = lambda *k: pltpu.VMEM((*k, E, 128), F32)
    fine = pltpu.VMEM((2, FINE, 128), F32)
    coarse = pltpu.VMEM((COARSE, 128), F32)
    line = lambda *k: pltpu.VMEM((*k, 128), F32)

    def shards(source, layer_counts):
        counts = jnp.broadcast_to(layer_counts.reshape(1, 1), (16, 128))
        parts = pl.pallas_call(
            functools.partial(kernel, (nx, nz, nc, ny)),
            out_shape=(block, block, block),
            in_specs=[hbm, vmem],
            out_specs=(vmem, vmem, vmem),
            scratch_shapes=[
                slots(2, 4), slots(2), slots(2, 4), slots(2, 4), slots(3, 2), slots(3, 2), *[fine] * 10,
                *[coarse] * 6, line(2, 32), line(2, 32), line(32), line(32), line(32),
                slots(2, 4), slots(2, 4), slots(2, 4),
                line(8), line(4), line(1), line(8 * size), line(4 * size), line(1), line(n_plane + 1, 1),
                line(1), line(1),
            ],
            compiler_params=pltpu.CompilerParams(
                collective_id=0, has_side_effects=True, vmem_limit_bytes=24 << 20),
        )(pltpu.with_memory_space_constraint(source, pltpu.HBM), counts)
        return pl.pallas_call(
            flush, out_shape=(block, block, block), in_specs=[vmem] * 3, out_specs=(hbm,) * 3,
            scratch_shapes=[dma((3,))],
            compiler_params=pltpu.CompilerParams(vmem_limit_bytes=1 << 20),
        )(*parts)

    spec = P("sfc", None, "grp")
    return jax.shard_map(
        shards, mesh=mesh, in_specs=(spec, P("sfc")), out_specs=(spec, spec, spec), check_vma=False)
```
